128 devices in a mesh: group: 8 (over x_lo, y), dp: 16 (over x_hi, z, core).
Axes of the slice: x: 4 (x_hi: 2, x_lo: 2; x = x_hi * 2 + x_lo), y: 4, z: 4, core: 2. Of those that a mesh axis runs over, the one named last changes fastest.
Arguments:
- observations: bfloat16 [128, 64, 4096], P('dp', None, 'group'), may hold values from -6 to 6
- next_observations: bfloat16 [2048, 4096], P('dp', 'group'), may hold values from -6 to 6
- trunk_weights: bfloat16 [2, 4096, 4096], P(None, 'dp', 'group'), may hold values from -0.125 to 0.125
- head_weights: bfloat16 [4096, 19], P('group'), may hold values from -0.25 to 0.25
- acting_policy_logits: float32 [128, 63, 18], P('dp'), may hold values from -16 to 330, as said below
- actions: int32 [128, 63], P('dp'), may hold values from 0 to 17
- rewards: float32 [128, 63], P('dp'), may hold values from -6 to 6
- episode_finished: int32 [128, 63], P('dp'), may hold values 0 or 1
Outputs:
- trunk_grads: float32 [2, 4096, 4096], P(None, 'dp', 'group')
- head_grads: float32 [4096, 19], P(('group', 'dp'))
- actor_logits: float32 [2048, 18], P('dp')
The draws below stay inside these ranges and needn't reach their ends.
Inputs may be any that keep to these rules, and one draw needn't show every extreme that they name: `acting_policy_logits`: Real-valued scores, one row for each step and trajectory.
All inputs are finite; a program needn't handle non-finite values. No bound on the sum of `episode_finished` on one device may be relied on, other than what follows from the above.
Results may differ from the reference program's by a relative error of at most 0.012.
Values may be sent and summed in bfloat16 or wider, within the bound.
A program may use at most 128 MiB of HBM per device.

```python
import jax
import jax.numpy as jnp
from jax import lax

D = 4096
A = 18
HEADS = 19
LAYERS = 2
STEPS = 64
TRAJ = 128
ACTORS = 2048


def draw_acting_policy_logits(key, part):
    base_key = jax.random.fold_in(key, 11)
    first_key = jax.random.fold_in(base_key, 0)
    shape = (TRAJ, STEPS - 1, A)
    score_values = jnp.clip(3.0 * jax.random.normal(first_key, shape, jnp.float32), -15.0, 15.0)
    return score_values


def plant(entries, stream_key, low, top_value):
    dims = entries.shape
    spot = [jax.random.randint(jax.random.fold_in(stream_key, axis), (), 0, dims[axis]) for axis in range(len(dims))]
    entries = entries.at[tuple(spot)].set(low)
    longest = dims.index(max(dims))
    spot[longest] = (spot[longest] + 1) % dims[longest]
    return entries.at[tuple(spot)].set(top_value)


def block_scale(stream_key, shape, shards, smallest, top_value):
    level = 1.0
    for axis_at, parts in shards:
        draws = jax.random.uniform(jax.random.fold_in(jax.random.fold_in(stream_key, 6), axis_at), (parts,), jnp.float32, smallest / len(shards), top_value / len(shards))
        level = level * jnp.repeat(jnp.exp(draws), shape[axis_at] // parts).reshape((-1,) + (1,) * (len(shape) - 1 - axis_at))
    return level


def bell_draw(own_key, extent, deviation, limit, cuts=(), kind=jnp.bfloat16):
    array = jax.random.normal(own_key, extent, jnp.float32) * deviation
    if len(cuts) > 0:
        array = block_scale(own_key, extent, cuts, -0.22, 0.18) * array
    return jnp.clip(array, min=-limit, max=limit).astype(kind)


def setup_inputs(seed: int = 0) -> dict:
    key_of = jax.random.split(jax.random.key(seed), 9)
    observations = bell_draw(key_of[0], (TRAJ, STEPS, D), 1.0, 6.0, ((0, 16), (2, 8)))
    next_observations = bell_draw(key_of[1], (ACTORS, D), 1.0, 6.0, ((0, 16), (1, 8)))
    trunk_weights = bell_draw(key_of[2], (LAYERS, D, D), (D // 2) ** -0.5, 0.125, ((1, 16), (2, 8)))
    head_weights = bell_draw(key_of[3], (D, HEADS), (D // 9) ** -0.5, 0.25, ((0, 8),))
    acting_policy_logits = draw_acting_policy_logits(jax.random.fold_in(key_of[8], 71), 0)
    actions = plant(jax.random.randint(key_of[5], (TRAJ, STEPS - 1), 0, A), jax.random.fold_in(key_of[5], 1), 0, A - 1).astype(jnp.int32)
    rewards = bell_draw(key_of[6], (TRAJ, STEPS - 1), 1.0, 6.0, ((0, 16),), jnp.float32)
    episode_finished = plant((jax.random.randint(key_of[7], (TRAJ, STEPS - 1), 0, 16) < 1).astype(jnp.int32), jax.random.fold_in(key_of[7], 1), 0, 1)
    return dict(observations=observations, next_observations=next_observations, trunk_weights=trunk_weights, head_weights=head_weights, acting_policy_logits=acting_policy_logits, actions=actions, rewards=rewards, episode_finished=episode_finished)


discount_rate = 0.99
value_weight = 0.5
entropy_weight = 0.1
loss_divisor = 16.0


def contract_rows(left, right):
    return lax.dot_general(left, right, (((0,), (0,)), ((), ())), preferred_element_type=jnp.float32)


def contract_cols(left, right):
    return lax.dot_general(left, right, (((1,), (1,)), ((), ())), preferred_element_type=jnp.float32)


def silu_slope(pre_value):
    sigma = jax.nn.sigmoid(pre_value)
    return sigma * (1.0 + pre_value * (1.0 - sigma))


def importance_trace_gradients(learner_output, acting_policy_logits, actions, rewards, episode_finished):
    number_of_actions = acting_policy_logits.shape[-1]
    logits = learner_output[:, :, :number_of_actions]
    values = learner_output[:, :, number_of_actions]
    log_policy = jax.nn.log_softmax(logits[:, :-1], axis=-1)
    log_behave = jax.nn.log_softmax(acting_policy_logits, axis=-1)
    chosen = (actions[:, :, None] == jnp.arange(number_of_actions, dtype=jnp.int32)[None, None, :]).astype(jnp.float32)
    ratio = jnp.exp(jnp.sum((log_policy - log_behave) * chosen, axis=-1))
    clipped = jnp.minimum(ratio, 1.0)
    discount = discount_rate * (1.0 - episode_finished.astype(jnp.float32))
    current = values[:, :-1]
    following = values[:, 1:]
    deltas = clipped * (rewards + discount * following - current)

    def backward_step(carried, step_item):
        delta_now, factor_now = step_item
        carried = delta_now + factor_now * carried
        return carried, carried

    start_carry = jnp.zeros((values.shape[0],), jnp.float32)
    _, corrections = lax.scan(backward_step, start_carry, (deltas.T, (discount * clipped).T), reverse=True)
    targets = current + corrections.T
    next_targets = jnp.concatenate([targets[:, 1:], values[:, -1:]], axis=1)
    advantage = clipped * (rewards + discount * next_targets - current)
    probability = jnp.exp(log_policy)
    entropy = -jnp.sum(probability * log_policy, axis=-1)
    logit_grad = (-advantage[..., None] * (chosen - probability)
                  + entropy_weight * probability * (log_policy + entropy[..., None])) / loss_divisor
    value_grad = -value_weight * (targets - current) / loss_divisor
    step_grad = jnp.concatenate([logit_grad, value_grad[..., None]], axis=-1)
    last_row = jnp.zeros((values.shape[0], 1, number_of_actions + 1), jnp.float32)
    return jnp.concatenate([step_grad, last_row], axis=1)


def reference(observations, next_observations, trunk_weights, head_weights, acting_policy_logits, actions, rewards, episode_finished):
    traj_total, step_total, width = observations.shape
    learner_rows = traj_total * step_total
    number_of_actions = acting_policy_logits.shape[-1]
    layer_input = jnp.concatenate([observations.reshape(learner_rows, width), next_observations], axis=0)
    inputs_kept = []
    products_kept = []
    for layer_index in range(trunk_weights.shape[0]):
        inputs_kept.append(layer_input[:learner_rows])
        product = jnp.dot(layer_input, trunk_weights[layer_index], preferred_element_type=jnp.float32)
        products_kept.append(product[:learner_rows])
        layer_input = jax.nn.silu(product).astype(jnp.bfloat16)
    head_out = jnp.dot(layer_input, head_weights, preferred_element_type=jnp.float32)
    actor_logits = head_out[learner_rows:, :number_of_actions]
    learner_output = head_out[:learner_rows].reshape(traj_total, step_total, number_of_actions + 1)
    output_gradient = importance_trace_gradients(learner_output, acting_policy_logits, actions, rewards, episode_finished)
    output_gradient = output_gradient.reshape(learner_rows, number_of_actions + 1).astype(jnp.bfloat16)
    head_grads = contract_rows(layer_input[:learner_rows], output_gradient)
    input_grad = contract_cols(output_gradient, head_weights)
    layer_total = trunk_weights.shape[0]
    grad_list = [None] * layer_total
    for layer_index in range(layer_total - 1, -1, -1):
        pre_grad = (input_grad * silu_slope(products_kept[layer_index])).astype(jnp.bfloat16)
        grad_list[layer_index] = contract_rows(inputs_kept[layer_index], pre_grad)
        if layer_index > 0:
            input_grad = contract_cols(pre_grad, trunk_weights[layer_index])
    return jnp.stack(grad_list), head_grads, actor_logits
```

```python
import functools

import jax
import jax.numpy as jnp
from jax import lax
from jax.experimental import pallas as pl
from jax.experimental.pallas import tpu as pltpu
from jax.sharding import Mesh
from jax.sharding import PartitionSpec as P

AXES = ("xl", "y", "xh", "z", "c")
SIZES = (2, 4, 2, 4, 2)
DP = ("xh", "z", "c")
GROUP = ("xl", "y")
MESH = pl.DeviceIdType.MESH
F32 = jnp.float32
BF16 = jnp.bfloat16

discount_rate = 0.99
value_weight = 0.5
entropy_weight = 0.1
loss_divisor = 16.0

TR = 512
AR = 128
FB = 512
WB = 256
STEPS = 64
ACT = 18
ER = 272
N_SEM = 192


def nn(a, b):
    return jnp.dot(a, b, preferred_element_type=F32)


def nt(a, b):
    return lax.dot_general(a, b, (((1,), (1,)), ((), ())), preferred_element_type=F32)


def tn(a, b):
    return lax.dot_general(a, b, (((0,), (0,)), ((), ())), preferred_element_type=F32)


def vtrace(logits, behave, action, reward, finished):
    row = lax.broadcasted_iota(jnp.int32, logits.shape, 0)
    step = lax.broadcasted_iota(jnp.int32, reward.shape, 1)
    live = step < STEPS - 1
    is_act = row < ACT

    def log_softmax(values):
        top = jnp.max(jnp.where(is_act, values, -3.0e38), axis=0, keepdims=True)
        shifted = jnp.where(is_act, values - top, 0.0)
        total = jnp.sum(jnp.where(is_act, jnp.exp(shifted), 0.0), axis=0, keepdims=True)
        return jnp.where(is_act, shifted - jnp.log(total), 0.0)

    log_policy = log_softmax(logits)
    log_behave = log_softmax(behave)
    chosen = jnp.where(row.astype(F32) == action, 1.0, 0.0)
    ratio = jnp.exp(jnp.sum((log_policy - log_behave) * chosen, axis=0, keepdims=True))
    clipped = jnp.minimum(ratio, 1.0)
    discount = discount_rate * (1.0 - finished)
    current = logits[ACT : ACT + 1, :]
    following = pltpu.roll(current, 127, 1)
    delta = jnp.where(live, clipped * (reward + discount * following - current), 0.0)
    factor = jnp.where(live, discount * clipped, 0.0)
    for shift in (1, 2, 4, 8, 16, 32):
        delta = delta + factor * pltpu.roll(delta, 128 - shift, 1)
        factor = factor * pltpu.roll(factor, 128 - shift, 1)
    targets = current + delta
    next_targets = pltpu.roll(targets, 127, 1)
    advantage = clipped * (reward + discount * next_targets - current)
    probability = jnp.where(is_act, jnp.exp(log_policy), 0.0)
    entropy = -jnp.sum(probability * log_policy, axis=0, keepdims=True)
    logit_grad = (
        -advantage * (chosen - probability)
        + entropy_weight * probability * (log_policy + entropy)
    ) / loss_divisor
    value_grad = -value_weight * (targets - current) / loss_divisor
    grad = jnp.where(is_act, logit_grad, jnp.where(row == ACT, value_grad, 0.0))
    return jnp.where(live, grad, 0.0)


def kernel(
    obs, nxt, wts, head, acting, actions, rewards, finished,
    dw_out, hg_out, al_out,
    xf0, xf1, wf0, wf1, acc, slope0, slope1, x2, headt, tmp, misc,
    hs, hr, ha_s, ha_r, og_s, og_r, pg1, pg0, hgp,
    sb, rb, own,
    dws1, dwr1, q1, rz1a, rz2a, xs1, rx1,
    dws0, dwr0, q0, rz1b, rz2b, xs0, rx0,
    ssem, rsem, lsem,
):
    xl, y, xh, z, c = (lax.axis_index(a) for a in AXES)
    g = xl * 4 + y
    xf, wf = (xf0, xf1), (wf0, wf1)

    def rel_g(dx, dy):
        return ((xl + dx) % 2) * 4 + (y + dy) % 4

    def rel_w(dx, dz):
        return ((xh + dx) % 2) * 4 + (z + dz) % 4

    x_peer = {"xl": 1 - xl}
    y_up, y_down = {"y": (y + 1) % 4}, {"y": (y + 3) % 4}
    h_peer = {"xh": 1 - xh}
    z_up, z_down = {"z": (z + 1) % 4}, {"z": (z + 3) % 4}
    sibling = {"c": 1 - c}

    count = [0]
    sent = []

    def send(src, dst, device):
        index = count[0]
        count[0] += 1
        copy = pltpu.make_async_remote_copy(
            src_ref=src, dst_ref=dst, send_sem=ssem.at[index], recv_sem=rsem.at[index],
            device_id=device, device_id_type=MESH,
        )
        copy.start()
        sent.append(copy)
        return copy

    cb = pl.multiple_of(c * WB, WB)
    wg = xh * 4 + z
    loads = [
        pltpu.make_async_copy(obs, xf0.at[g, pl.ds(0, TR), :], lsem.at[0]),
        pltpu.make_async_copy(wts.at[0], wf0.at[wg, pl.ds(cb, WB), :], lsem.at[1]),
        pltpu.make_async_copy(wts.at[1], wf1.at[wg, pl.ds(cb, WB), :], lsem.at[2]),
        pltpu.make_async_copy(nxt, xf0.at[g, pl.ds(TR, AR), :], lsem.at[3]),
    ]
    for load in loads:
        load.start()

    barrier = pltpu.get_barrier_semaphore()
    friends = [h_peer, z_up, z_down, sibling]
    for k in range(1, 8):
        gt = (g + k) % 8
        friends.append({"xl": gt // 4, "y": gt % 4})
    for friend in friends:
        pl.semaphore_signal(barrier, inc=1, device_id=friend, device_id_type=MESH)
    pl.semaphore_wait(barrier, len(friends))

    def x_start(layer, first, amount):
        buf, half = xf[layer], amount // 2
        lo, hi = pl.ds(first, half), pl.ds(first + half, half)

        def go(block, rows, device):
            return send(buf.at[block, rows, :], buf.at[block, rows, :], device)

        st = {"go": go, "lo": lo, "hi": hi}
        return st

    def x_own(st, rows):
        go, lo = st["go"], st["lo"]
        if rows == "lo":
            st["up_lo"] = go(g, lo, y_up)
            st["x_lo"] = go(g, lo, x_peer)
            st["dn_lo"] = None
        else:
            st["dn_hi"] = go(g, st["hi"], y_down)
            st["x_hi"] = go(g, st["hi"], x_peer)
            st["up_hi"] = go(g, st["hi"], y_up)
            st["dn_lo"] = go(g, lo, y_down)

    def x_fwd1(st):
        go = st["go"]
        st["up_lo"].wait_recv()
        st["f_lo"] = go(rel_g(0, 3), st["lo"], y_up)
        st["dn_hi"].wait_recv()
        st["f_hi"] = go(rel_g(0, 1), st["hi"], y_down)

    def x_fwd2(st):
        go, far = st["go"], rel_g(1, 0)
        st["x_lo"].wait_recv()
        st["p_up_lo"] = go(far, st["lo"], y_up)
        st["p_dn_lo"] = go(far, st["lo"], y_down)
        st["x_hi"].wait_recv()
        st["p_up_hi"] = go(far, st["hi"], y_up)
        st["p_dn_hi"] = go(far, st["hi"], y_down)

    def x_fwd3(st):
        go, far = st["go"], rel_g(0, 2)
        st["f_lo"].wait_recv()
        st["x2_lo"] = go(far, st["lo"], x_peer)
        st["f_hi"].wait_recv()
        st["x2_hi"] = go(far, st["hi"], x_peer)

    def x_near(st):
        st["up_hi"].wait_recv()
        st["dn_lo"].wait_recv()

    def x_far(st):
        for name in ("p_up_lo", "p_up_hi", "p_dn_lo", "p_dn_hi", "x2_lo", "x2_hi"):
            st[name].wait_recv()

    half_w = WB // 2

    def w_piece(block, part):
        if part == "all":
            return (block, pl.ds(cb, WB), slice(None))
        start = cb if part == "lo" else cb + half_w
        return (block, pl.ds(pl.multiple_of(start, half_w), half_w), slice(None))

    def w_start(layer):
        buf = wf[layer]

        def go(block, part, device):
            where = w_piece(block, part)
            return send(buf.at[where], buf.at[where], device)

        st = {"go": go}
        st["up_lo"] = go(wg, "lo", z_up)
        st["dn_hi"] = go(wg, "hi", z_down)
        st["h"] = go(wg, "all", h_peer)
        st["up_hi"] = go(wg, "hi", z_up)
        st["dn_lo"] = go(wg, "lo", z_down)
        st["sib"] = [go(wg, "all", sibling)]
        return st

    def w_share(st, block):
        st["sib"].append(st["go"](block, "all", sibling))

    def w_fwd1(st):
        go = st["go"]
        st["up_lo"].wait_recv()
        st["f_lo"] = go(rel_w(0, 3), "lo", z_up)
        st["dn_hi"].wait_recv()
        st["f_hi"] = go(rel_w(0, 1), "hi", z_down)

    def w_fwd2(st):
        go, far = st["go"], rel_w(1, 0)
        st["h"].wait_recv()
        st["h_up_lo"] = go(far, "lo", z_up)
        st["h_dn_hi"] = go(far, "hi", z_down)
        st["h_up_hi"] = go(far, "hi", z_up)
        st["h_dn_lo"] = go(far, "lo", z_down)
        w_share(st, far)
        st["up_hi"].wait_recv()
        w_share(st, rel_w(0, 3))
        st["dn_lo"].wait_recv()
        w_share(st, rel_w(0, 1))

    def w_fwd3(st):
        go = st["go"]
        st["h_up_lo"].wait_recv()
        st["g_lo"] = go(rel_w(1, 3), "lo", z_up)
        st["h_dn_hi"].wait_recv()
        st["g_hi"] = go(rel_w(1, 1), "hi", z_down)
        st["f_lo"].wait_recv()
        st["f_hi"].wait_recv()
        w_share(st, rel_w(0, 2))

    def w_finish(st):
        st["h_up_hi"].wait_recv()
        w_share(st, rel_w(1, 3))
        st["h_dn_lo"].wait_recv()
        w_share(st, rel_w(1, 1))
        st["g_lo"].wait_recv()
        st["g_hi"].wait_recv()
        w_share(st, rel_w(1, 2))
        for copy in st["sib"]:
            copy.wait_recv()

    def blocks(layer, first, amount, j0, j1, fresh):
        buf, weights = xf[layer], wf[layer]
        tile = min(amount, 256)
        if fresh:
            for r in range(0, amount, tile):
                acc[first + r : first + r + tile, :] = nn(buf[g, first + r : first + r + tile, :], weights[g])

        def body(j, carry):
            block = ((xl + j // 4) % 2) * 4 + (y + j % 4) % 4
            for r in range(0, amount, tile):
                rows = slice(first + r, first + r + tile)
                acc[rows, :] += nn(buf[block, rows, :], weights[block])
            return carry

        lax.fori_loop(j0, j1, body, 0)

    def activate(first, amount, out, slope, tile=64):
        def body(i, carry):
            rows = pl.ds(pl.multiple_of(first + i * tile, tile), tile)
            value = acc[rows, :]
            sigma = jax.nn.sigmoid(value)
            out(rows, (value * sigma).astype(BF16))
            if slope is not None:
                slope[rows, :] = sigma * (1.0 + value * (1.0 - sigma))
            return carry

        lax.fori_loop(0, amount // tile, body, 0)

    def into_x1(rows, value):
        xf1[g, rows, :] = value

    def into_x2(rows, value):
        x2[rows, :] = value

    loads[0].wait()
    loads[1].wait()
    w0 = w_start(0)
    t0 = x_start(0, 0, TR)
    x_own(t0, "lo")
    x_own(t0, "hi")
    loads[2].wait()
    loads[3].wait()

    tmp[...] = jnp.zeros_like(tmp)
    tmp[:, 0 : ACT + 1] = head[...].astype(F32)
    headt[...] = tmp[...].T.astype(BF16)
    tmp[0:128, :] = jnp.zeros((128, 128), F32)
    tmp[0 : STEPS - 1, 0:ACT] = acting[g]
    misc[...] = jnp.zeros_like(misc)
    misc[0:24, :] = tmp[0:128, :].T[0:24, :]
    misc[24:25, 0 : STEPS - 1] = actions[pl.ds(g, 1), :].astype(F32)
    misc[25:26, 0 : STEPS - 1] = rewards[pl.ds(g, 1), :]
    misc[26:27, 0 : STEPS - 1] = finished[pl.ds(g, 1), :].astype(F32)
    hs[...] = jnp.zeros_like(hs)
    tmp[0:128, :] = jnp.zeros((128, 128), F32)

    w_fwd1(w0)
    x_fwd1(t0)
    x_fwd2(t0)
    w_fwd2(w0)
    w_fwd3(w0)
    x_fwd3(t0)
    w_finish(w0)
    w1 = w_start(1)
    x_near(t0)
    blocks(0, 0, TR, 1, 5, True)
    w_fwd1(w1)
    x_far(t0)
    blocks(0, 0, TR, 5, 8, False)

    t1 = x_start(1, 0, TR)
    activate(0, TR // 2, into_x1, slope0)
    x_own(t1, "lo")
    activate(TR // 2, TR // 2, into_x1, slope0)
    x_own(t1, "hi")

    w_fwd2(w1)
    x_fwd1(t1)
    x_fwd2(t1)
    w_fwd3(w1)
    x_fwd3(t1)
    a0 = x_start(0, TR, AR)
    x_own(a0, "lo")
    x_own(a0, "hi")
    w_finish(w1)
    x_near(t1)
    blocks(1, 0, TR, 1, 5, True)
    x_far(t1)
    blocks(1, 0, TR, 5, 8, False)
    activate(0, TR, into_x2, slope1)

    part = nt(headt[0:32, :], x2[0:TR, :])
    for r in range(8):
        hs[r, :, 0:STEPS] = part[0:24, STEPS * r : STEPS * (r + 1)]
    heads = []
    for k in range(1, 8):
        gt = (g + k) % 8
        heads.append(send(hs.at[gt], hr.at[g], {"xl": gt // 4, "y": gt % 4}))
    x_fwd1(a0)
    x_fwd2(a0)
    x_fwd3(a0)
    total = hs[g]
    for k in range(1, 8):
        heads[k - 1].wait_recv()
    for k in range(1, 8):
        total = total + hr[(g + 8 - k) % 8]
    grad = vtrace(total, misc[0:24, :], misc[24:25, :], misc[25:26, :], misc[26:27, :])
    tmp[0:24, :] = grad
    og_s[...] = tmp[0:128, :].T[0:STEPS, :].astype(BF16)
    og_r[g] = og_s[...]
    outs = []
    for k in range(1, 8):
        gt = (g + k) % 8
        outs.append(send(og_s, og_r.at[g], {"xl": gt // 4, "y": gt % 4}))
    for copy in outs:
        copy.wait_recv()

    def slopes(first, amount):
        for r in range(first, first + amount, 256):
            rows = slice(r, r + 256)
            og = og_r[r // STEPS : (r + 256) // STEPS].reshape(256, 128)
            pg1[rows, :] = (nn(og, headt[...]) * slope1[rows, :]).astype(BF16)

    slopes(0, TR)
    lo, hi = slice(0, TR // 2), slice(TR // 2, TR)

    def piece(block, rows):
        return nt(pg1[rows, :], wf1[block])

    def push(k, rows, device):
        start = 0 if rows is lo else TR // 2
        where = (k, pl.ds(start, TR // 2), slice(None))
        return send(sb.at[where], rb.at[where], device)

    where_g = (rel_g(1, 2), rel_g(1, 1), rel_g(1, 3), rel_g(0, 1), rel_g(0, 3), rel_g(0, 2), rel_g(1, 0))

    def make(k):
        for rows in (lo, hi):
            sb[k, rows, :] = piece(where_g[k], rows).astype(BF16)

    make(0)
    s1 = [push(0, lo, x_peer), push(0, hi, x_peer)]
    make(1)
    s2u = [push(1, lo, y_up), push(1, hi, y_up)]
    make(2)
    s2d = [push(2, lo, y_down), push(2, hi, y_down)]
    make(3)
    s5u = [push(3, hi, y_up)]
    make(4)
    s5d = [push(4, lo, y_down)]

    def head_rows(dst, i, block, core):
        base = pl.multiple_of((2 * block + core) * 32, 32)
        dst[i, WB:ER, 0:128] = hgp[pl.ds(base, 16), :].astype(BF16)
        dst[i, WB:ER, 128:256] = hgp[pl.ds(pl.multiple_of(base + 16, 16), 16), :].astype(BF16)
        dst[i, WB:ER, 256:512] = jnp.zeros((ER - WB, 256), BF16)

    def dw_block(i):
        return ((xh + 1 - i % 2) % 2) * 4 + (z + 2 + i // 2) % 4

    def dw_open(layer, pg, dws, dwr, extra):
        base = count[0]
        count[0] += 8
        other = pl.multiple_of((1 - c) * WB, WB)

        def copy_of(i):
            return pltpu.make_async_remote_copy(
                src_ref=dws.at[i], dst_ref=dwr.at[i], send_sem=ssem.at[base + i], recv_sem=rsem.at[base + i],
                device_id=sibling, device_id_type=MESH,
            )

        def body(i, carry):
            block = dw_block(i)
            term = tn(xf[layer][block, 0:TR, pl.ds(other, WB)], pg[...])
            dws[i, 0:WB, :] = term.astype(BF16)
            if extra:
                head_rows(dws, i, block, 1 - c)
            copy_of(i).start()
            return carry

        lax.fori_loop(0, 8, body, 0)
        return copy_of

    def dw_close(layer, pg, copy_of, dwr, q, extra):
        def body(i, carry):
            block = dw_block(i)
            term = tn(xf[layer][block, 0:TR, pl.ds(cb, WB)], pg[...])
            copy_of(i).wait_recv()
            q[i, 0:WB, :] = (term + dwr[i, 0:WB, :].astype(F32)).astype(BF16)
            if extra:
                head_rows(q, i, block, c)
                q[i, WB:ER, :] = (q[i, WB:ER, :].astype(F32) + dwr[i, WB:ER, :].astype(F32)).astype(BF16)
            return carry

        lax.fori_loop(0, 8, body, 0)

    def z_first(q, rz1, size):
        low, high = pl.ds(0, 128), pl.ds(128, size - 128)
        st = {}
        for xr in (0, 1):
            st["a", xr] = send(q.at[xr, low, :], rz1.at[xr, low, :], z_up)
            st["b", xr] = send(q.at[xr, high, :], rz1.at[xr, high, :], z_down)
        return st

    def z_plain(st, q, rz2, size):
        low, high = pl.ds(0, 128), pl.ds(128, size - 128)
        for xr in (0, 1):
            st["up_hi", xr] = send(q.at[6 + xr, high, :], rz2.at[xr, 0, high, :], z_up)
            st["dn_lo", xr] = send(q.at[2 + xr, low, :], rz2.at[xr, 1, low, :], z_down)

    def z_added(st, q, rz1, rz2, size):
        low, high = pl.ds(0, 128), pl.ds(128, size - 128)
        for xr in (0, 1):
            st["a", xr].wait_recv()
            q[6 + xr, 0:128, :] = (q[6 + xr, 0:128, :].astype(F32) + rz1[xr, 0:128, :].astype(F32)).astype(BF16)
            st["up_lo", xr] = send(q.at[6 + xr, low, :], rz2.at[xr, 0, low, :], z_up)
            st["b", xr].wait_recv()
            q[2 + xr, 128:size, :] = (
                q[2 + xr, 128:size, :].astype(F32) + rz1[xr, 128:size, :].astype(F32)
            ).astype(BF16)
            st["dn_hi", xr] = send(q.at[2 + xr, high, :], rz2.at[xr, 1, high, :], z_down)

    def z_sum(st, xr, q, rz2):
        for name in ("up_hi", "dn_lo", "up_lo", "dn_hi"):
            st[name, xr].wait_recv()
        return q[4 + xr].astype(F32) + rz2[xr, 0].astype(F32) + rz2[xr, 1].astype(F32)

    hgp[...] = tn(x2[0:TR, :], og_r[...].reshape(TR, 128))
    copy1 = dw_open(1, pg1, dws1, dwr1, True)
    make(5)
    make(6)
    dw_close(1, pg1, copy1, dwr1, q1, True)
    st1 = z_first(q1, rz1a, ER)
    z_plain(st1, q1, rz2a, ER)
    for rows in (lo, hi):
        own[rows, :] = piece(g, rows)

    def add_in(k, rows, *terms):
        value = sb[k, rows, :].astype(F32)
        for term in terms:
            value = value + rb[term, rows, :].astype(F32)
        sb[k, rows, :] = value.astype(BF16)

    s1[0].wait_recv()
    add_in(5, lo, 0)
    s4u = push(5, lo, y_up)
    s1[1].wait_recv()
    add_in(5, hi, 0)
    s4d = push(5, hi, y_down)
    z_added(st1, q1, rz1a, rz2a, ER)
    s3 = []
    for i, rows in enumerate((lo, hi)):
        s2u[i].wait_recv()
        s2d[i].wait_recv()
        add_in(6, rows, 1, 2)
        s3.append(push(6, rows, x_peer))
    s4u.wait_recv()
    add_in(3, lo, 5)
    s5u.append(push(3, lo, y_up))
    s4d.wait_recv()
    add_in(4, hi, 5)
    s5d.append(push(4, hi, y_down))

    x_near(a0)
    x_far(a0)
    blocks(0, TR, AR, 1, 8, True)
    activate(TR, AR, into_x1, None)

    xs1[...] = z_sum(st1, 0, q1, rz2a).astype(BF16)
    h1 = send(xs1, rx1, h_peer)

    for copy in s5u + s5d + s3:
        copy.wait_recv()
    for r in range(0, TR, 64):
        rows = slice(r, r + 64)
        value = own[rows, :] + rb[3, rows, :].astype(F32) + rb[4, rows, :].astype(F32) + rb[6, rows, :].astype(F32)
        pg0[rows, :] = (value * slope0[rows, :]).astype(BF16)

    a1 = x_start(1, TR, AR)
    x_own(a1, "lo")
    x_own(a1, "hi")
    copy0 = dw_open(0, pg0, dws0, dwr0, False)
    dw_close(0, pg0, copy0, dwr0, q0, False)
    st0 = z_first(q0, rz1b, WB)
    z_plain(st0, q0, rz2b, WB)

    x_fwd1(a1)
    x_fwd2(a1)
    value = z_sum(st1, 1, q1, rz2a)
    h1.wait_recv()
    value = value + rx1[...].astype(F32)
    dw_out[1] = value[0:WB, :]
    hg_out[0:16, :] = value[WB:ER, 0 : ACT + 1]
    hg_out[16:32, :] = value[WB:ER, 128 : 128 + ACT + 1]
    z_added(st0, q0, rz1b, rz2b, WB)
    x_fwd3(a1)
    x_near(a1)
    x_far(a1)
    blocks(1, TR, AR, 1, 8, True)
    activate(TR, AR, into_x2, None)
    ha_s[...] = nt(headt[0:32, :], x2[TR : TR + AR, :])[0:24, :]
    acts = []
    for k in range(1, 8):
        gt = (g + k) % 8
        acts.append(send(ha_s, ha_r.at[g], {"xl": gt // 4, "y": gt % 4}))

    xs0[...] = z_sum(st0, 0, q0, rz2b).astype(BF16)
    h0 = send(xs0, rx0, h_peer)
    for copy in acts:
        copy.wait_recv()
    total = ha_s[...]
    for k in range(1, 8):
        total = total + ha_r[(g + 8 - k) % 8]
    tmp[0:24, :] = total
    al_out[...] = tmp[0:128, :].T[:, 0:ACT]
    value = z_sum(st0, 1, q0, rz2b)
    h0.wait_recv()
    dw_out[0] = value + rx0[...].astype(F32)

    for copy in sent:
        copy.wait_send()

    def drain(i, carry):
        copy1(i).wait_send()
        copy0(i).wait_send()
        return carry

    lax.fori_loop(0, 8, drain, 0)


def per_device(observations, next_observations, trunk_weights, head_weights, acting, actions, rewards, finished):
    v = pltpu.VMEM
    dw_bufs = lambda rows: [
        v((8, rows, FB), BF16), v((8, rows, FB), BF16), v((8, rows, FB), BF16), v((2, rows, FB), BF16),
        v((2, 2, rows, FB), BF16), v((rows, FB), BF16), v((rows, FB), BF16),
    ]
    scratch = [
        v((8, TR + AR, FB), BF16), v((8, TR + AR, FB), BF16), v((8, FB, FB), BF16), v((8, FB, FB), BF16),
        v((TR + AR, FB), F32), v((TR, FB), F32), v((TR, FB), F32), v((TR + AR, FB), BF16),
        v((128, FB), BF16), v((FB, 128), F32), v((32, 128), F32),
        v((8, 24, 128), F32), v((8, 24, 128), F32), v((24, 128), F32), v((8, 24, 128), F32),
        v((STEPS, 128), BF16), v((8, STEPS, 128), BF16), v((TR, FB), BF16), v((TR, FB), BF16), v((FB, 128), F32),
        v((7, TR, FB), BF16), v((7, TR, FB), BF16), v((TR, FB), F32),
        *dw_bufs(ER), *dw_bufs(WB),
        pltpu.SemaphoreType.DMA((N_SEM,)), pltpu.SemaphoreType.DMA((N_SEM,)), pltpu.SemaphoreType.DMA((4,)),
    ]
    hbm = pl.BlockSpec(memory_space=pltpu.HBM)
    vmem = pl.BlockSpec(memory_space=pltpu.VMEM)
    return pl.pallas_call(
        kernel,
        out_shape=(
            jax.ShapeDtypeStruct((2, WB, FB), F32),
            jax.ShapeDtypeStruct((32, ACT + 1), F32),
            jax.ShapeDtypeStruct((AR, ACT), F32),
        ),
        in_specs=[hbm, hbm, hbm, vmem, vmem, vmem, vmem, vmem],
        out_specs=(vmem, vmem, vmem),
        scratch_shapes=scratch,
        compiler_params=pltpu.CompilerParams(
            collective_id=0, has_side_effects=True, vmem_limit_bytes=62 * 1024 * 1024
        ),
        name="learner_step",
    )(observations.reshape(TR, FB), next_observations, trunk_weights, head_weights, acting, actions, rewards, finished)


def solution(mesh):
    split = Mesh(mesh.devices.reshape(SIZES), AXES)
    return jax.shard_map(
        per_device,
        mesh=split,
        in_specs=(
            P(DP, None, GROUP),
            P(DP, GROUP),
            P(None, DP, GROUP),
            P(GROUP, None),
            P(DP, None, None),
            P(DP, None),
            P(DP, None),
            P(DP, None),
        ),
        out_specs=(P(None, DP, GROUP), P(GROUP + DP, None), P(DP, None)),
        check_vma=False,
    )
```

```python
import functools

import jax
import jax.numpy as jnp
from jax import lax
from jax.experimental import pallas as pl
from jax.experimental.pallas import tpu as pltpu
from jax.sharding import Mesh
from jax.sharding import PartitionSpec as P

AXES = ("xl", "y", "xh", "z", "c")
SIZES = (2, 4, 2, 4, 2)
DP = ("xh", "z", "c")
GROUP = ("xl", "y")
MESH = pl.DeviceIdType.MESH
F32 = jnp.float32
BF16 = jnp.bfloat16

discount_rate = 0.99
value_weight = 0.5
entropy_weight = 0.1
loss_divisor = 16.0

TR = 512
AR = 128
FB = 512
WB = 256
STEPS = 64
ACT = 18
ER = 272
N_SEM = 192


def nn(a, b):
    return jnp.dot(a, b, preferred_element_type=F32)


def nt(a, b):
    return lax.dot_general(a, b, (((1,), (1,)), ((), ())), preferred_element_type=F32)


def tn(a, b):
    return lax.dot_general(a, b, (((0,), (0,)), ((), ())), preferred_element_type=F32)


def vtrace(logits, behave, action, reward, finished):
    row = lax.broadcasted_iota(jnp.int32, logits.shape, 0)
    step = lax.broadcasted_iota(jnp.int32, reward.shape, 1)
    live = step < STEPS - 1
    is_act = row < ACT

    def log_softmax(values):
        top = jnp.max(jnp.where(is_act, values, -3.0e38), axis=0, keepdims=True)
        shifted = jnp.where(is_act, values - top, 0.0)
        total = jnp.sum(jnp.where(is_act, jnp.exp(shifted), 0.0), axis=0, keepdims=True)
        return jnp.where(is_act, shifted - jnp.log(total), 0.0)

    log_policy = log_softmax(logits)
    log_behave = log_softmax(behave)
    chosen = jnp.where(row.astype(F32) == action, 1.0, 0.0)
    ratio = jnp.exp(jnp.sum((log_policy - log_behave) * chosen, axis=0, keepdims=True))
    clipped = jnp.minimum(ratio, 1.0)
    discount = discount_rate * (1.0 - finished)
    current = logits[ACT : ACT + 1, :]
    following = pltpu.roll(current, 127, 1)
    delta = jnp.where(live, clipped * (reward + discount * following - current), 0.0)
    factor = jnp.where(live, discount * clipped, 0.0)
    for shift in (1, 2, 4, 8, 16, 32):
        delta = delta + factor * pltpu.roll(delta, 128 - shift, 1)
        factor = factor * pltpu.roll(factor, 128 - shift, 1)
    targets = current + delta
    next_targets = pltpu.roll(targets, 127, 1)
    advantage = clipped * (reward + discount * next_targets - current)
    probability = jnp.where(is_act, jnp.exp(log_policy), 0.0)
    entropy = -jnp.sum(probability * log_policy, axis=0, keepdims=True)
    logit_grad = (
        -advantage * (chosen - probability)
        + entropy_weight * probability * (log_policy + entropy)
    ) / loss_divisor
    value_grad = -value_weight * (targets - current) / loss_divisor
    grad = jnp.where(is_act, logit_grad, jnp.where(row == ACT, value_grad, 0.0))
    return jnp.where(live, grad, 0.0)


def kernel(
    obs, nxt, wts, head, acting, actions, rewards, finished,
    dw_out, hg_out, al_out,
    xf0, xf1, wf0, wf1, acc, slope0, slope1, x2, headt, tmp, misc,
    hs, hr, ha_s, ha_r, og_s, og_r, pg1, pg0, hgp,
    sb, rb, own,
    dws1, dwr1, q1, rz1a, rz2a, xs1, rx1,
    dws0, dwr0, q0, rz1b, rz2b, xs0, rx0,
    ssem, rsem, lsem,
):
    xl, y, xh, z, c = (lax.axis_index(a) for a in AXES)
    g = xl * 4 + y
    xf, wf = (xf0, xf1), (wf0, wf1)

    def rel_g(dx, dy):
        return ((xl + dx) % 2) * 4 + (y + dy) % 4

    def rel_w(dx, dz):
        return ((xh + dx) % 2) * 4 + (z + dz) % 4

    x_peer = {"xl": 1 - xl}
    y_up, y_down = {"y": (y + 1) % 4}, {"y": (y + 3) % 4}
    h_peer = {"xh": 1 - xh}
    z_up, z_down = {"z": (z + 1) % 4}, {"z": (z + 3) % 4}
    sibling = {"c": 1 - c}

    count = [0]
    sent = []

    def send(src, dst, device):
        index = count[0]
        count[0] += 1
        copy = pltpu.make_async_remote_copy(
            src_ref=src, dst_ref=dst, send_sem=ssem.at[index], recv_sem=rsem.at[index],
            device_id=device, device_id_type=MESH,
        )
        copy.start()
        sent.append(copy)
        return copy

    cb = pl.multiple_of(c * WB, WB)
    wg = xh * 4 + z
    loads = [
        pltpu.make_async_copy(obs, xf0.at[g, pl.ds(0, TR), :], lsem.at[0]),
        pltpu.make_async_copy(wts.at[0], wf0.at[wg, pl.ds(cb, WB), :], lsem.at[1]),
        pltpu.make_async_copy(wts.at[1], wf1.at[wg, pl.ds(cb, WB), :], lsem.at[2]),
        pltpu.make_async_copy(nxt, xf0.at[g, pl.ds(TR, AR), :], lsem.at[3]),
    ]
    for load in loads:
        load.start()

    barrier = pltpu.get_barrier_semaphore()
    friends = [h_peer, z_up, z_down, sibling]
    for k in range(1, 8):
        gt = (g + k) % 8
        friends.append({"xl": gt // 4, "y": gt % 4})
    for friend in friends:
        pl.semaphore_signal(barrier, inc=1, device_id=friend, device_id_type=MESH)
    pl.semaphore_wait(barrier, len(friends))

    def x_start(layer, first, amount):
        buf, half = xf[layer], amount // 2
        lo, hi = pl.ds(first, half), pl.ds(first + half, half)

        def go(block, rows, device):
            return send(buf.at[block, rows, :], buf.at[block, rows, :], device)

        st = {"go": go, "lo": lo, "hi": hi}
        return st

    def x_own(st, rows):
        go, lo = st["go"], st["lo"]
        if rows == "lo":
            st["up_lo"] = go(g, lo, y_up)
            st["x_lo"] = go(g, lo, x_peer)
            st["dn_lo"] = None
        else:
            st["dn_hi"] = go(g, st["hi"], y_down)
            st["x_hi"] = go(g, st["hi"], x_peer)
            st["up_hi"] = go(g, st["hi"], y_up)
            st["dn_lo"] = go(g, lo, y_down)

    def x_fwd1(st):
        go = st["go"]
        st["up_lo"].wait_recv()
        st["f_lo"] = go(rel_g(0, 3), st["lo"], y_up)
        st["dn_hi"].wait_recv()
        st["f_hi"] = go(rel_g(0, 1), st["hi"], y_down)

    def x_fwd2(st):
        go, far = st["go"], rel_g(1, 0)
        st["x_lo"].wait_recv()
        st["p_up_lo"] = go(far, st["lo"], y_up)
        st["p_dn_lo"] = go(far, st["lo"], y_down)
        st["x_hi"].wait_recv()
        st["p_up_hi"] = go(far, st["hi"], y_up)
        st["p_dn_hi"] = go(far, st["hi"], y_down)

    def x_fwd3(st):
        go, far = st["go"], rel_g(0, 2)
        st["f_lo"].wait_recv()
        st["x2_lo"] = go(far, st["lo"], x_peer)
        st["f_hi"].wait_recv()
        st["x2_hi"] = go(far, st["hi"], x_peer)

    def x_near(st):
        st["up_hi"].wait_recv()
        st["dn_lo"].wait_recv()

    def x_far(st):
        for name in ("p_up_lo", "p_up_hi", "p_dn_lo", "p_dn_hi", "x2_lo", "x2_hi"):
            st[name].wait_recv()

    half_w = WB // 2

    def w_piece(block, part):
        if part == "all":
            return (block, pl.ds(cb, WB), slice(None))
        start = cb if part == "lo" else cb + half_w
        return (block, pl.ds(pl.multiple_of(start, half_w), half_w), slice(None))

    def w_start(layer):
        buf = wf[layer]

        def go(block, part, device):
            where = w_piece(block, part)
            return send(buf.at[where], buf.at[where], device)

        st = {"go": go}
        st["up_lo"] = go(wg, "lo", z_up)
        st["dn_hi"] = go(wg, "hi", z_down)
        st["h"] = go(wg, "all", h_peer)
        st["up_hi"] = go(wg, "hi", z_up)
        st["dn_lo"] = go(wg, "lo", z_down)
        st["sib"] = [go(wg, "all", sibling)]
        return st

    def w_share(st, block):
        st["sib"].append(st["go"](block, "all", sibling))

    def w_fwd1(st):
        go = st["go"]
        st["up_lo"].wait_recv()
        st["f_lo"] = go(rel_w(0, 3), "lo", z_up)
        st["dn_hi"].wait_recv()
        st["f_hi"] = go(rel_w(0, 1), "hi", z_down)

    def w_fwd2(st):
        go, far = st["go"], rel_w(1, 0)
        st["h"].wait_recv()
        st["h_up_lo"] = go(far, "lo", z_up)
        st["h_dn_hi"] = go(far, "hi", z_down)
        st["h_up_hi"] = go(far, "hi", z_up)
        st["h_dn_lo"] = go(far, "lo", z_down)
        w_share(st, far)
        st["up_hi"].wait_recv()
        w_share(st, rel_w(0, 3))
        st["dn_lo"].wait_recv()
        w_share(st, rel_w(0, 1))

    def w_fwd3(st):
        go = st["go"]
        st["h_up_lo"].wait_recv()
        st["g_lo"] = go(rel_w(1, 3), "lo", z_up)
        st["h_dn_hi"].wait_recv()
        st["g_hi"] = go(rel_w(1, 1), "hi", z_down)
        st["f_lo"].wait_recv()
        st["f_hi"].wait_recv()
        w_share(st, rel_w(0, 2))

    def w_finish(st):
        st["h_up_hi"].wait_recv()
        w_share(st, rel_w(1, 3))
        st["h_dn_lo"].wait_recv()
        w_share(st, rel_w(1, 1))
        st["g_lo"].wait_recv()
        st["g_hi"].wait_recv()
        w_share(st, rel_w(1, 2))
        for copy in st["sib"]:
            copy.wait_recv()

    def blocks(layer, first, amount, j0, j1, fresh):
        buf, weights = xf[layer], wf[layer]
        tile = min(amount, 256)
        if fresh:
            for r in range(0, amount, tile):
                acc[first + r : first + r + tile, :] = nn(buf[g, first + r : first + r + tile, :], weights[g])

        def body(j, carry):
            block = ((xl + j // 4) % 2) * 4 + (y + j % 4) % 4
            for r in range(0, amount, tile):
                rows = slice(first + r, first + r + tile)
                acc[rows, :] += nn(buf[block, rows, :], weights[block])
            return carry

        lax.fori_loop(j0, j1, body, 0)

    def activate(first, amount, out, slope, tile=64):
        def body(i, carry):
            rows = pl.ds(pl.multiple_of(first + i * tile, tile), tile)
            value = acc[rows, :]
            sigma = jax.nn.sigmoid(value)
            out(rows, (value * sigma).astype(BF16))
            if slope is not None:
                slope[rows, :] = sigma * (1.0 + value * (1.0 - sigma))
            return carry

        lax.fori_loop(0, amount // tile, body, 0)

    def into_x1(rows, value):
        xf1[g, rows, :] = value

    def into_x2(rows, value):
        x2[rows, :] = value

    loads[0].wait()
    loads[1].wait()
    w0 = w_start(0)
    t0 = x_start(0, 0, TR)
    x_own(t0, "lo")
    x_own(t0, "hi")
    loads[2].wait()
    loads[3].wait()

    headt[...] = jnp.zeros_like(headt)
    headt[0 : ACT + 1, :] = head[...]
    misc[...] = jnp.zeros_like(misc)
    misc[0:ACT, 0 : STEPS - 1] = acting[:, pl.ds(g, 1), :].reshape(ACT, STEPS - 1)
    misc[24:25, 0 : STEPS - 1] = actions[pl.ds(g, 1), :].astype(F32)
    misc[25:26, 0 : STEPS - 1] = rewards[pl.ds(g, 1), :]
    misc[26:27, 0 : STEPS - 1] = finished[pl.ds(g, 1), :].astype(F32)
    hs[...] = jnp.zeros_like(hs)
    tmp[...] = jnp.zeros_like(tmp)

    w_fwd1(w0)
    x_fwd1(t0)
    x_fwd2(t0)
    w_fwd2(w0)
    x_fwd3(t0)
    w_fwd3(w0)
    w_finish(w0)
    w1 = w_start(1)
    x_near(t0)
    blocks(0, 0, TR, 1, 5, True)
    w_fwd1(w1)
    x_far(t0)
    blocks(0, 0, TR, 5, 8, False)

    t1 = x_start(1, 0, TR)
    activate(0, TR // 2, into_x1, slope0)
    x_own(t1, "lo")
    activate(TR // 2, TR // 2, into_x1, slope0)
    x_own(t1, "hi")

    w_fwd2(w1)
    x_fwd1(t1)
    x_fwd2(t1)
    w_fwd3(w1)
    x_fwd3(t1)
    a0 = x_start(0, TR, AR)
    x_own(a0, "lo")
    x_own(a0, "hi")
    w_finish(w1)
    x_near(t1)
    blocks(1, 0, TR, 1, 5, True)
    x_far(t1)
    blocks(1, 0, TR, 5, 8, False)
    activate(0, TR, into_x2, slope1)

    part = nt(headt[0:32, :], x2[0:TR, :])
    for r in range(8):
        hs[r, :, 0:STEPS] = part[0:24, STEPS * r : STEPS * (r + 1)]
    heads = []
    for k in range(1, 8):
        gt = (g + k) % 8
        heads.append(send(hs.at[gt], hr.at[g], {"xl": gt // 4, "y": gt % 4}))
    x_fwd1(a0)
    x_fwd2(a0)
    x_fwd3(a0)
    total = hs[g]
    for k in range(1, 8):
        heads[k - 1].wait_recv()
    for k in range(1, 8):
        total = total + hr[(g + 8 - k) % 8]
    grad = vtrace(total, misc[0:24, :], misc[24:25, :], misc[25:26, :], misc[26:27, :])
    tmp[0:24, :] = grad
    og_s[...] = tmp[...].T[0:STEPS, :].astype(BF16)
    og_r[g] = og_s[...]
    outs = []
    for k in range(1, 8):
        gt = (g + k) % 8
        outs.append(send(og_s, og_r.at[g], {"xl": gt // 4, "y": gt % 4}))
    for copy in outs:
        copy.wait_recv()

    def slopes(first, amount):
        for r in range(first, first + amount, 256):
            rows = slice(r, r + 256)
            og = og_r[r // STEPS : (r + 256) // STEPS].reshape(256, 128)
            pg1[rows, :] = (nn(og, headt[...]) * slope1[rows, :]).astype(BF16)

    slopes(0, TR)
    lo, hi = slice(0, TR // 2), slice(TR // 2, TR)

    def piece(block, rows):
        return nt(pg1[rows, :], wf1[block])

    def push(k, rows, device):
        start = 0 if rows is lo else TR // 2
        where = (k, pl.ds(start, TR // 2), slice(None))
        return send(sb.at[where], rb.at[where], device)

    where_g = (rel_g(1, 2), rel_g(1, 1), rel_g(1, 3), rel_g(0, 1), rel_g(0, 3), rel_g(0, 2), rel_g(1, 0))

    def make(k):
        for rows in (lo, hi):
            sb[k, rows, :] = piece(where_g[k], rows).astype(BF16)

    make(0)
    s1 = [push(0, lo, x_peer), push(0, hi, x_peer)]
    make(1)
    s2u = [push(1, lo, y_up), push(1, hi, y_up)]
    make(2)
    s2d = [push(2, lo, y_down), push(2, hi, y_down)]
    make(3)
    s5u = [push(3, hi, y_up)]
    make(4)
    s5d = [push(4, lo, y_down)]

    def head_rows(dst, i, block, core):
        base = pl.multiple_of((2 * block + core) * 32, 32)
        dst[i, WB:ER, 0:128] = hgp[pl.ds(base, 16), :].astype(BF16)
        dst[i, WB:ER, 128:256] = hgp[pl.ds(pl.multiple_of(base + 16, 16), 16), :].astype(BF16)
        dst[i, WB:ER, 256:512] = jnp.zeros((ER - WB, 256), BF16)

    def dw_block(i):
        return ((xh + 1 - i % 2) % 2) * 4 + (z + 2 + i // 2) % 4

    def dw_parts(layer, pg, dws, dwr, q, extra):
        base = count[0]
        count[0] += 8
        other = pl.multiple_of((1 - c) * WB, WB)

        def copy_of(i):
            return pltpu.make_async_remote_copy(
                src_ref=dws.at[i], dst_ref=dwr.at[i], send_sem=ssem.at[base + i], recv_sem=rsem.at[base + i],
                device_id=sibling, device_id_type=MESH,
            )

        def give(i, carry):
            block = dw_block(i)
            dws[i, 0:WB, :] = tn(xf[layer][block, 0:TR, pl.ds(other, WB)], pg[...]).astype(BF16)
            if extra:
                head_rows(dws, i, block, 1 - c)
            copy_of(i).start()
            return carry

        def keep(i, carry):
            block = dw_block(i)
            term = tn(xf[layer][block, 0:TR, pl.ds(cb, WB)], pg[...])
            copy_of(i).wait_recv()
            q[i, 0:WB, :] = (term + dwr[i, 0:WB, :].astype(F32)).astype(BF16)
            if extra:
                head_rows(q, i, block, c)
                q[i, WB:ER, :] = (q[i, WB:ER, :].astype(F32) + dwr[i, WB:ER, :].astype(F32)).astype(BF16)
            return carry

        return give, keep, copy_of

    def dw_run(layer, pg, dws, dwr, q, rz1, rz2, extra, size):
        give, keep, copy_of = dw_parts(layer, pg, dws, dwr, q, extra)
        lax.fori_loop(0, 4, give, 0)
        lax.fori_loop(0, 2, keep, 0)
        st = z_first(q, rz1, size)
        lax.fori_loop(4, 8, give, 0)
        lax.fori_loop(2, 4, keep, 0)
        lax.fori_loop(6, 8, keep, 0)
        z_plain(st, q, rz2, size)
        lax.fori_loop(4, 6, keep, 0)
        return st, copy_of

    def z_first(q, rz1, size):
        low, high = pl.ds(0, 128), pl.ds(128, size - 128)
        st = {}
        for xr in (0, 1):
            st["a", xr] = send(q.at[xr, low, :], rz1.at[xr, low, :], z_up)
            st["b", xr] = send(q.at[xr, high, :], rz1.at[xr, high, :], z_down)
        return st

    def z_plain(st, q, rz2, size):
        low, high = pl.ds(0, 128), pl.ds(128, size - 128)
        for xr in (0, 1):
            st["up_hi", xr] = send(q.at[6 + xr, high, :], rz2.at[xr, 0, high, :], z_up)
            st["dn_lo", xr] = send(q.at[2 + xr, low, :], rz2.at[xr, 1, low, :], z_down)

    def z_added(st, q, rz1, rz2, size):
        low, high = pl.ds(0, 128), pl.ds(128, size - 128)
        for xr in (0, 1):
            st["a", xr].wait_recv()
            q[6 + xr, 0:128, :] = (q[6 + xr, 0:128, :].astype(F32) + rz1[xr, 0:128, :].astype(F32)).astype(BF16)
            st["up_lo", xr] = send(q.at[6 + xr, low, :], rz2.at[xr, 0, low, :], z_up)
            st["b", xr].wait_recv()
            q[2 + xr, 128:size, :] = (
                q[2 + xr, 128:size, :].astype(F32) + rz1[xr, 128:size, :].astype(F32)
            ).astype(BF16)
            st["dn_hi", xr] = send(q.at[2 + xr, high, :], rz2.at[xr, 1, high, :], z_down)

    def z_sum(st, xr, q, rz2):
        for name in ("up_hi", "dn_lo", "up_lo", "dn_hi"):
            st[name, xr].wait_recv()
        return q[4 + xr].astype(F32) + rz2[xr, 0].astype(F32) + rz2[xr, 1].astype(F32)

    hgp[...] = tn(x2[0:TR, :], og_r[...].reshape(TR, 128))
    make(5)
    make(6)
    st1, copy1 = dw_run(1, pg1, dws1, dwr1, q1, rz1a, rz2a, True, ER)
    for rows in (lo, hi):
        own[rows, :] = piece(g, rows)

    def add_in(k, rows, *terms):
        value = sb[k, rows, :].astype(F32)
        for term in terms:
            value = value + rb[term, rows, :].astype(F32)
        sb[k, rows, :] = value.astype(BF16)

    s1[0].wait_recv()
    add_in(5, lo, 0)
    s4u = push(5, lo, y_up)
    s1[1].wait_recv()
    add_in(5, hi, 0)
    s4d = push(5, hi, y_down)
    z_added(st1, q1, rz1a, rz2a, ER)
    s3 = []
    for i, rows in enumerate((lo, hi)):
        s2u[i].wait_recv()
        s2d[i].wait_recv()
        add_in(6, rows, 1, 2)
        s3.append(push(6, rows, x_peer))
    s4u.wait_recv()
    add_in(3, lo, 5)
    s5u.append(push(3, lo, y_up))
    s4d.wait_recv()
    add_in(4, hi, 5)
    s5d.append(push(4, hi, y_down))

    x_near(a0)
    x_far(a0)
    blocks(0, TR, AR, 1, 8, True)
    activate(TR, AR, into_x1, None)

    xs1[...] = z_sum(st1, 0, q1, rz2a).astype(BF16)
    h1 = send(xs1, rx1, h_peer)

    for copy in s5u + s5d + s3:
        copy.wait_recv()
    for r in range(0, TR, 64):
        rows = slice(r, r + 64)
        value = own[rows, :] + rb[3, rows, :].astype(F32) + rb[4, rows, :].astype(F32) + rb[6, rows, :].astype(F32)
        pg0[rows, :] = (value * slope0[rows, :]).astype(BF16)

    a1 = x_start(1, TR, AR)
    x_own(a1, "lo")
    x_own(a1, "hi")
    st0, copy0 = dw_run(0, pg0, dws0, dwr0, q0, rz1b, rz2b, False, WB)

    x_fwd1(a1)
    x_fwd2(a1)
    value = z_sum(st1, 1, q1, rz2a)
    h1.wait_recv()
    value = value + rx1[...].astype(F32)
    dw_out[1] = value[0:WB, :]
    tmp[0:16, :] = value[WB:ER, 0:128]
    tmp[16:32, :] = value[WB:ER, 128:256]
    hg_out[...] = tmp[...].T[0 : ACT + 1, 0:32]
    z_added(st0, q0, rz1b, rz2b, WB)
    x_fwd3(a1)
    x_near(a1)
    x_far(a1)
    blocks(1, TR, AR, 1, 8, True)
    activate(TR, AR, into_x2, None)
    ha_s[...] = nt(headt[0:32, :], x2[TR : TR + AR, :])[0:24, :]
    acts = []
    for k in range(1, 8):
        gt = (g + k) % 8
        acts.append(send(ha_s, ha_r.at[g], {"xl": gt // 4, "y": gt % 4}))

    xs0[...] = z_sum(st0, 0, q0, rz2b).astype(BF16)
    h0 = send(xs0, rx0, h_peer)
    for copy in acts:
        copy.wait_recv()
    total = ha_s[...]
    for k in range(1, 8):
        total = total + ha_r[(g + 8 - k) % 8]
    al_out[...] = total[0:ACT, :]
    value = z_sum(st0, 1, q0, rz2b)
    h0.wait_recv()
    dw_out[0] = value + rx0[...].astype(F32)

    for copy in sent:
        copy.wait_send()

    def drain(i, carry):
        copy1(i).wait_send()
        copy0(i).wait_send()
        return carry

    lax.fori_loop(0, 8, drain, 0)


def per_device(observations, next_observations, trunk_weights, head_weights, acting, actions, rewards, finished):
    v = pltpu.VMEM
    dw_bufs = lambda rows: [
        v((8, rows, FB), BF16), v((8, rows, FB), BF16), v((8, rows, FB), BF16), v((2, rows, FB), BF16),
        v((2, 2, rows, FB), BF16), v((rows, FB), BF16), v((rows, FB), BF16),
    ]
    scratch = [
        v((8, TR + AR, FB), BF16), v((8, TR + AR, FB), BF16), v((8, FB, FB), BF16), v((8, FB, FB), BF16),
        v((TR + AR, FB), F32), v((TR, FB), F32), v((TR, FB), F32), v((TR + AR, FB), BF16),
        v((128, FB), BF16), v((128, 128), F32), v((32, 128), F32),
        v((8, 24, 128), F32), v((8, 24, 128), F32), v((24, 128), F32), v((8, 24, 128), F32),
        v((STEPS, 128), BF16), v((8, STEPS, 128), BF16), v((TR, FB), BF16), v((TR, FB), BF16), v((FB, 128), F32),
        v((7, TR, FB), BF16), v((7, TR, FB), BF16), v((TR, FB), F32),
        *dw_bufs(ER), *dw_bufs(WB),
        pltpu.SemaphoreType.DMA((N_SEM,)), pltpu.SemaphoreType.DMA((N_SEM,)), pltpu.SemaphoreType.DMA((4,)),
    ]
    hbm = pl.BlockSpec(memory_space=pltpu.HBM)
    vmem = pl.BlockSpec(memory_space=pltpu.VMEM)
    trunk_grads, head_grads, actor_logits = pl.pallas_call(
        kernel,
        out_shape=(
            jax.ShapeDtypeStruct((2, WB, FB), F32),
            jax.ShapeDtypeStruct((ACT + 1, 32), F32),
            jax.ShapeDtypeStruct((ACT, AR), F32),
        ),
        in_specs=[hbm, hbm, hbm, vmem, vmem, vmem, vmem, vmem],
        out_specs=(vmem, vmem, vmem),
        scratch_shapes=scratch,
        compiler_params=pltpu.CompilerParams(
            collective_id=0, has_side_effects=True, vmem_limit_bytes=62 * 1024 * 1024
        ),
        name="learner_step",
    )(
        observations.reshape(TR, FB), next_observations, trunk_weights, head_weights.T, acting.transpose(2, 0, 1),
        actions, rewards, finished,
    )
    return trunk_grads, head_grads.T, actor_logits.T


def solution(mesh):
    split = Mesh(mesh.devices.reshape(SIZES), AXES)
    return jax.shard_map(
        per_device,
        mesh=split,
        in_specs=(
            P(DP, None, GROUP),
            P(DP, GROUP),
            P(None, DP, GROUP),
            P(GROUP, None),
            P(DP, None, None),
            P(DP, None),
            P(DP, None),
            P(DP, None),
        ),
        out_specs=(P(None, DP, GROUP), P(GROUP + DP, None), P(DP, None)),
        check_vma=False,
    )
```

```python
import functools

import jax
import jax.numpy as jnp
from jax import lax
from jax.experimental import pallas as pl
from jax.experimental.pallas import tpu as pltpu
from jax.sharding import Mesh
from jax.sharding import PartitionSpec as P

AXES = ("xl", "y", "xh", "z", "c")
SIZES = (2, 4, 2, 4, 2)
DP = ("xh", "z", "c")
GROUP = ("xl", "y")
MESH = pl.DeviceIdType.MESH
F32 = jnp.float32
BF16 = jnp.bfloat16

discount_rate = 0.99
value_weight = 0.5
entropy_weight = 0.1
loss_divisor = 16.0

TR = 512
AR = 128
FB = 512
WB = 256
STEPS = 64
ACT = 18
ER = 544
N_RECV, N_SEND = 148, 21
CH = 256


def nn(a, b):
    return jnp.dot(a, b, preferred_element_type=F32)


def nt(a, b):
    return lax.dot_general(a, b, (((1,), (1,)), ((), ())), preferred_element_type=F32)


def tn(a, b):
    return lax.dot_general(a, b, (((0,), (0,)), ((), ())), preferred_element_type=F32)


def vtrace(logits, behave, action, reward, finished):
    row = lax.broadcasted_iota(jnp.int32, logits.shape, 0)
    step = lax.broadcasted_iota(jnp.int32, reward.shape, 1)
    live = step % STEPS < STEPS - 1
    lanes = reward.shape[1]
    is_act = row < ACT

    def log_softmax(values):
        top = jnp.max(jnp.where(is_act, values, -3.0e38), axis=0, keepdims=True)
        shifted = jnp.where(is_act, values - top, 0.0)
        total = jnp.sum(jnp.where(is_act, jnp.exp(shifted), 0.0), axis=0, keepdims=True)
        return jnp.where(is_act, shifted - jnp.log(total), 0.0)

    log_policy = log_softmax(logits)
    log_behave = log_softmax(behave)
    chosen = jnp.where(row.astype(F32) == action, 1.0, 0.0)
    ratio = jnp.exp(jnp.sum((log_policy - log_behave) * chosen, axis=0, keepdims=True))
    clipped = jnp.minimum(ratio, 1.0)
    discount = discount_rate * (1.0 - finished)
    current = logits[ACT : ACT + 1, :]
    following = pltpu.roll(current, lanes - 1, 1)
    delta = jnp.where(live, clipped * (reward + discount * following - current), 0.0)
    factor = jnp.where(live, discount * clipped, 0.0)
    for shift in (1, 2, 4, 8, 16, 32):
        delta = delta + factor * pltpu.roll(delta, lanes - shift, 1)
        factor = factor * pltpu.roll(factor, lanes - shift, 1)
    targets = current + delta
    next_targets = pltpu.roll(targets, lanes - 1, 1)
    advantage = clipped * (reward + discount * next_targets - current)
    probability = jnp.where(is_act, jnp.exp(log_policy), 0.0)
    entropy = -jnp.sum(probability * log_policy, axis=0, keepdims=True)
    logit_grad = (
        -advantage * (chosen - probability)
        + entropy_weight * probability * (log_policy + entropy)
    ) / loss_divisor
    value_grad = -value_weight * (targets - current) / loss_divisor
    grad = jnp.where(is_act, logit_grad, jnp.where(row == ACT, value_grad, 0.0))
    return jnp.where(live, grad, 0.0)


def kernel(
    obs, nxt, wts, head, acting, actions, rewards, finished,
    dw_out, hg_out, al_out,
    xf0, xf1, wf0, wf1, acc, slope0, slope1, x2, headt, tmp, misc,
    hs, hr, ha_s, ha_r, og_r, pg1, pg1t, pg0t, hgp,
    sb, rb, own,
    dws1, dwr1, q1, rz1a, rz2a, xs1, rx1,
    dws0, dwr0, q0, rz1b, rz2b, xs0, rx0, rxx,
    ssem, rsem, lsem,
):
    xl, y, xh, z, c = (lax.axis_index(a) for a in AXES)
    g = xl * 4 + y
    xf, wf = (xf0, xf1), (wf0, wf1)

    def rel_g(dx, dy):
        return ((xl + dx) % 2) * 4 + (y + dy) % 4

    def rel_w(dx, dz):
        return ((xh + dx) % 2) * 4 + (z + dz) % 4

    x_peer = {"xl": 1 - xl}
    y_up, y_down = {"y": (y + 1) % 4}, {"y": (y + 3) % 4}
    h_peer = {"xh": 1 - xh}
    z_up, z_down = {"z": (z + 1) % 4}, {"z": (z + 3) % 4}
    sibling = {"c": 1 - c}

    count = [0, 0]
    sends = []

    def new_recv():
        count[0] += 1
        return rsem.at[count[0] - 1]

    def new_send(view):
        count[1] += 1
        sem = ssem.at[count[1] - 1]
        sends.append((view, sem))
        return sem

    class Recv:
        def __init__(self, sem, view):
            self.sem, self.view = sem, view

        def wait_recv(self):
            pltpu.make_async_remote_copy(
                src_ref=self.view, dst_ref=self.view, send_sem=ssem.at[0], recv_sem=self.sem,
                device_id=x_peer, device_id_type=MESH,
            ).wait_recv()

    def send(src, dst, device, send_sem, recv_sem=None):
        copy = pltpu.make_async_remote_copy(
            src_ref=src, dst_ref=dst, send_sem=send_sem, recv_sem=new_recv() if recv_sem is None else recv_sem,
            device_id=device, device_id_type=MESH,
        )
        copy.start()
        return copy

    cb = pl.multiple_of(c * WB, WB)
    wg = xh * 4 + z
    loads = [
        pltpu.make_async_copy(obs, xf0.at[g, pl.ds(0, TR), :], lsem.at[0]),
        pltpu.make_async_copy(wts.at[0], wf0.at[wg, pl.ds(cb, WB), :], lsem.at[1]),
        pltpu.make_async_copy(wts.at[1], wf1.at[wg, pl.ds(cb, WB), :], lsem.at[2]),
        pltpu.make_async_copy(nxt, xf0.at[g, pl.ds(TR, AR), :], lsem.at[3]),
    ]
    for load in loads:
        load.start()

    barrier = pltpu.get_barrier_semaphore()
    friends = [h_peer, z_up, z_down, sibling]
    for k in range(1, 8):
        gt = (g + k) % 8
        friends.append({"xl": gt // 4, "y": gt % 4})
    for friend in friends:
        pl.semaphore_signal(barrier, inc=1, device_id=friend, device_id_type=MESH)
    pl.semaphore_wait(barrier, len(friends))

    def x_start(layer, first, amount):
        buf, half = xf[layer], amount // 2
        lo, hi = pl.ds(first, half), pl.ds(first + half, half)

        out = new_send(buf.at[pl.ds(0, 7), pl.ds(0, amount), :])

        def go(block, rows, device, recv_sem=None):
            return send(buf.at[block, rows, :], buf.at[block, rows, :], device, out, recv_sem)

        near = Recv(new_recv(), buf.at[0, pl.ds(0, amount), :])
        far = Recv(new_recv(), buf.at[pl.ds(0, 3), pl.ds(0, amount), :])
        return {"go": go, "lo": lo, "hi": hi, "near": near, "far": far}

    def x_own(st, rows):
        go, lo = st["go"], st["lo"]
        if rows == "lo":
            st["up_lo"] = go(g, lo, y_up)
            st["x_lo"] = go(g, lo, x_peer)
        else:
            st["dn_hi"] = go(g, st["hi"], y_down)
            st["x_hi"] = go(g, st["hi"], x_peer)
            go(g, st["hi"], y_up, st["near"].sem)
            go(g, lo, y_down, st["near"].sem)

    def x_fwd1(st):
        go = st["go"]
        st["up_lo"].wait_recv()
        st["f_lo"] = go(rel_g(0, 3), st["lo"], y_up)
        st["dn_hi"].wait_recv()
        st["f_hi"] = go(rel_g(0, 1), st["hi"], y_down)

    def x_fwd2(st):
        go, block, far = st["go"], rel_g(1, 0), st["far"].sem
        st["x_lo"].wait_recv()
        go(block, st["lo"], y_up, far)
        go(block, st["lo"], y_down, far)
        st["x_hi"].wait_recv()
        go(block, st["hi"], y_up, far)
        go(block, st["hi"], y_down, far)

    def x_fwd3(st):
        go, block, far = st["go"], rel_g(0, 2), st["far"].sem
        st["f_lo"].wait_recv()
        go(block, st["lo"], x_peer, far)
        st["f_hi"].wait_recv()
        go(block, st["hi"], x_peer, far)

    def x_near(st):
        st["near"].wait_recv()

    def x_far(st):
        st["far"].wait_recv()

    half_w = WB // 2

    def w_piece(block, part):
        if part == "all":
            return (block, pl.ds(cb, WB), slice(None))
        start = cb if part == "lo" else cb + half_w
        return (block, pl.ds(pl.multiple_of(start, half_w), half_w), slice(None))

    def w_start(layer):
        buf = wf[layer]

        out = new_send(xf[layer].at[pl.ds(0, 6), :, :])

        def go(block, part, device, recv_sem=None):
            where = w_piece(block, part)
            return send(buf.at[where], buf.at[where], device, out, recv_sem)

        st = {"go": go}
        st["f"] = Recv(new_recv(), buf.at[0, pl.ds(0, WB), :])
        st["g"] = Recv(new_recv(), buf.at[0, pl.ds(0, WB), :])
        st["sib"] = Recv(new_recv(), buf.at[pl.ds(0, 4), :, :])
        st["up_lo"] = go(wg, "lo", z_up)
        st["dn_hi"] = go(wg, "hi", z_down)
        st["h"] = go(wg, "all", h_peer)
        st["up_hi"] = go(wg, "hi", z_up)
        st["dn_lo"] = go(wg, "lo", z_down)
        w_share(st, wg)
        return st

    def w_share(st, block):
        st["go"](block, "all", sibling, st["sib"].sem)

    def w_fwd1(st):
        go = st["go"]
        st["up_lo"].wait_recv()
        go(rel_w(0, 3), "lo", z_up, st["f"].sem)
        st["dn_hi"].wait_recv()
        go(rel_w(0, 1), "hi", z_down, st["f"].sem)

    def w_fwd2(st):
        go, far = st["go"], rel_w(1, 0)
        st["h"].wait_recv()
        st["h_up_lo"] = go(far, "lo", z_up)
        st["h_dn_hi"] = go(far, "hi", z_down)
        st["h_up_hi"] = go(far, "hi", z_up)
        st["h_dn_lo"] = go(far, "lo", z_down)
        w_share(st, far)
        st["up_hi"].wait_recv()
        w_share(st, rel_w(0, 3))
        st["dn_lo"].wait_recv()
        w_share(st, rel_w(0, 1))

    def w_fwd3(st):
        go = st["go"]
        st["h_up_lo"].wait_recv()
        go(rel_w(1, 3), "lo", z_up, st["g"].sem)
        st["h_dn_hi"].wait_recv()
        go(rel_w(1, 1), "hi", z_down, st["g"].sem)
        st["f"].wait_recv()
        w_share(st, rel_w(0, 2))

    def w_finish(st):
        st["h_up_hi"].wait_recv()
        w_share(st, rel_w(1, 3))
        st["h_dn_lo"].wait_recv()
        w_share(st, rel_w(1, 1))
        st["g"].wait_recv()
        w_share(st, rel_w(1, 2))
        st["sib"].wait_recv()

    def blocks(layer, first, amount, j0, j1, fresh):
        buf, weights = xf[layer], wf[layer]
        rows = slice(first, first + amount)
        if fresh:
            acc[rows, :] = nn(buf[g, rows, :], weights[g])

        def body(j, carry):
            block = ((xl + j // 4) % 2) * 4 + (y + j % 4) % 4
            acc[rows, :] += nn(buf[block, rows, :], weights[block])
            return carry

        lax.fori_loop(j0, j1, body, 0)

    def activate(first, amount, out, slope, tile=64):
        def body(i, carry):
            rows = pl.ds(pl.multiple_of(first + i * tile, tile), tile)
            value = acc[rows, :]
            sigma = jax.nn.sigmoid(value)
            out(rows, (value * sigma).astype(BF16))
            if slope is not None:
                slope[rows, :] = sigma * (1.0 + value * (1.0 - sigma))
            return carry

        lax.fori_loop(0, amount // tile, body, 0)

    def into_x1(rows, value):
        xf1[g, rows, :] = value

    def into_x2(rows, value):
        x2[rows, :] = value

    def next_layer(first, slope):
        st = x_start(1, first, CH)
        activate(first, CH // 2, into_x1, slope)
        x_own(st, "lo")
        activate(first + CH // 2, CH // 2, into_x1, slope)
        x_own(st, "hi")
        return st

    def to_group(src, dst, landed):
        out, got = new_send(landed), new_recv()
        for k in range(1, 8):
            gt = (g + k) % 8
            send(src, dst.at[g], {"xl": gt // 4, "y": gt % 4}, out, got)
        return Recv(got, landed)

    def from_group(own_part, dst):
        total = own_part[...]
        for k in range(1, 8):
            total = total + dst[(g + 8 - k) % 8]
        return total

    def head_send(ch):
        hs[ch] = nt(headt[0:32, :], x2[CH * ch : CH * (ch + 1), :])[0:24, :]
        return to_group(hs.at[ch], hr.at[ch], hr.at[ch, pl.ds(0, 7), :, :])

    def head_loss(ch, got):
        got.wait_recv()
        total = from_group(hs.at[ch], hr.at[ch])
        grad = vtrace(total, misc[ch, 0:24, :], misc[ch, 24:25, :], misc[ch, 25:26, :], misc[ch, 26:27, :])
        tmp[0:24, :] = grad
        rows = slice(CH * ch, CH * (ch + 1))
        og_r[rows, :] = tmp[...].T.astype(BF16)
        pg1[rows, :] = (nn(og_r[rows, :], headt[...]) * slope1[rows, :]).astype(BF16)
        pg1t[:, rows] = pg1[rows, :].T

    where_g = (rel_g(1, 2), rel_g(1, 1), rel_g(1, 3), rel_g(0, 1), rel_g(0, 3), rel_g(0, 2), rel_g(1, 0))

    class Scatter:
        def __init__(self, first, amount, col, cols):
            half = amount // 2
            self.rows = slice(first, first + amount)
            self.lo, self.hi = slice(first, first + half), slice(first + half, first + amount)
            self.cs = slice(col, col + cols)
            self.out = new_send(sb.at[:, self.ds(self.rows), self.ds(self.cs)])
            self.s2 = [Recv(new_recv(), rb.at[pl.ds(0, 2), self.ds(rows), self.ds(self.cs)]) for rows in (self.lo, self.hi)]
            self.last = Recv(new_recv(), rb.at[pl.ds(0, 3), self.ds(self.rows), self.ds(self.cs)])

        def ds(self, rows):
            return pl.ds(rows.start, rows.stop - rows.start)

        def piece(self, block):
            return nt(pg1[self.rows, :], wf1[block, self.cs, :])

        def make(self, k):
            sb[k, self.rows, self.cs] = self.piece(where_g[k]).astype(BF16)

        def push(self, k, rows, device, recv_sem=None):
            where = (k, self.ds(rows), self.ds(self.cs))
            return send(sb.at[where], rb.at[where], device, self.out, recv_sem)

        def add_in(self, k, rows, *terms):
            value = sb[k, rows, self.cs].astype(F32)
            for term in terms:
                value = value + rb[term, rows, self.cs].astype(F32)
            sb[k, rows, self.cs] = value.astype(BF16)

        def make_all(self):
            self.make(0)
            self.s1 = [self.push(0, self.lo, x_peer), self.push(0, self.hi, x_peer)]
            for k in range(1, 7):
                self.make(k)
            own[self.rows, self.cs] = self.piece(g)

        def push_y(self):
            for i, rows in enumerate((self.lo, self.hi)):
                self.push(1, rows, y_up, self.s2[i].sem)
                self.push(2, rows, y_down, self.s2[i].sem)
            self.push(3, self.hi, y_up, self.last.sem)
            self.push(4, self.lo, y_down, self.last.sem)

        def mid1(self):
            self.s1[0].wait_recv()
            self.add_in(5, self.lo, 0)
            self.s4u = self.push(5, self.lo, y_up)
            self.s1[1].wait_recv()
            self.add_in(5, self.hi, 0)
            self.s4d = self.push(5, self.hi, y_down)

        def mid2(self):
            for i, rows in enumerate((self.lo, self.hi)):
                self.s2[i].wait_recv()
                self.add_in(6, rows, 1, 2)
                self.push(6, rows, x_peer, self.last.sem)

        def mid3(self):
            self.s4u.wait_recv()
            self.add_in(3, self.lo, 5)
            self.push(3, self.lo, y_up, self.last.sem)
            self.s4d.wait_recv()
            self.add_in(4, self.hi, 5)
            self.push(4, self.hi, y_down, self.last.sem)

        def close(self):
            self.last.wait_recv()
            cs = self.cs
            for r in range(self.rows.start, self.rows.stop, 128):
                rows = slice(r, r + 128)
                value = own[rows, cs] + rb[3, rows, cs].astype(F32) + rb[4, rows, cs].astype(F32) + rb[6, rows, cs].astype(F32)
                pg0t[cs, rows] = (value * slope0[rows, cs]).astype(BF16).T

    class Weights:
        def __init__(self, layer, pgt, bufs, col, cols, extra, halves=(0, 1)):
            self.halves = halves
            self.layer, self.pgt, self.extra = layer, pgt, extra
            self.dws, self.dwr, self.q, self.rz1, self.rz2, self.xs, self.rx = bufs
            self.cols, self.size = cols, cols + extra
            self.cs, self.top = slice(col, col + cols), slice(col + cols, col + cols + extra)
            self.all, half = slice(col, col + self.size), col + cols // 2
            self.low, self.high = slice(col, half), slice(half, col + self.size)
            self.base = count[0]
            count[0] += 8
            every = self.ds(self.all)
            self.out = new_send(self.q.at[pl.ds(0, 7), every, :])
            self.give_sem = new_send(self.dws.at[:, every, :])
            self.sums = {xr: Recv(new_recv(), self.rz2.at[xr, :, every, :]) for xr in halves}
            self.st = {}

        def ds(self, rows):
            return pl.ds(rows.start, rows.stop - rows.start)

        def block(self, i):
            return ((xh + 1 - i % 2) % 2) * 4 + (z + 2 + i // 2) % 4

        def copy_of(self, i):
            every = self.ds(self.all)
            return pltpu.make_async_remote_copy(
                src_ref=self.dws.at[i, every, :], dst_ref=self.dwr.at[i, every, :],
                send_sem=self.give_sem, recv_sem=rsem.at[self.base + i],
                device_id=sibling, device_id_type=MESH,
            )

        def head_rows(self, block, core):
            return hgp[pl.ds(pl.multiple_of((2 * block + core) * 32, 32), 32), :]

        def give(self, i0, i1):
            other = pl.multiple_of((1 - c) * WB, WB)

            def body(i, carry):
                block = self.block(i)
                term = nn(self.pgt[self.cs, :], xf[self.layer][block, 0:TR, pl.ds(other, WB)])
                self.dws[i, self.cs, :] = term.astype(BF16)
                if self.extra:
                    self.dws[i, self.top, 0:128] = self.head_rows(block, 1 - c).astype(BF16)
                    self.dws[i, self.top, 128:256] = jnp.zeros((self.extra, 128), BF16)
                self.copy_of(i).start()
                return carry

            lax.fori_loop(i0, i1, body, 0)

        def keep(self, i0, i1):
            q, dwr, cs, top = self.q, self.dwr, self.cs, self.top

            def body(i, carry):
                block = self.block(i)
                term = nn(self.pgt[cs, :], xf[self.layer][block, 0:TR, pl.ds(cb, WB)])
                self.copy_of(i).wait_recv()
                q[i, cs, :] = (term + dwr[i, cs, :].astype(F32)).astype(BF16)
                if self.extra:
                    q[i, top, 0:128] = (self.head_rows(block, c) + dwr[i, top, 0:128].astype(F32)).astype(BF16)
                    q[i, top, 128:256] = jnp.zeros((self.extra, 128), BF16)
                return carry

            lax.fori_loop(i0, i1, body, 0)

        def go(self, i, rows, dst, device, recv_sem=None):
            where = self.ds(rows)
            return send(self.q.at[i, where, :], dst.at[where, :], device, self.out, recv_sem)

        def z_first(self):
            for xr in self.halves:
                self.st["a", xr] = self.go(xr, self.low, self.rz1.at[xr], z_up)
                self.st["b", xr] = self.go(xr, self.high, self.rz1.at[xr], z_down)

        def z_plain(self):
            for xr in self.halves:
                self.go(6 + xr, self.high, self.rz2.at[xr, 0], z_up, self.sums[xr].sem)
                self.go(2 + xr, self.low, self.rz2.at[xr, 1], z_down, self.sums[xr].sem)

        def early(self):
            self.give(0, 4)
            self.keep(0, 2)
            self.z_first()
            self.give(4, 8)

        def late(self):
            self.keep(2, 4)
            self.keep(6, 8)
            self.z_plain()
            self.keep(4, 6)

        def z_added(self):
            q, rz1, st = self.q, self.rz1, self.st
            for xr in self.halves:
                for name, i, rows, side, device in (("a", 6, self.low, 0, z_up), ("b", 2, self.high, 1, z_down)):
                    st[name, xr].wait_recv()
                    value = q[i + xr, rows, :].astype(F32) + rz1[xr, rows, :].astype(F32)
                    q[i + xr, rows, :] = value.astype(BF16)
                    self.go(i + xr, rows, self.rz2.at[xr, side], device, self.sums[xr].sem)

        def z_sum(self, xr):
            self.sums[xr].wait_recv()
            every = self.all
            return (
                self.q[4 + xr, every, :].astype(F32)
                + self.rz2[xr, 0, every, :].astype(F32)
                + self.rz2[xr, 1, every, :].astype(F32)
            )

        def cross(self):
            every = self.ds(self.all)
            self.xs[self.all, :] = self.z_sum(0).astype(BF16)
            self.h = send(self.xs.at[every, :], self.rx.at[every, :], h_peer, self.out)

        def x_open(self):
            self.give(0, 4)
            self.keep(0, 2)
            self.x_push(0)
            self.keep(2, 4)
            self.x_push(2)
            self.give(4, 8)
            self.keep(6, 8)
            self.x_push(6)
            self.keep(4, 6)
            self.x_push(4)

        def x_push(self, i):
            every = self.ds(self.all)
            self.st["x", i] = send(self.q.at[i, every, :], rxx.at[i // 2], h_peer, self.out)

        def x_take(self, i):
            self.st["x", i].wait_recv()
            value = self.q[i + 1, self.all, :].astype(F32) + rxx[i // 2].astype(F32)
            self.q[i + 1, self.all, :] = value.astype(BF16)

        def result(self):
            value = self.z_sum(1)
            if 0 in self.halves:
                self.h.wait_recv()
                value = value + self.rx[self.all, :].astype(F32)
            dw_out[self.layer, :, self.cs] = value[0 : self.cols, :].T
            if self.extra:
                hg_out[...] = value[self.cols :, 0:128].T[0 : ACT + 1, :]

    loads[0].wait()
    loads[1].wait()
    w0 = w_start(0)
    a0, b0 = x_start(0, 0, CH), x_start(0, CH, CH)
    x_own(a0, "lo")
    x_own(a0, "hi")
    x_own(b0, "lo")
    x_own(b0, "hi")
    loads[2].wait()
    loads[3].wait()

    headt[...] = jnp.zeros_like(headt)
    headt[0 : ACT + 1, :] = head[...]
    misc[...] = jnp.zeros_like(misc)
    for r in range(8):
        ch, lane = r // 4, STEPS * (r % 4)
        steps = slice(lane, lane + STEPS - 1)
        misc[ch, 0:ACT, steps] = acting[:, r, :]
        misc[ch, 24:25, steps] = actions[r : r + 1, :].astype(F32)
        misc[ch, 25:26, steps] = rewards[r : r + 1, :]
        misc[ch, 26:27, steps] = finished[r : r + 1, :].astype(F32)
    tmp[...] = jnp.zeros_like(tmp)

    w_fwd1(w0)
    x_fwd1(a0)
    w_fwd2(w0)
    x_fwd1(b0)
    x_fwd2(a0)
    w_fwd3(w0)
    x_fwd3(a0)
    x_fwd2(b0)
    x_fwd3(b0)
    w1 = w_start(1)
    w_finish(w0)
    x_near(a0)
    blocks(0, 0, CH, 1, 5, True)
    x_far(a0)
    blocks(0, 0, CH, 5, 8, False)
    a1 = next_layer(0, slope0)
    w_fwd1(w1)
    x_near(b0)
    blocks(0, CH, CH, 1, 5, True)
    x_far(b0)
    blocks(0, CH, CH, 5, 8, False)
    b1 = next_layer(CH, slope0)

    x_fwd1(a1)
    w_fwd2(w1)
    x_fwd1(b1)
    x_fwd2(a1)
    w_fwd3(w1)
    x_fwd3(a1)
    x_fwd3(b1)
    x_fwd2(b1)
    w_finish(w1)
    x_near(a1)
    blocks(1, 0, CH, 1, 5, True)
    x_far(a1)
    blocks(1, 0, CH, 5, 8, False)
    activate(0, CH, into_x2, slope1)
    head_a = head_send(0)
    c0 = x_start(0, TR, AR)
    x_own(c0, "lo")
    x_own(c0, "hi")
    x_near(b1)
    blocks(1, CH, CH, 1, 5, True)
    x_far(b1)
    blocks(1, CH, CH, 5, 8, False)
    activate(CH, CH, into_x2, slope1)
    head_b = head_send(1)
    x_fwd1(c0)
    x_fwd2(c0)

    da1, da2 = Scatter(0, CH, 0, CH), Scatter(0, CH, CH, CH)
    db1, db2 = Scatter(CH, CH, 0, CH), Scatter(CH, CH, CH, CH)
    g1 = Weights(1, pg1t, (dws1, dwr1, q1, rz1a, rz2a, xs1, rx1), 0, FB, ER - FB)
    bufs0 = (dws0, dwr0, q0, rz1b, rz2b, xs0, rx0)
    g0a = Weights(0, pg0t, bufs0, 0, CH, 0)
    g0b = Weights(0, pg0t, bufs0, CH, CH, 0)
    head_loss(0, head_a)
    da1.make_all()
    da1.push_y()
    da2.make_all()
    da2.push_y()
    head_loss(1, head_b)
    db1.make_all()
    db1.push_y()
    da1.mid1()
    hgp[...] = tn(x2[0:TR, :], og_r[...])
    g1.give(0, 4)
    g1.keep(0, 2)
    g1.z_first()
    da1.mid2()
    db1.mid1()
    x_fwd3(c0)
    da2.mid1()
    db2.make_all()
    db2.push_y()
    da1.mid3()
    db1.mid2()
    g1.give(4, 8)
    da2.mid2()
    g1.keep(2, 4)
    db1.mid3()
    db2.mid1()
    g1.keep(6, 8)
    g1.z_plain()
    da2.mid3()
    g1.keep(4, 6)
    db2.mid2()
    g1.z_added()
    da1.close()
    x_near(c0)
    x_far(c0)
    blocks(0, TR, AR, 1, 8, True)
    activate(TR, AR, into_x1, None)
    db1.close()
    g0a.give(0, 4)
    db2.mid3()
    c1 = x_start(1, TR, AR)
    x_own(c1, "lo")
    x_own(c1, "hi")
    g0a.keep(0, 2)
    g0a.z_first()
    g0a.give(4, 8)
    g0a.late()
    da2.close()
    x_fwd1(c1)
    x_fwd2(c1)
    db2.close()
    g0b.early()
    g0a.z_added()
    x_fwd3(c1)
    g0b.late()
    g1.cross()
    x_near(c1)
    x_far(c1)
    blocks(1, TR, AR, 1, 8, True)
    activate(TR, AR, into_x2, None)
    ha_s[...] = nt(headt[0:32, :], x2[TR : TR + AR, :])[0:24, :]
    acts = to_group(ha_s, ha_r, ha_r.at[pl.ds(0, 7), :, :])
    g0a.cross()
    g0b.z_added()
    g1.result()
    acts.wait_recv()
    al_out[...] = from_group(ha_s, ha_r)[0:ACT, :]
    g0b.cross()
    g0a.result()
    g0b.result()

    for view, sem in sends:
        pltpu.make_async_remote_copy(
            src_ref=view, dst_ref=view, send_sem=sem, recv_sem=rsem.at[0], device_id=x_peer, device_id_type=MESH,
        ).wait_send()
    assert (count[0], count[1]) == (N_RECV, N_SEND), count


def per_device(observations, next_observations, trunk_weights, head_weights, acting, actions, rewards, finished):
    v = pltpu.VMEM
    dw_bufs = lambda rows: [
        v((8, rows, WB), BF16), v((8, rows, WB), BF16), v((8, rows, WB), BF16), v((2, rows, WB), BF16),
        v((2, 2, rows, WB), BF16), v((rows, WB), BF16), v((rows, WB), BF16),
    ]
    scratch = [
        v((8, TR + AR, FB), BF16), v((8, TR + AR, FB), BF16), v((8, FB, FB), BF16), v((8, FB, FB), BF16),
        v((TR + AR, FB), F32), v((TR, FB), F32), v((TR, FB), F32), v((TR + AR, FB), BF16),
        v((128, FB), BF16), v((128, CH), F32), v((2, 32, CH), F32),
        v((2, 24, CH), F32), v((2, 8, 24, CH), F32), v((24, 128), F32), v((8, 24, 128), F32),
        v((TR, 128), BF16), v((TR, FB), BF16), v((FB, TR), BF16), v((FB, TR), BF16), v((FB, 128), F32),
        v((7, TR, FB), BF16), v((7, TR, FB), BF16), v((TR, FB), F32),
        *dw_bufs(ER), *dw_bufs(FB), v((4, CH, WB), BF16),
        pltpu.SemaphoreType.DMA((N_SEND,)), pltpu.SemaphoreType.DMA((N_RECV,)), pltpu.SemaphoreType.DMA((4,)),
    ]
    hbm = pl.BlockSpec(memory_space=pltpu.HBM)
    vmem = pl.BlockSpec(memory_space=pltpu.VMEM)
    trunk_grads, head_grads, actor_logits = pl.pallas_call(
        kernel,
        out_shape=(
            jax.ShapeDtypeStruct((2, WB, FB), F32),
            jax.ShapeDtypeStruct((ACT + 1, 32), F32),
            jax.ShapeDtypeStruct((ACT, AR), F32),
        ),
        in_specs=[hbm, hbm, hbm, vmem, vmem, vmem, vmem, vmem],
        out_specs=(vmem, vmem, vmem),
        scratch_shapes=scratch,
        compiler_params=pltpu.CompilerParams(
            collective_id=0, has_side_effects=True, vmem_limit_bytes=62 * 1024 * 1024
        ),
        name="learner_step",
    )(
        observations.reshape(TR, FB), next_observations, trunk_weights, head_weights.T, acting.transpose(2, 0, 1),
        actions, rewards, finished,
    )
    return trunk_grads, head_grads.T, actor_logits.T


def solution(mesh):
    split = Mesh(mesh.devices.reshape(SIZES), AXES)
    return jax.shard_map(
        per_device,
        mesh=split,
        in_specs=(
            P(DP, None, GROUP),
            P(DP, GROUP),
            P(None, DP, GROUP),
            P(GROUP, None),
            P(DP, None, None),
            P(DP, None),
            P(DP, None),
            P(DP, None),
        ),
        out_specs=(P(None, DP, GROUP), P(GROUP + DP, None), P(DP, None)),
        check_vma=False,
    )
```

```python
import functools

import jax
import jax.numpy as jnp
from jax import lax
from jax.experimental import pallas as pl
from jax.experimental.pallas import tpu as pltpu
from jax.sharding import Mesh
from jax.sharding import PartitionSpec as P

AXES = ("xl", "y", "xh", "z", "c")
SIZES = (2, 4, 2, 4, 2)
DP = ("xh", "z", "c")
GROUP = ("xl", "y")
MESH = pl.DeviceIdType.MESH
F32 = jnp.float32
BF16 = jnp.bfloat16

discount_rate = 0.99
value_weight = 0.5
entropy_weight = 0.1
loss_divisor = 16.0

TR = 512
AR = 128
FB = 512
WB = 256
STEPS = 64
ACT = 18
ER = 544
N_RECV, N_SEND = 148, 21
CH = 256


def nn(a, b):
    return jnp.dot(a, b, preferred_element_type=F32)


def nt(a, b):
    return lax.dot_general(a, b, (((1,), (1,)), ((), ())), preferred_element_type=F32)


def tn(a, b):
    return lax.dot_general(a, b, (((0,), (0,)), ((), ())), preferred_element_type=F32)


def vtrace(logits, behave, action, reward, finished):
    row = lax.broadcasted_iota(jnp.int32, logits.shape, 0)
    step = lax.broadcasted_iota(jnp.int32, reward.shape, 1)
    live = step % STEPS < STEPS - 1
    lanes = reward.shape[1]
    is_act = row < ACT

    def log_softmax(values):
        top = jnp.max(jnp.where(is_act, values, -3.0e38), axis=0, keepdims=True)
        shifted = jnp.where(is_act, values - top, 0.0)
        total = jnp.sum(jnp.where(is_act, jnp.exp(shifted), 0.0), axis=0, keepdims=True)
        return jnp.where(is_act, shifted - jnp.log(total), 0.0)

    log_policy = log_softmax(logits)
    log_behave = log_softmax(behave)
    chosen = jnp.where(row.astype(F32) == action, 1.0, 0.0)
    ratio = jnp.exp(jnp.sum((log_policy - log_behave) * chosen, axis=0, keepdims=True))
    clipped = jnp.minimum(ratio, 1.0)
    discount = discount_rate * (1.0 - finished)
    current = logits[ACT : ACT + 1, :]
    following = pltpu.roll(current, lanes - 1, 1)
    delta = jnp.where(live, clipped * (reward + discount * following - current), 0.0)
    factor = jnp.where(live, discount * clipped, 0.0)
    for shift in (1, 2, 4, 8, 16, 32):
        delta = delta + factor * pltpu.roll(delta, lanes - shift, 1)
        factor = factor * pltpu.roll(factor, lanes - shift, 1)
    targets = current + delta
    next_targets = pltpu.roll(targets, lanes - 1, 1)
    advantage = clipped * (reward + discount * next_targets - current)
    probability = jnp.where(is_act, jnp.exp(log_policy), 0.0)
    entropy = -jnp.sum(probability * log_policy, axis=0, keepdims=True)
    logit_grad = (
        -advantage * (chosen - probability)
        + entropy_weight * probability * (log_policy + entropy)
    ) / loss_divisor
    value_grad = -value_weight * (targets - current) / loss_divisor
    grad = jnp.where(is_act, logit_grad, jnp.where(row == ACT, value_grad, 0.0))
    return jnp.where(live, grad, 0.0)


def kernel(
    obs, nxt, wts, head, acting, actions, rewards, finished,
    dw_out, hg_out, al_out,
    xf0, xf1, wf0, wf1, acc, slope0, slope1, x2, headt, tmp, misc,
    hs, hr, ha_s, ha_r, og_r, pg1, pg1t, pg0t, hgp,
    sb, rb, own,
    dws1, dwr1, q1, rz1a, rz2a, xs1, rx1,
    dws0, dwr0, q0, rz1b, rz2b, xs0, rx0,
    ssem, rsem, lsem,
):
    xl, y, xh, z, c = (lax.axis_index(a) for a in AXES)
    g = xl * 4 + y
    xf, wf = (xf0, xf1), (wf0, wf1)

    def rel_g(dx, dy):
        return ((xl + dx) % 2) * 4 + (y + dy) % 4

    def rel_w(dx, dz):
        return ((xh + dx) % 2) * 4 + (z + dz) % 4

    x_peer = {"xl": 1 - xl}
    y_up, y_down = {"y": (y + 1) % 4}, {"y": (y + 3) % 4}
    h_peer = {"xh": 1 - xh}
    z_up, z_down = {"z": (z + 1) % 4}, {"z": (z + 3) % 4}
    sibling = {"c": 1 - c}

    count = [0, 0]
    sends = []

    def new_recv():
        count[0] += 1
        return rsem.at[count[0] - 1]

    def new_send(view):
        count[1] += 1
        sem = ssem.at[count[1] - 1]
        sends.append((view, sem))
        return sem

    class Recv:
        def __init__(self, sem, view):
            self.sem, self.view = sem, view

        def wait_recv(self):
            pltpu.make_async_remote_copy(
                src_ref=self.view, dst_ref=self.view, send_sem=ssem.at[0], recv_sem=self.sem,
                device_id=x_peer, device_id_type=MESH,
            ).wait_recv()

    def send(src, dst, device, send_sem, recv_sem=None):
        copy = pltpu.make_async_remote_copy(
            src_ref=src, dst_ref=dst, send_sem=send_sem, recv_sem=new_recv() if recv_sem is None else recv_sem,
            device_id=device, device_id_type=MESH,
        )
        copy.start()
        return copy

    cb = pl.multiple_of(c * WB, WB)
    wg = xh * 4 + z
    loads = [
        pltpu.make_async_copy(obs, xf0.at[g, pl.ds(0, TR), :], lsem.at[0]),
        pltpu.make_async_copy(wts.at[0], wf0.at[wg, pl.ds(cb, WB), :], lsem.at[1]),
        pltpu.make_async_copy(wts.at[1], wf1.at[wg, pl.ds(cb, WB), :], lsem.at[2]),
        pltpu.make_async_copy(nxt, xf0.at[g, pl.ds(TR, AR), :], lsem.at[3]),
    ]
    for load in loads:
        load.start()

    barrier = pltpu.get_barrier_semaphore()
    friends = [h_peer, z_up, z_down, sibling]
    for k in range(1, 8):
        gt = (g + k) % 8
        friends.append({"xl": gt // 4, "y": gt % 4})
    for friend in friends:
        pl.semaphore_signal(barrier, inc=1, device_id=friend, device_id_type=MESH)
    pl.semaphore_wait(barrier, len(friends))

    def x_start(layer, first, amount):
        buf, half = xf[layer], amount // 2
        lo, hi = pl.ds(first, half), pl.ds(first + half, half)

        out = new_send(buf.at[pl.ds(0, 7), pl.ds(0, amount), :])

        def go(block, rows, device, recv_sem=None):
            return send(buf.at[block, rows, :], buf.at[block, rows, :], device, out, recv_sem)

        near = Recv(new_recv(), buf.at[0, pl.ds(0, amount), :])
        far = Recv(new_recv(), buf.at[pl.ds(0, 3), pl.ds(0, amount), :])
        return {"go": go, "lo": lo, "hi": hi, "near": near, "far": far}

    def x_own(st, rows):
        go, lo = st["go"], st["lo"]
        if rows == "lo":
            st["up_lo"] = go(g, lo, y_up)
            st["x_lo"] = go(g, lo, x_peer)
        else:
            st["dn_hi"] = go(g, st["hi"], y_down)
            st["x_hi"] = go(g, st["hi"], x_peer)
            go(g, st["hi"], y_up, st["near"].sem)
            go(g, lo, y_down, st["near"].sem)

    def x_fwd1(st):
        go = st["go"]
        st["up_lo"].wait_recv()
        st["f_lo"] = go(rel_g(0, 3), st["lo"], y_up)
        st["dn_hi"].wait_recv()
        st["f_hi"] = go(rel_g(0, 1), st["hi"], y_down)

    def x_fwd2(st):
        go, block, far = st["go"], rel_g(1, 0), st["far"].sem
        st["x_lo"].wait_recv()
        go(block, st["lo"], y_up, far)
        go(block, st["lo"], y_down, far)
        st["x_hi"].wait_recv()
        go(block, st["hi"], y_up, far)
        go(block, st["hi"], y_down, far)

    def x_fwd3(st):
        go, block, far = st["go"], rel_g(0, 2), st["far"].sem
        st["f_lo"].wait_recv()
        go(block, st["lo"], x_peer, far)
        st["f_hi"].wait_recv()
        go(block, st["hi"], x_peer, far)

    def x_near(st):
        st["near"].wait_recv()

    def x_far(st):
        st["far"].wait_recv()

    half_w = WB // 2

    def w_piece(block, part):
        if part == "all":
            return (block, pl.ds(cb, WB), slice(None))
        start = cb if part == "lo" else cb + half_w
        return (block, pl.ds(pl.multiple_of(start, half_w), half_w), slice(None))

    def w_start(layer):
        buf = wf[layer]

        out = new_send(xf[layer].at[pl.ds(0, 6), :, :])

        def go(block, part, device, recv_sem=None):
            where = w_piece(block, part)
            return send(buf.at[where], buf.at[where], device, out, recv_sem)

        st = {"go": go}
        st["f"] = Recv(new_recv(), buf.at[0, pl.ds(0, WB), :])
        st["g"] = Recv(new_recv(), buf.at[0, pl.ds(0, WB), :])
        st["sib"] = Recv(new_recv(), buf.at[pl.ds(0, 4), :, :])
        st["up_lo"] = go(wg, "lo", z_up)
        st["dn_hi"] = go(wg, "hi", z_down)
        st["h"] = go(wg, "all", h_peer)
        st["up_hi"] = go(wg, "hi", z_up)
        st["dn_lo"] = go(wg, "lo", z_down)
        w_share(st, wg)
        return st

    def w_share(st, block):
        st["go"](block, "all", sibling, st["sib"].sem)

    def w_fwd1(st):
        go = st["go"]
        st["up_lo"].wait_recv()
        go(rel_w(0, 3), "lo", z_up, st["f"].sem)
        st["dn_hi"].wait_recv()
        go(rel_w(0, 1), "hi", z_down, st["f"].sem)

    def w_fwd2(st):
        go, far = st["go"], rel_w(1, 0)
        st["h"].wait_recv()
        st["h_up_lo"] = go(far, "lo", z_up)
        st["h_dn_hi"] = go(far, "hi", z_down)
        st["h_up_hi"] = go(far, "hi", z_up)
        st["h_dn_lo"] = go(far, "lo", z_down)
        w_share(st, far)
        st["up_hi"].wait_recv()
        w_share(st, rel_w(0, 3))
        st["dn_lo"].wait_recv()
        w_share(st, rel_w(0, 1))

    def w_fwd3(st):
        go = st["go"]
        st["h_up_lo"].wait_recv()
        go(rel_w(1, 3), "lo", z_up, st["g"].sem)
        st["h_dn_hi"].wait_recv()
        go(rel_w(1, 1), "hi", z_down, st["g"].sem)
        st["f"].wait_recv()
        w_share(st, rel_w(0, 2))

    def w_finish(st):
        st["h_up_hi"].wait_recv()
        w_share(st, rel_w(1, 3))
        st["h_dn_lo"].wait_recv()
        w_share(st, rel_w(1, 1))
        st["g"].wait_recv()
        w_share(st, rel_w(1, 2))
        st["sib"].wait_recv()

    def blocks(layer, first, amount, j0, j1, fresh):
        buf, weights = xf[layer], wf[layer]
        rows = slice(first, first + amount)
        if fresh:
            acc[rows, :] = nn(buf[g, rows, :], weights[g])

        def body(j, carry):
            block = ((xl + j // 4) % 2) * 4 + (y + j % 4) % 4
            acc[rows, :] += nn(buf[block, rows, :], weights[block])
            return carry

        lax.fori_loop(j0, j1, body, 0)

    def activate(first, amount, out, slope, tile=64):
        def body(i, carry):
            rows = pl.ds(pl.multiple_of(first + i * tile, tile), tile)
            value = acc[rows, :]
            sigma = jax.nn.sigmoid(value)
            out(rows, (value * sigma).astype(BF16))
            if slope is not None:
                slope[rows, :] = sigma * (1.0 + value * (1.0 - sigma))
            return carry

        lax.fori_loop(0, amount // tile, body, 0)

    def into_x1(rows, value):
        xf1[g, rows, :] = value

    def into_x2(rows, value):
        x2[rows, :] = value

    def next_layer(first, slope):
        st = x_start(1, first, CH)
        activate(first, CH // 2, into_x1, slope)
        x_own(st, "lo")
        activate(first + CH // 2, CH // 2, into_x1, slope)
        x_own(st, "hi")
        return st

    def to_group(src, dst, landed):
        out, got = new_send(landed), new_recv()
        for k in range(1, 8):
            gt = (g + k) % 8
            send(src, dst.at[g], {"xl": gt // 4, "y": gt % 4}, out, got)
        return Recv(got, landed)

    def from_group(own_part, dst):
        total = own_part[...]
        for k in range(1, 8):
            total = total + dst[(g + 8 - k) % 8]
        return total

    def head_send(ch):
        hs[ch] = nt(headt[0:32, :], x2[CH * ch : CH * (ch + 1), :])[0:24, :]
        return to_group(hs.at[ch], hr.at[ch], hr.at[ch, pl.ds(0, 7), :, :])

    def head_loss(ch, got):
        got.wait_recv()
        total = from_group(hs.at[ch], hr.at[ch])
        grad = vtrace(total, misc[ch, 0:24, :], misc[ch, 24:25, :], misc[ch, 25:26, :], misc[ch, 26:27, :])
        tmp[0:24, :] = grad
        rows = slice(CH * ch, CH * (ch + 1))
        og_r[rows, :] = tmp[...].T.astype(BF16)
        pg1[rows, :] = (nn(og_r[rows, :], headt[...]) * slope1[rows, :]).astype(BF16)
        pg1t[:, rows] = pg1[rows, :].T

    where_g = (rel_g(1, 2), rel_g(1, 1), rel_g(1, 3), rel_g(0, 1), rel_g(0, 3), rel_g(0, 2), rel_g(1, 0))

    class Scatter:
        def __init__(self, first, amount, col, cols):
            half = amount // 2
            self.rows = slice(first, first + amount)
            self.lo, self.hi = slice(first, first + half), slice(first + half, first + amount)
            self.cs = slice(col, col + cols)
            self.out = new_send(sb.at[:, self.ds(self.rows), self.ds(self.cs)])
            self.s2 = [Recv(new_recv(), rb.at[pl.ds(0, 2), self.ds(rows), self.ds(self.cs)]) for rows in (self.lo, self.hi)]
            self.last = Recv(new_recv(), rb.at[pl.ds(0, 3), self.ds(self.rows), self.ds(self.cs)])

        def ds(self, rows):
            return pl.ds(rows.start, rows.stop - rows.start)

        def piece(self, block):
            return nt(pg1[self.rows, :], wf1[block, self.cs, :])

        def make(self, k):
            sb[k, self.rows, self.cs] = self.piece(where_g[k]).astype(BF16)

        def push(self, k, rows, device, recv_sem=None):
            where = (k, self.ds(rows), self.ds(self.cs))
            return send(sb.at[where], rb.at[where], device, self.out, recv_sem)

        def add_in(self, k, rows, *terms):
            value = sb[k, rows, self.cs].astype(F32)
            for term in terms:
                value = value + rb[term, rows, self.cs].astype(F32)
            sb[k, rows, self.cs] = value.astype(BF16)

        def first(self):
            self.make(0)
            self.s1 = [self.push(0, self.lo, x_peer), self.push(0, self.hi, x_peer)]

        def make_rest(self):
            self.make(5)
            self.make(6)
            own[self.rows, self.cs] = self.piece(g)

        def push_two(self):
            for i, rows in enumerate((self.lo, self.hi)):
                self.push(1, rows, y_up, self.s2[i].sem)
                self.push(2, rows, y_down, self.s2[i].sem)

        def push_plain(self):
            self.push(3, self.hi, y_up, self.last.sem)
            self.push(4, self.lo, y_down, self.last.sem)

        def rest(self):
            self.make(1)
            self.make(2)
            self.push_two()
            self.make(3)
            self.make(4)
            self.push_plain()
            self.make_rest()

        def prepare(self):
            self.first()
            for k in range(1, 5):
                self.make(k)
            self.make_rest()

        def mid1(self):
            self.s1[0].wait_recv()
            self.add_in(5, self.lo, 0)
            self.s4u = self.push(5, self.lo, y_up)
            self.s1[1].wait_recv()
            self.add_in(5, self.hi, 0)
            self.s4d = self.push(5, self.hi, y_down)

        def mid2(self):
            for i, rows in enumerate((self.lo, self.hi)):
                self.s2[i].wait_recv()
                self.add_in(6, rows, 1, 2)
                self.push(6, rows, x_peer, self.last.sem)

        def mid3(self):
            self.s4u.wait_recv()
            self.add_in(3, self.lo, 5)
            self.push(3, self.lo, y_up, self.last.sem)
            self.s4d.wait_recv()
            self.add_in(4, self.hi, 5)
            self.push(4, self.hi, y_down, self.last.sem)

        def close(self):
            self.last.wait_recv()
            cs = self.cs
            for r in range(self.rows.start, self.rows.stop, 128):
                rows = slice(r, r + 128)
                value = own[rows, cs] + rb[3, rows, cs].astype(F32) + rb[4, rows, cs].astype(F32) + rb[6, rows, cs].astype(F32)
                pg0t[cs, rows] = (value * slope0[rows, cs]).astype(BF16).T

    class Weights:
        def __init__(self, layer, pgt, bufs, col, cols, extra, halves=(0, 1)):
            self.halves = halves
            self.layer, self.pgt, self.extra = layer, pgt, extra
            self.dws, self.dwr, self.q, self.rz1, self.rz2, self.xs, self.rx = bufs
            self.cols, self.size = cols, cols + extra
            self.cs, self.top = slice(col, col + cols), slice(col + cols, col + cols + extra)
            self.all, half = slice(col, col + self.size), col + cols // 2
            self.low, self.high = slice(col, half), slice(half, col + self.size)
            self.base = count[0]
            count[0] += 8
            every = self.ds(self.all)
            self.out = new_send(self.q.at[pl.ds(0, 7), every, :])
            self.give_sem = new_send(self.dws.at[:, every, :])
            self.sums = {xr: Recv(new_recv(), self.rz2.at[xr, :, every, :]) for xr in halves}
            self.st = {}

        def ds(self, rows):
            return pl.ds(rows.start, rows.stop - rows.start)

        def block(self, i):
            return ((xh + 1 - i % 2) % 2) * 4 + (z + 2 + i // 2) % 4

        def copy_of(self, i):
            every = self.ds(self.all)
            return pltpu.make_async_remote_copy(
                src_ref=self.dws.at[i, every, :], dst_ref=self.dwr.at[i, every, :],
                send_sem=self.give_sem, recv_sem=rsem.at[self.base + i],
                device_id=sibling, device_id_type=MESH,
            )

        def head_rows(self, block, core):
            return hgp[pl.ds(pl.multiple_of((2 * block + core) * 32, 32), 32), :]

        def give(self, i0, i1):
            other = pl.multiple_of((1 - c) * WB, WB)

            def body(i, carry):
                block = self.block(i)
                term = nn(self.pgt[self.cs, :], xf[self.layer][block, 0:TR, pl.ds(other, WB)])
                self.dws[i, self.cs, :] = term.astype(BF16)
                if self.extra:
                    self.dws[i, self.top, 0:128] = self.head_rows(block, 1 - c).astype(BF16)
                    self.dws[i, self.top, 128:256] = jnp.zeros((self.extra, 128), BF16)
                self.copy_of(i).start()
                return carry

            lax.fori_loop(i0, i1, body, 0)

        def keep(self, i0, i1):
            q, dwr, cs, top = self.q, self.dwr, self.cs, self.top

            def body(i, carry):
                block = self.block(i)
                term = nn(self.pgt[cs, :], xf[self.layer][block, 0:TR, pl.ds(cb, WB)])
                self.copy_of(i).wait_recv()
                q[i, cs, :] = (term + dwr[i, cs, :].astype(F32)).astype(BF16)
                if self.extra:
                    q[i, top, 0:128] = (self.head_rows(block, c) + dwr[i, top, 0:128].astype(F32)).astype(BF16)
                    q[i, top, 128:256] = jnp.zeros((self.extra, 128), BF16)
                return carry

            lax.fori_loop(i0, i1, body, 0)

        def go(self, i, rows, dst, device, recv_sem=None):
            where = self.ds(rows)
            return send(self.q.at[i, where, :], dst.at[where, :], device, self.out, recv_sem)

        def z_first(self):
            for xr in self.halves:
                self.st["a", xr] = self.go(xr, self.low, self.rz1.at[xr], z_up)
                self.st["b", xr] = self.go(xr, self.high, self.rz1.at[xr], z_down)

        def z_plain(self):
            for xr in self.halves:
                self.go(6 + xr, self.high, self.rz2.at[xr, 0], z_up, self.sums[xr].sem)
                self.go(2 + xr, self.low, self.rz2.at[xr, 1], z_down, self.sums[xr].sem)

        def early(self):
            self.give(0, 4)
            self.keep(0, 2)
            self.z_first()
            self.give(4, 8)

        def late(self):
            self.keep(2, 4)
            self.keep(6, 8)
            self.z_plain()
            self.keep(4, 6)

        def z_added(self):
            q, rz1, st = self.q, self.rz1, self.st
            for xr in self.halves:
                for name, i, rows, side, device in (("a", 6, self.low, 0, z_up), ("b", 2, self.high, 1, z_down)):
                    st[name, xr].wait_recv()
                    value = q[i + xr, rows, :].astype(F32) + rz1[xr, rows, :].astype(F32)
                    q[i + xr, rows, :] = value.astype(BF16)
                    self.go(i + xr, rows, self.rz2.at[xr, side], device, self.sums[xr].sem)

        def z_sum(self, xr):
            self.sums[xr].wait_recv()
            every = self.all
            return (
                self.q[4 + xr, every, :].astype(F32)
                + self.rz2[xr, 0, every, :].astype(F32)
                + self.rz2[xr, 1, every, :].astype(F32)
            )

        def cross(self):
            every = self.ds(self.all)
            self.xs[self.all, :] = self.z_sum(0).astype(BF16)
            self.h = send(self.xs.at[every, :], self.rx.at[every, :], h_peer, self.out)

        def result(self):
            value = self.z_sum(1)
            if 0 in self.halves:
                self.h.wait_recv()
                value = value + self.rx[self.all, :].astype(F32)
            dw_out[self.layer, :, self.cs] = value[0 : self.cols, :].T
            if self.extra:
                hg_out[...] = value[self.cols :, 0:128].T[0 : ACT + 1, :]

    loads[0].wait()
    loads[1].wait()
    w0 = w_start(0)
    a0, b0 = x_start(0, 0, CH), x_start(0, CH, CH)
    x_own(a0, "lo")
    x_own(a0, "hi")
    x_own(b0, "lo")
    x_own(b0, "hi")
    loads[2].wait()
    loads[3].wait()

    headt[...] = jnp.zeros_like(headt)
    headt[0 : ACT + 1, :] = head[...]
    misc[...] = jnp.zeros_like(misc)
    for r in range(8):
        ch, lane = r // 4, STEPS * (r % 4)
        steps = slice(lane, lane + STEPS - 1)
        misc[ch, 0:ACT, steps] = acting[:, r, :]
        misc[ch, 24:25, steps] = actions[r : r + 1, :].astype(F32)
        misc[ch, 25:26, steps] = rewards[r : r + 1, :]
        misc[ch, 26:27, steps] = finished[r : r + 1, :].astype(F32)
    tmp[...] = jnp.zeros_like(tmp)

    w_fwd1(w0)
    x_fwd1(a0)
    w_fwd2(w0)
    x_fwd1(b0)
    x_fwd2(a0)
    w_fwd3(w0)
    x_fwd3(a0)
    x_fwd2(b0)
    x_fwd3(b0)
    w1 = w_start(1)
    w_finish(w0)
    x_near(a0)
    blocks(0, 0, CH, 1, 5, True)
    x_far(a0)
    blocks(0, 0, CH, 5, 8, False)
    a1 = next_layer(0, slope0)
    w_fwd1(w1)
    x_near(b0)
    blocks(0, CH, CH, 1, 5, True)
    x_far(b0)
    blocks(0, CH, CH, 5, 8, False)
    b1 = next_layer(CH, slope0)

    x_fwd1(a1)
    w_fwd2(w1)
    x_fwd1(b1)
    x_fwd2(a1)
    w_fwd3(w1)
    x_fwd3(a1)
    x_fwd3(b1)
    x_fwd2(b1)
    w_finish(w1)
    x_near(a1)
    blocks(1, 0, CH, 1, 5, True)
    x_far(a1)
    blocks(1, 0, CH, 5, 8, False)
    activate(0, CH, into_x2, slope1)
    head_a = head_send(0)
    c0 = x_start(0, TR, AR)
    x_own(c0, "lo")
    x_own(c0, "hi")
    x_near(b1)
    blocks(1, CH, CH, 1, 5, True)
    x_far(b1)
    blocks(1, CH, CH, 5, 8, False)
    activate(CH, CH, into_x2, slope1)
    head_b = head_send(1)

    da1, da2 = Scatter(0, CH, 0, CH), Scatter(0, CH, CH, CH)
    db1, db2 = Scatter(CH, CH, 0, CH), Scatter(CH, CH, CH, CH)
    g1 = Weights(1, pg1t, (dws1, dwr1, q1, rz1a, rz2a, xs1, rx1), 0, FB, ER - FB)
    bufs0 = (dws0, dwr0, q0, rz1b, rz2b, xs0, rx0)
    g0a = Weights(0, pg0t, bufs0, 0, CH, 0)
    g0b = Weights(0, pg0t, bufs0, CH, CH, 0)
    head_loss(0, head_a)
    da1.first()
    da1.rest()
    x_fwd1(c0)
    da2.prepare()
    head_loss(1, head_b)
    db1.first()
    hgp[...] = tn(x2[0:TR, :], og_r[...])
    g1.give(0, 4)
    db1.rest()
    g1.keep(0, 2)
    g1.z_first()
    da1.mid1()
    da1.mid2()
    g1.give(4, 8)
    db2.prepare()
    db1.mid1()
    x_fwd2(c0)
    g1.keep(2, 4)
    db1.mid2()
    g1.keep(6, 8)
    g1.z_plain()
    da1.mid3()
    g1.keep(4, 6)
    db1.mid3()
    da2.mid1()
    db2.mid1()
    da2.push_two()
    db2.push_two()
    da2.push_plain()
    db2.push_plain()
    x_fwd3(c0)
    g1.z_added()
    da1.close()
    db1.close()
    g0a.give(0, 4)
    g0a.keep(0, 2)
    g0a.z_first()
    da2.mid3()
    db2.mid3()
    g0a.give(4, 8)
    x_near(c0)
    x_far(c0)
    blocks(0, TR, AR, 1, 8, True)
    activate(TR, AR, into_x1, None)
    da2.mid2()
    g0a.keep(2, 4)
    g0a.keep(6, 8)
    g0a.z_plain()
    db2.mid2()
    c1 = x_start(1, TR, AR)
    x_own(c1, "lo")
    x_own(c1, "hi")
    g0a.keep(4, 6)
    g0a.z_added()
    g1.cross()
    da2.close()
    db2.close()
    g0b.give(0, 4)
    x_fwd1(c1)
    x_fwd2(c1)
    g0b.keep(0, 2)
    g0b.z_first()
    g0b.give(4, 8)
    g0b.late()
    x_fwd3(c1)
    g0b.z_added()
    g0a.cross()
    x_near(c1)
    x_far(c1)
    blocks(1, TR, AR, 1, 8, True)
    activate(TR, AR, into_x2, None)
    ha_s[...] = nt(headt[0:32, :], x2[TR : TR + AR, :])[0:24, :]
    acts = to_group(ha_s, ha_r, ha_r.at[pl.ds(0, 7), :, :])
    g0b.cross()
    g1.result()
    g0a.result()
    acts.wait_recv()
    al_out[...] = from_group(ha_s, ha_r)[0:ACT, :]
    g0b.result()

    for view, sem in sends:
        pltpu.make_async_remote_copy(
            src_ref=view, dst_ref=view, send_sem=sem, recv_sem=rsem.at[0], device_id=x_peer, device_id_type=MESH,
        ).wait_send()
    assert (count[0], count[1]) == (N_RECV, N_SEND), count


def per_device(observations, next_observations, trunk_weights, head_weights, acting, actions, rewards, finished):
    v = pltpu.VMEM
    dw_bufs = lambda rows: [
        v((8, rows, WB), BF16), v((8, rows, WB), BF16), v((8, rows, WB), BF16), v((2, rows, WB), BF16),
        v((2, 2, rows, WB), BF16), v((rows, WB), BF16), v((rows, WB), BF16),
    ]
    scratch = [
        v((8, TR + AR, FB), BF16), v((8, TR + AR, FB), BF16), v((8, FB, FB), BF16), v((8, FB, FB), BF16),
        v((TR + AR, FB), F32), v((TR, FB), F32), v((TR, FB), F32), v((TR + AR, FB), BF16),
        v((128, FB), BF16), v((128, CH), F32), v((2, 32, CH), F32),
        v((2, 24, CH), F32), v((2, 8, 24, CH), F32), v((24, 128), F32), v((8, 24, 128), F32),
        v((TR, 128), BF16), v((TR, FB), BF16), v((FB, TR), BF16), v((FB, TR), BF16), v((FB, 128), F32),
        v((7, TR, FB), BF16), v((7, TR, FB), BF16), v((TR, FB), F32),
        *dw_bufs(ER), *dw_bufs(FB),
        pltpu.SemaphoreType.DMA((N_SEND,)), pltpu.SemaphoreType.DMA((N_RECV,)), pltpu.SemaphoreType.DMA((4,)),
    ]
    hbm = pl.BlockSpec(memory_space=pltpu.HBM)
    vmem = pl.BlockSpec(memory_space=pltpu.VMEM)
    trunk_grads, head_grads, actor_logits = pl.pallas_call(
        kernel,
        out_shape=(
            jax.ShapeDtypeStruct((2, WB, FB), F32),
            jax.ShapeDtypeStruct((ACT + 1, 32), F32),
            jax.ShapeDtypeStruct((ACT, AR), F32),
        ),
        in_specs=[hbm, hbm, hbm, vmem, vmem, vmem, vmem, vmem],
        out_specs=(vmem, vmem, vmem),
        scratch_shapes=scratch,
        compiler_params=pltpu.CompilerParams(
            collective_id=0, has_side_effects=True, vmem_limit_bytes=62 * 1024 * 1024
        ),
        name="learner_step",
    )(
        observations.reshape(TR, FB), next_observations, trunk_weights, head_weights.T, acting.transpose(2, 0, 1),
        actions, rewards, finished,
    )
    return trunk_grads, head_grads.T, actor_logits.T


def solution(mesh):
    split = Mesh(mesh.devices.reshape(SIZES), AXES)
    return jax.shard_map(
        per_device,
        mesh=split,
        in_specs=(
            P(DP, None, GROUP),
            P(DP, GROUP),
            P(None, DP, GROUP),
            P(GROUP, None),
            P(DP, None, None),
            P(DP, None),
            P(DP, None),
            P(DP, None),
        ),
        out_specs=(P(None, DP, GROUP), P(GROUP + DP, None), P(DP, None)),
        check_vma=False,
    )
```

```python
import functools

import jax
import jax.numpy as jnp
from jax import lax
from jax.experimental import pallas as pl
from jax.experimental.pallas import tpu as pltpu
from jax.sharding import Mesh
from jax.sharding import PartitionSpec as P

AXES = ("xl", "y", "xh", "z", "c")
SIZES = (2, 4, 2, 4, 2)
DP = ("xh", "z", "c")
GROUP = ("xl", "y")
MESH = pl.DeviceIdType.MESH
F32 = jnp.float32
BF16 = jnp.bfloat16

discount_rate = 0.99
value_weight = 0.5
entropy_weight = 0.1
loss_divisor = 16.0

TR = 512
AR = 128
FB = 512
WB = 256
STEPS = 64
ACT = 18
ER = 544
N_RECV, N_SEND = 148, 21
CH = 256


def nn(a, b):
    return jnp.dot(a, b, preferred_element_type=F32)


def nt(a, b):
    return lax.dot_general(a, b, (((1,), (1,)), ((), ())), preferred_element_type=F32)


def tn(a, b):
    return lax.dot_general(a, b, (((0,), (0,)), ((), ())), preferred_element_type=F32)


def vtrace(logits, behave, action, reward, finished):
    row = lax.broadcasted_iota(jnp.int32, logits.shape, 0)
    step = lax.broadcasted_iota(jnp.int32, reward.shape, 1)
    live = step % STEPS < STEPS - 1
    lanes = reward.shape[1]
    is_act = row < ACT

    def log_softmax(values):
        top = jnp.max(jnp.where(is_act, values, -3.0e38), axis=0, keepdims=True)
        shifted = jnp.where(is_act, values - top, 0.0)
        total = jnp.sum(jnp.where(is_act, jnp.exp(shifted), 0.0), axis=0, keepdims=True)
        return jnp.where(is_act, shifted - jnp.log(total), 0.0)

    log_policy = log_softmax(logits)
    log_behave = log_softmax(behave)
    chosen = jnp.where(row.astype(F32) == action, 1.0, 0.0)
    ratio = jnp.exp(jnp.sum((log_policy - log_behave) * chosen, axis=0, keepdims=True))
    clipped = jnp.minimum(ratio, 1.0)
    discount = discount_rate * (1.0 - finished)
    current = logits[ACT : ACT + 1, :]
    following = pltpu.roll(current, lanes - 1, 1)
    delta = jnp.where(live, clipped * (reward + discount * following - current), 0.0)
    factor = jnp.where(live, discount * clipped, 0.0)
    for shift in (1, 2, 4, 8, 16, 32):
        delta = delta + factor * pltpu.roll(delta, lanes - shift, 1)
        factor = factor * pltpu.roll(factor, lanes - shift, 1)
    targets = current + delta
    next_targets = pltpu.roll(targets, lanes - 1, 1)
    advantage = clipped * (reward + discount * next_targets - current)
    probability = jnp.where(is_act, jnp.exp(log_policy), 0.0)
    entropy = -jnp.sum(probability * log_policy, axis=0, keepdims=True)
    logit_grad = (
        -advantage * (chosen - probability)
        + entropy_weight * probability * (log_policy + entropy)
    ) / loss_divisor
    value_grad = -value_weight * (targets - current) / loss_divisor
    grad = jnp.where(is_act, logit_grad, jnp.where(row == ACT, value_grad, 0.0))
    return jnp.where(live, grad, 0.0)


def kernel(
    obs, nxt, wts, head_in, acting_in, actions_in, rewards_in, finished_in,
    dw_out, hg_out, al_out,
    xf0, xf1, wf0, wf1, acc, slope0, slope1, x2, headt, tmp, misc,
    hs, hr, ha_s, ha_r, og_r, pg1, pg1t, pg0t, hgp,
    sb, rb, own,
    dws1, dwr1, q1, rz1a, rz2a, xs1, rx1,
    dws0, dwr0, q0, rz1b, rz2b, xs0, rx0,
    dwv, hgv, alv, head, acting, actions, rewards, finished, ssem, rsem, lsem,
):
    xl, y, xh, z, c = (lax.axis_index(a) for a in AXES)
    g = xl * 4 + y
    xf, wf = (xf0, xf1), (wf0, wf1)

    def rel_g(dx, dy):
        return ((xl + dx) % 2) * 4 + (y + dy) % 4

    def rel_w(dx, dz):
        return ((xh + dx) % 2) * 4 + (z + dz) % 4

    x_peer = {"xl": 1 - xl}
    y_up, y_down = {"y": (y + 1) % 4}, {"y": (y + 3) % 4}
    h_peer = {"xh": 1 - xh}
    z_up, z_down = {"z": (z + 1) % 4}, {"z": (z + 3) % 4}
    sibling = {"c": 1 - c}

    count = [0, 0]
    sends = []

    def new_recv():
        count[0] += 1
        return rsem.at[count[0] - 1]

    def new_send(view):
        count[1] += 1
        sem = ssem.at[count[1] - 1]
        sends.append((view, sem))
        return sem

    class Recv:
        def __init__(self, sem, view):
            self.sem, self.view = sem, view

        def wait_recv(self):
            pltpu.make_async_remote_copy(
                src_ref=self.view, dst_ref=self.view, send_sem=ssem.at[0], recv_sem=self.sem,
                device_id=x_peer, device_id_type=MESH,
            ).wait_recv()

    def send(src, dst, device, send_sem, recv_sem=None):
        copy = pltpu.make_async_remote_copy(
            src_ref=src, dst_ref=dst, send_sem=send_sem, recv_sem=new_recv() if recv_sem is None else recv_sem,
            device_id=device, device_id_type=MESH,
        )
        copy.start()
        return copy

    cb = pl.multiple_of(c * WB, WB)
    wg = xh * 4 + z
    loads = [
        pltpu.make_async_copy(obs, xf0.at[g, pl.ds(0, TR), :], lsem.at[0]),
        pltpu.make_async_copy(wts.at[0], wf0.at[wg, pl.ds(cb, WB), :], lsem.at[1]),
        pltpu.make_async_copy(wts.at[1], wf1.at[wg, pl.ds(cb, WB), :], lsem.at[2]),
        pltpu.make_async_copy(nxt, xf0.at[g, pl.ds(TR, AR), :], lsem.at[3]),
        pltpu.make_async_copy(head_in, head, lsem.at[4]),
        pltpu.make_async_copy(acting_in, acting, lsem.at[5]),
        pltpu.make_async_copy(actions_in, actions, lsem.at[6]),
        pltpu.make_async_copy(rewards_in, rewards, lsem.at[7]),
        pltpu.make_async_copy(finished_in, finished, lsem.at[8]),
    ]
    for load in loads:
        load.start()

    stores = []

    def store(src, dst):
        stores.append(pltpu.make_async_copy(src, dst, lsem.at[9 + len(stores)]))
        stores[-1].start()

    barrier = pltpu.get_barrier_semaphore()
    friends = [x_peer, y_up, y_down, h_peer, z_up, z_down, sibling]
    for friend in friends:
        pl.semaphore_signal(barrier, inc=1, device_id=friend, device_id_type=MESH)
    pl.semaphore_wait(barrier, len(friends))

    def x_start(layer, first, amount):
        buf, half = xf[layer], amount // 2
        lo, hi = pl.ds(first, half), pl.ds(first + half, half)

        out = new_send(buf.at[pl.ds(0, 7), pl.ds(0, amount), :])

        def go(block, rows, device, recv_sem=None):
            return send(buf.at[block, rows, :], buf.at[block, rows, :], device, out, recv_sem)

        near = Recv(new_recv(), buf.at[0, pl.ds(0, amount), :])
        far = Recv(new_recv(), buf.at[pl.ds(0, 3), pl.ds(0, amount), :])
        return {"go": go, "lo": lo, "hi": hi, "near": near, "far": far}

    def x_own(st, rows):
        go, lo = st["go"], st["lo"]
        if rows == "lo":
            st["up_lo"] = go(g, lo, y_up)
            st["x_lo"] = go(g, lo, x_peer)
        else:
            st["dn_hi"] = go(g, st["hi"], y_down)
            st["x_hi"] = go(g, st["hi"], x_peer)
            go(g, st["hi"], y_up, st["near"].sem)
            go(g, lo, y_down, st["near"].sem)

    def x_fwd1(st):
        go = st["go"]
        st["up_lo"].wait_recv()
        st["f_lo"] = go(rel_g(0, 3), st["lo"], y_up)
        st["dn_hi"].wait_recv()
        st["f_hi"] = go(rel_g(0, 1), st["hi"], y_down)

    def x_fwd2(st):
        go, block, far = st["go"], rel_g(1, 0), st["far"].sem
        st["x_lo"].wait_recv()
        go(block, st["lo"], y_up, far)
        go(block, st["lo"], y_down, far)
        st["x_hi"].wait_recv()
        go(block, st["hi"], y_up, far)
        go(block, st["hi"], y_down, far)

    def x_fwd3(st):
        go, block, far = st["go"], rel_g(0, 2), st["far"].sem
        st["f_lo"].wait_recv()
        go(block, st["lo"], x_peer, far)
        st["f_hi"].wait_recv()
        go(block, st["hi"], x_peer, far)

    def x_near(st):
        st["near"].wait_recv()

    def x_far(st):
        st["far"].wait_recv()

    half_w = WB // 2

    def w_piece(block, part):
        if part == "all":
            return (block, pl.ds(cb, WB), slice(None))
        start = cb if part == "lo" else cb + half_w
        return (block, pl.ds(pl.multiple_of(start, half_w), half_w), slice(None))

    def w_start(layer):
        buf = wf[layer]

        out = new_send(xf[layer].at[pl.ds(0, 6), :, :])

        def go(block, part, device, recv_sem=None):
            where = w_piece(block, part)
            return send(buf.at[where], buf.at[where], device, out, recv_sem)

        st = {"go": go}
        st["f"] = Recv(new_recv(), buf.at[0, pl.ds(0, WB), :])
        st["g"] = Recv(new_recv(), buf.at[0, pl.ds(0, WB), :])
        st["sib"] = Recv(new_recv(), buf.at[pl.ds(0, 4), :, :])
        st["up_lo"] = go(wg, "lo", z_up)
        st["dn_hi"] = go(wg, "hi", z_down)
        st["h"] = go(wg, "all", h_peer)
        st["up_hi"] = go(wg, "hi", z_up)
        st["dn_lo"] = go(wg, "lo", z_down)
        w_share(st, wg)
        return st

    def w_share(st, block):
        st["go"](block, "all", sibling, st["sib"].sem)

    def w_fwd1(st):
        go = st["go"]
        st["up_lo"].wait_recv()
        go(rel_w(0, 3), "lo", z_up, st["f"].sem)
        st["dn_hi"].wait_recv()
        go(rel_w(0, 1), "hi", z_down, st["f"].sem)

    def w_fwd2(st):
        go, far = st["go"], rel_w(1, 0)
        st["h"].wait_recv()
        st["h_up_lo"] = go(far, "lo", z_up)
        st["h_dn_hi"] = go(far, "hi", z_down)
        st["h_up_hi"] = go(far, "hi", z_up)
        st["h_dn_lo"] = go(far, "lo", z_down)
        w_share(st, far)
        st["up_hi"].wait_recv()
        w_share(st, rel_w(0, 3))
        st["dn_lo"].wait_recv()
        w_share(st, rel_w(0, 1))

    def w_fwd3(st):
        go = st["go"]
        st["h_up_lo"].wait_recv()
        go(rel_w(1, 3), "lo", z_up, st["g"].sem)
        st["h_dn_hi"].wait_recv()
        go(rel_w(1, 1), "hi", z_down, st["g"].sem)
        st["f"].wait_recv()
        w_share(st, rel_w(0, 2))

    def w_finish(st):
        st["h_up_hi"].wait_recv()
        w_share(st, rel_w(1, 3))
        st["h_dn_lo"].wait_recv()
        w_share(st, rel_w(1, 1))
        st["g"].wait_recv()
        w_share(st, rel_w(1, 2))
        st["sib"].wait_recv()

    def blocks(layer, first, amount, j0, j1, fresh):
        buf, weights = xf[layer], wf[layer]
        rows = slice(first, first + amount)
        if fresh:
            acc[rows, :] = nn(buf[g, rows, :], weights[g])

        def body(j, carry):
            block = ((xl + j // 4) % 2) * 4 + (y + j % 4) % 4
            acc[rows, :] += nn(buf[block, rows, :], weights[block])
            return carry

        lax.fori_loop(j0, j1, body, 0)

    def activate(first, amount, out, slope, tile=64):
        def body(i, carry):
            rows = pl.ds(pl.multiple_of(first + i * tile, tile), tile)
            value = acc[rows, :]
            sigma = jax.nn.sigmoid(value)
            out(rows, (value * sigma).astype(BF16))
            if slope is not None:
                slope[rows, :] = sigma * (1.0 + value * (1.0 - sigma))
            return carry

        lax.fori_loop(0, amount // tile, body, 0)

    def into_x1(rows, value):
        xf1[g, rows, :] = value

    def into_x2(rows, value):
        x2[rows, :] = value

    def next_layer(first, slope):
        st = x_start(1, first, CH)
        activate(first, CH // 2, into_x1, slope)
        x_own(st, "lo")
        activate(first + CH // 2, CH // 2, into_x1, slope)
        x_own(st, "hi")
        return st

    def to_group(src, dst, landed):
        out, got = new_send(landed), new_recv()
        for k in range(1, 8):
            gt = (g + k) % 8
            send(src, dst.at[g], {"xl": gt // 4, "y": gt % 4}, out, got)
        return Recv(got, landed)

    def from_group(own_part, dst):
        total = own_part[...]
        for k in range(1, 8):
            total = total + dst[(g + 8 - k) % 8]
        return total

    def head_send(ch):
        hs[ch] = nt(headt[0:32, :], x2[CH * ch : CH * (ch + 1), :])[0:24, :]
        return to_group(hs.at[ch], hr.at[ch], hr.at[ch, pl.ds(0, 7), :, :])

    def head_loss(ch, got):
        got.wait_recv()
        total = from_group(hs.at[ch], hr.at[ch])
        grad = vtrace(total, misc[ch, 0:24, :], misc[ch, 24:25, :], misc[ch, 25:26, :], misc[ch, 26:27, :])
        tmp[0:24, :] = grad
        rows = slice(CH * ch, CH * (ch + 1))
        og_r[rows, :] = tmp[...].T.astype(BF16)
        pg1[rows, :] = (nn(og_r[rows, :], headt[...]) * slope1[rows, :]).astype(BF16)
        pg1t[:, rows] = pg1[rows, :].T

    where_g = (rel_g(1, 2), rel_g(1, 1), rel_g(1, 3), rel_g(0, 1), rel_g(0, 3), rel_g(0, 2), rel_g(1, 0))

    class Scatter:
        def __init__(self, first, amount, col, cols):
            half = amount // 2
            self.rows = slice(first, first + amount)
            self.lo, self.hi = slice(first, first + half), slice(first + half, first + amount)
            self.cs = slice(col, col + cols)
            self.out = new_send(sb.at[:, self.ds(self.rows), self.ds(self.cs)])
            self.s2 = [Recv(new_recv(), rb.at[pl.ds(0, 2), self.ds(rows), self.ds(self.cs)]) for rows in (self.lo, self.hi)]
            self.last = Recv(new_recv(), rb.at[pl.ds(0, 3), self.ds(self.rows), self.ds(self.cs)])

        def ds(self, rows):
            return pl.ds(rows.start, rows.stop - rows.start)

        def piece(self, block):
            return nt(pg1[self.rows, :], wf1[block, self.cs, :])

        def make(self, k):
            sb[k, self.rows, self.cs] = self.piece(where_g[k]).astype(BF16)

        def push(self, k, rows, device, recv_sem=None):
            where = (k, self.ds(rows), self.ds(self.cs))
            return send(sb.at[where], rb.at[where], device, self.out, recv_sem)

        def add_in(self, k, rows, *terms):
            value = sb[k, rows, self.cs].astype(F32)
            for term in terms:
                value = value + rb[term, rows, self.cs].astype(F32)
            sb[k, rows, self.cs] = value.astype(BF16)

        def first(self):
            self.make(0)
            self.s1 = [self.push(0, self.lo, x_peer), self.push(0, self.hi, x_peer)]

        def make_rest(self):
            self.make(5)
            self.make(6)
            own[self.rows, self.cs] = self.piece(g)

        def push_two(self):
            for i, rows in enumerate((self.lo, self.hi)):
                self.push(1, rows, y_up, self.s2[i].sem)
                self.push(2, rows, y_down, self.s2[i].sem)

        def push_plain(self):
            self.push(3, self.hi, y_up, self.last.sem)
            self.push(4, self.lo, y_down, self.last.sem)

        def rest(self):
            self.make(1)
            self.make(2)
            self.push_two()
            self.make(3)
            self.make(4)
            self.push_plain()
            self.make_rest()

        def prepare(self):
            self.first()
            for k in range(1, 5):
                self.make(k)
            self.make_rest()

        def mid1(self):
            self.s1[0].wait_recv()
            self.add_in(5, self.lo, 0)
            self.s4u = self.push(5, self.lo, y_up)
            self.s1[1].wait_recv()
            self.add_in(5, self.hi, 0)
            self.s4d = self.push(5, self.hi, y_down)

        def mid2(self):
            for i, rows in enumerate((self.lo, self.hi)):
                self.s2[i].wait_recv()
                self.add_in(6, rows, 1, 2)
                self.push(6, rows, x_peer, self.last.sem)

        def mid3(self):
            self.s4u.wait_recv()
            self.add_in(3, self.lo, 5)
            self.push(3, self.lo, y_up, self.last.sem)
            self.s4d.wait_recv()
            self.add_in(4, self.hi, 5)
            self.push(4, self.hi, y_down, self.last.sem)

        def close(self):
            self.last.wait_recv()
            cs = self.cs
            for r in range(self.rows.start, self.rows.stop, 128):
                rows = slice(r, r + 128)
                value = own[rows, cs] + rb[3, rows, cs].astype(F32) + rb[4, rows, cs].astype(F32) + rb[6, rows, cs].astype(F32)
                pg0t[cs, rows] = (value * slope0[rows, cs]).astype(BF16).T

    class Weights:
        def __init__(self, layer, pgt, bufs, col, cols, extra, halves=(0, 1)):
            self.halves = halves
            self.layer, self.pgt, self.extra = layer, pgt, extra
            self.dws, self.dwr, self.q, self.rz1, self.rz2, self.xs, self.rx = bufs
            self.cols, self.size = cols, cols + extra
            self.cs, self.top = slice(col, col + cols), slice(col + cols, col + cols + extra)
            self.all, half = slice(col, col + self.size), col + cols // 2
            self.low, self.high = slice(col, half), slice(half, col + self.size)
            self.base = count[0]
            count[0] += 8
            every = self.ds(self.all)
            self.out = new_send(self.q.at[pl.ds(0, 7), every, :])
            self.give_sem = new_send(self.dws.at[:, every, :])
            self.sums = {xr: Recv(new_recv(), self.rz2.at[xr, :, every, :]) for xr in halves}
            self.st = {}

        def ds(self, rows):
            return pl.ds(rows.start, rows.stop - rows.start)

        def block(self, i):
            return ((xh + 1 - i % 2) % 2) * 4 + (z + 2 + i // 2) % 4

        def copy_of(self, i):
            every = self.ds(self.all)
            return pltpu.make_async_remote_copy(
                src_ref=self.dws.at[i, every, :], dst_ref=self.dwr.at[i, every, :],
                send_sem=self.give_sem, recv_sem=rsem.at[self.base + i],
                device_id=sibling, device_id_type=MESH,
            )

        def head_rows(self, block, core):
            return hgp[pl.ds(pl.multiple_of((2 * block + core) * 32, 32), 32), :]

        def give(self, i0, i1):
            other = pl.multiple_of((1 - c) * WB, WB)

            def body(i, carry):
                block = self.block(i)
                term = nn(self.pgt[self.cs, :], xf[self.layer][block, 0:TR, pl.ds(other, WB)])
                self.dws[i, self.cs, :] = term.astype(BF16)
                if self.extra:
                    self.dws[i, self.top, 0:128] = self.head_rows(block, 1 - c).astype(BF16)
                    self.dws[i, self.top, 128:256] = jnp.zeros((self.extra, 128), BF16)
                self.copy_of(i).start()
                return carry

            lax.fori_loop(i0, i1, body, 0)

        def keep(self, i0, i1):
            q, dwr, cs, top = self.q, self.dwr, self.cs, self.top

            def body(i, carry):
                block = self.block(i)
                term = nn(self.pgt[cs, :], xf[self.layer][block, 0:TR, pl.ds(cb, WB)])
                self.copy_of(i).wait_recv()
                q[i, cs, :] = (term + dwr[i, cs, :].astype(F32)).astype(BF16)
                if self.extra:
                    q[i, top, 0:128] = (self.head_rows(block, c) + dwr[i, top, 0:128].astype(F32)).astype(BF16)
                    q[i, top, 128:256] = jnp.zeros((self.extra, 128), BF16)
                return carry

            lax.fori_loop(i0, i1, body, 0)

        def go(self, i, rows, dst, device, recv_sem=None):
            where = self.ds(rows)
            return send(self.q.at[i, where, :], dst.at[where, :], device, self.out, recv_sem)

        def z_first(self):
            for xr in self.halves:
                self.st["a", xr] = self.go(xr, self.low, self.rz1.at[xr], z_up)
                self.st["b", xr] = self.go(xr, self.high, self.rz1.at[xr], z_down)

        def z_plain(self):
            for xr in self.halves:
                self.go(6 + xr, self.high, self.rz2.at[xr, 0], z_up, self.sums[xr].sem)
                self.go(2 + xr, self.low, self.rz2.at[xr, 1], z_down, self.sums[xr].sem)

        def late(self):
            self.keep(2, 4)
            self.keep(6, 8)
            self.z_plain()
            self.keep(4, 6)

        def z_added(self):
            q, rz1, st = self.q, self.rz1, self.st
            for xr in self.halves:
                for name, i, rows, side, device in (("a", 6, self.low, 0, z_up), ("b", 2, self.high, 1, z_down)):
                    st[name, xr].wait_recv()
                    value = q[i + xr, rows, :].astype(F32) + rz1[xr, rows, :].astype(F32)
                    q[i + xr, rows, :] = value.astype(BF16)
                    self.go(i + xr, rows, self.rz2.at[xr, side], device, self.sums[xr].sem)

        def z_sum(self, xr):
            self.sums[xr].wait_recv()
            every = self.all
            return (
                self.q[4 + xr, every, :].astype(F32)
                + self.rz2[xr, 0, every, :].astype(F32)
                + self.rz2[xr, 1, every, :].astype(F32)
            )

        def cross(self):
            every = self.ds(self.all)
            self.xs[self.all, :] = self.z_sum(0).astype(BF16)
            self.h = send(self.xs.at[every, :], self.rx.at[every, :], h_peer, self.out)

        def result(self):
            value = self.z_sum(1)
            if 0 in self.halves:
                self.h.wait_recv()
                value = value + self.rx[self.all, :].astype(F32)
            dwv[self.layer, :, self.cs] = value[0 : self.cols, :].T
            where = (self.layer, slice(None), self.ds(self.cs))
            store(dwv.at[where], dw_out.at[where])
            if self.extra:
                hgv[...] = value[self.cols :, 0:128].T[0 : ACT + 1, :]
                store(hgv, hg_out)

    loads[0].wait()
    loads[1].wait()
    w0 = w_start(0)
    a0, b0 = x_start(0, 0, CH), x_start(0, CH, CH)
    x_own(a0, "lo")
    x_own(a0, "hi")
    x_own(b0, "lo")
    x_own(b0, "hi")
    for load in loads[2:]:
        load.wait()

    headt[...] = jnp.zeros_like(headt)
    headt[0 : ACT + 1, :] = head[...]
    misc[...] = jnp.zeros_like(misc)
    for r in range(8):
        ch, lane = r // 4, STEPS * (r % 4)
        steps = slice(lane, lane + STEPS - 1)
        misc[ch, 0:ACT, steps] = acting[:, r, :]
        misc[ch, 24:25, steps] = actions[r : r + 1, :].astype(F32)
        misc[ch, 25:26, steps] = rewards[r : r + 1, :]
        misc[ch, 26:27, steps] = finished[r : r + 1, :].astype(F32)
    tmp[...] = jnp.zeros_like(tmp)

    w_fwd1(w0)
    x_fwd1(a0)
    w_fwd2(w0)
    x_fwd1(b0)
    x_fwd2(a0)
    w_fwd3(w0)
    x_fwd3(a0)
    x_fwd2(b0)
    x_fwd3(b0)
    w1 = w_start(1)
    w_finish(w0)
    x_near(a0)
    blocks(0, 0, CH, 1, 5, True)
    x_far(a0)
    blocks(0, 0, CH, 5, 8, False)
    a1 = next_layer(0, slope0)
    w_fwd1(w1)
    x_near(b0)
    blocks(0, CH, CH, 1, 5, True)
    x_far(b0)
    blocks(0, CH, CH, 5, 8, False)
    b1 = next_layer(CH, slope0)

    x_fwd1(a1)
    w_fwd2(w1)
    x_fwd1(b1)
    x_fwd2(a1)
    w_fwd3(w1)
    x_fwd3(a1)
    x_fwd3(b1)
    x_fwd2(b1)
    w_finish(w1)
    x_near(a1)
    blocks(1, 0, CH, 1, 5, True)
    x_far(a1)
    blocks(1, 0, CH, 5, 8, False)
    activate(0, CH, into_x2, slope1)
    head_a = head_send(0)
    c0 = x_start(0, TR, AR)
    x_own(c0, "lo")
    x_own(c0, "hi")
    x_near(b1)
    blocks(1, CH, CH, 1, 5, True)
    x_far(b1)
    blocks(1, CH, CH, 5, 8, False)
    activate(CH, CH, into_x2, slope1)
    head_b = head_send(1)

    da1, da2 = Scatter(0, CH, 0, CH), Scatter(0, CH, CH, CH)
    db1, db2 = Scatter(CH, CH, 0, CH), Scatter(CH, CH, CH, CH)
    g1 = Weights(1, pg1t, (dws1, dwr1, q1, rz1a, rz2a, xs1, rx1), 0, FB, ER - FB)
    bufs0 = (dws0, dwr0, q0, rz1b, rz2b, xs0, rx0)
    g0a = Weights(0, pg0t, bufs0, 0, CH, 0)
    g0b = Weights(0, pg0t, bufs0, CH, CH, 0)
    head_loss(0, head_a)
    da1.first()
    da1.rest()
    x_fwd1(c0)
    da2.prepare()
    head_loss(1, head_b)
    db1.first()
    hgp[...] = tn(x2[0:TR, :], og_r[...])
    g1.give(0, 2)
    db1.rest()
    g1.keep(0, 2)
    g1.z_first()
    da1.mid1()
    da1.mid2()
    g1.give(2, 8)
    db2.prepare()
    db1.mid1()
    x_fwd2(c0)
    x_fwd3(c0)
    g1.keep(2, 4)
    db1.mid2()
    g1.keep(6, 8)
    g1.z_plain()
    da1.mid3()
    g1.keep(4, 6)
    db1.mid3()
    da2.mid1()
    db2.mid1()
    da2.push_two()
    db2.push_two()
    da2.push_plain()
    db2.push_plain()
    g1.z_added()
    x_near(c0)
    x_far(c0)
    blocks(0, TR, AR, 1, 8, True)
    activate(TR, AR, into_x1, None)
    da1.close()
    db1.close()
    g0a.give(0, 2)
    g0a.keep(0, 2)
    g0a.z_first()
    da2.mid3()
    db2.mid3()
    g0a.give(2, 8)
    da2.mid2()
    g0a.keep(2, 4)
    g0a.keep(6, 8)
    g0a.z_plain()
    db2.mid2()
    c1 = x_start(1, TR, AR)
    x_own(c1, "lo")
    x_own(c1, "hi")
    g0a.keep(4, 6)
    g0a.z_added()
    g1.cross()
    da2.close()
    db2.close()
    g0b.give(0, 2)
    g0b.keep(0, 2)
    g0b.z_first()
    x_fwd1(c1)
    x_fwd2(c1)
    g0b.give(2, 8)
    g0b.late()
    x_fwd3(c1)
    x_near(c1)
    blocks(1, TR, AR, 1, 5, True)
    g0b.z_added()
    g0a.cross()
    x_far(c1)
    g0b.cross()
    blocks(1, TR, AR, 5, 8, False)
    activate(TR, AR, into_x2, None)
    ha_s[...] = nt(headt[0:32, :], x2[TR : TR + AR, :])[0:24, :]
    acts = to_group(ha_s, ha_r, ha_r.at[pl.ds(0, 7), :, :])
    g1.result()
    g0a.result()
    acts.wait_recv()
    alv[...] = from_group(ha_s, ha_r)[0:ACT, :]
    store(alv, al_out)
    g0b.result()

    for copy in stores:
        copy.wait()
    for view, sem in sends:
        pltpu.make_async_remote_copy(
            src_ref=view, dst_ref=view, send_sem=sem, recv_sem=rsem.at[0], device_id=x_peer, device_id_type=MESH,
        ).wait_send()
    assert (count[0], count[1]) == (N_RECV, N_SEND), count


def hand_out_kernel(dw, hg, al, dw_out, hg_out, al_out, dwv, hgv, alv, isem, osem):
    views = [(dw.at[p], dwv.at[p], dw_out.at[p]) for p in range(dw.shape[0])]
    views += [(hg, hgv, hg_out), (al, alv, al_out)]
    loads = [pltpu.make_async_copy(a, b, isem.at[i]) for i, (a, b, _) in enumerate(views)]
    stores = [pltpu.make_async_copy(b, o, osem.at[i]) for i, (_, b, o) in enumerate(views)]
    for copy in loads:
        copy.start()
    for load, copy in zip(loads, stores):
        load.wait()
        copy.start()
    for copy in stores:
        copy.wait()


def hand_out(dw, hg, al):
    parts = dw.reshape(4, WB // 2, FB)
    arrays = (parts, hg, al)
    hbm = pl.BlockSpec(memory_space=pltpu.HBM)
    moved, hg, al = pl.pallas_call(
        hand_out_kernel,
        out_shape=tuple(jax.ShapeDtypeStruct(a.shape, a.dtype) for a in arrays),
        in_specs=[hbm] * 3,
        out_specs=(hbm,) * 3,
        scratch_shapes=[pltpu.VMEM(a.shape, a.dtype) for a in arrays]
        + [pltpu.SemaphoreType.DMA((6,)), pltpu.SemaphoreType.DMA((6,))],
        name="hand_out",
    )(*arrays)
    return moved.reshape(dw.shape), hg, al


def per_device(observations, next_observations, trunk_weights, head_weights, acting, actions, rewards, finished):
    v = pltpu.VMEM
    dw_bufs = lambda rows: [
        v((8, rows, WB), BF16), v((8, rows, WB), BF16), v((8, rows, WB), BF16), v((2, rows, WB), BF16),
        v((2, 2, rows, WB), BF16), v((rows, WB), BF16), v((rows, WB), BF16),
    ]
    scratch = [
        v((8, TR + AR, FB), BF16), v((8, TR + AR, FB), BF16), v((8, FB, FB), BF16), v((8, FB, FB), BF16),
        v((TR + AR, FB), F32), v((TR, FB), F32), v((TR, FB), F32), v((TR + AR, FB), BF16),
        v((128, FB), BF16), v((128, CH), F32), v((2, 32, CH), F32),
        v((2, 24, CH), F32), v((2, 8, 24, CH), F32), v((24, 128), F32), v((8, 24, 128), F32),
        v((TR, 128), BF16), v((TR, FB), BF16), v((FB, TR), BF16), v((FB, TR), BF16), v((FB, 128), F32),
        v((7, TR, FB), BF16), v((7, TR, FB), BF16), v((TR, FB), F32),
        *dw_bufs(ER), *dw_bufs(FB),
        v((2, WB, FB), F32), v((ACT + 1, 32), F32), v((ACT, AR), F32),
        v((ACT + 1, FB), BF16), v((ACT, 8, STEPS - 1), F32), v((8, STEPS - 1), jnp.int32), v((8, STEPS - 1), F32),
        v((8, STEPS - 1), jnp.int32),
        pltpu.SemaphoreType.DMA((N_SEND,)), pltpu.SemaphoreType.DMA((N_RECV,)), pltpu.SemaphoreType.DMA((14,)),
    ]
    hbm = pl.BlockSpec(memory_space=pltpu.HBM)
    trunk_grads, head_grads, actor_logits = pl.pallas_call(
        kernel,
        out_shape=(
            jax.ShapeDtypeStruct((2, WB, FB), F32),
            jax.ShapeDtypeStruct((ACT + 1, 32), F32),
            jax.ShapeDtypeStruct((ACT, AR), F32),
        ),
        in_specs=[hbm] * 8,
        out_specs=(hbm, hbm, hbm),
        scratch_shapes=scratch,
        compiler_params=pltpu.CompilerParams(
            collective_id=0, has_side_effects=True, vmem_limit_bytes=62 * 1024 * 1024
        ),
        name="learner_step",
    )(
        observations.reshape(TR, FB), next_observations, trunk_weights, head_weights.T, acting.transpose(2, 0, 1),
        actions, rewards, finished,
    )
    trunk_grads, head_grads, actor_logits = hand_out(trunk_grads, head_grads, actor_logits)
    return trunk_grads, head_grads.T, actor_logits.T


def solution(mesh):
    split = Mesh(mesh.devices.reshape(SIZES), AXES)
    return jax.shard_map(
        per_device,
        mesh=split,
        in_specs=(
            P(DP, None, GROUP),
            P(DP, GROUP),
            P(None, DP, GROUP),
            P(GROUP, None),
            P(DP, None, None),
            P(DP, None),
            P(DP, None),
            P(DP, None),
        ),
        out_specs=(P(None, DP, GROUP), P(GROUP + DP, None), P(DP, None)),
        check_vma=False,
    )
```

```python
import functools

import jax
import jax.numpy as jnp
from jax import lax
from jax.experimental import pallas as pl
from jax.experimental.pallas import tpu as pltpu
from jax.sharding import Mesh
from jax.sharding import PartitionSpec as P

AXES = ("xl", "y", "xh", "z", "c")
SIZES = (2, 4, 2, 4, 2)
DP = ("xh", "z", "c")
GROUP = ("xl", "y")
MESH = pl.DeviceIdType.MESH
F32 = jnp.float32
BF16 = jnp.bfloat16

discount_rate = 0.99
value_weight = 0.5
entropy_weight = 0.1
loss_divisor = 16.0

TR = 512
AR = 128
FB = 512
WB = 256
STEPS = 64
ACT = 18
ER = 544
N_RECV, N_SEND = 148, 21
CH = 256


def nn(a, b):
    return jnp.dot(a, b, preferred_element_type=F32)


def nt(a, b):
    return lax.dot_general(a, b, (((1,), (1,)), ((), ())), preferred_element_type=F32)


def tn(a, b):
    return lax.dot_general(a, b, (((0,), (0,)), ((), ())), preferred_element_type=F32)


def vtrace(logits, behave, action, reward, finished):
    row = lax.broadcasted_iota(jnp.int32, logits.shape, 0)
    step = lax.broadcasted_iota(jnp.int32, reward.shape, 1)
    live = step % STEPS < STEPS - 1
    lanes = reward.shape[1]
    is_act = row < ACT

    def log_softmax(values):
        top = jnp.max(jnp.where(is_act, values, -3.0e38), axis=0, keepdims=True)
        shifted = jnp.where(is_act, values - top, 0.0)
        total = jnp.sum(jnp.where(is_act, jnp.exp(shifted), 0.0), axis=0, keepdims=True)
        return jnp.where(is_act, shifted - jnp.log(total), 0.0)

    log_policy = log_softmax(logits)
    log_behave = log_softmax(behave)
    chosen = jnp.where(row.astype(F32) == action, 1.0, 0.0)
    ratio = jnp.exp(jnp.sum((log_policy - log_behave) * chosen, axis=0, keepdims=True))
    clipped = jnp.minimum(ratio, 1.0)
    discount = discount_rate * (1.0 - finished)
    current = logits[ACT : ACT + 1, :]
    following = pltpu.roll(current, lanes - 1, 1)
    delta = jnp.where(live, clipped * (reward + discount * following - current), 0.0)
    factor = jnp.where(live, discount * clipped, 0.0)
    for shift in (1, 2, 4, 8, 16, 32):
        delta = delta + factor * pltpu.roll(delta, lanes - shift, 1)
        factor = factor * pltpu.roll(factor, lanes - shift, 1)
    targets = current + delta
    next_targets = pltpu.roll(targets, lanes - 1, 1)
    advantage = clipped * (reward + discount * next_targets - current)
    probability = jnp.where(is_act, jnp.exp(log_policy), 0.0)
    entropy = -jnp.sum(probability * log_policy, axis=0, keepdims=True)
    logit_grad = (
        -advantage * (chosen - probability)
        + entropy_weight * probability * (log_policy + entropy)
    ) / loss_divisor
    value_grad = -value_weight * (targets - current) / loss_divisor
    grad = jnp.where(is_act, logit_grad, jnp.where(row == ACT, value_grad, 0.0))
    return jnp.where(live, grad, 0.0)


def kernel(
    obs, nxt, wts, head_in, acting_in, actions_in, rewards_in, finished_in,
    dw_out, hg_out, al_out,
    xf0, xf1, wf0, wf1, acc, slope0, slope1, x2, headt, tmp, misc,
    hs, hr, ha_s, ha_r, og_r, pg1, pg1t, pg0t, hgp,
    sb, rb, own,
    dws1, dwr1, q1, rz1a, rz2a, xs1, rx1,
    dws0, dwr0, q0, rz1b, rz2b, xs0, rx0,
    head, acting, actions, rewards, finished, ssem, rsem, lsem,
):
    xl, y, xh, z, c = (lax.axis_index(a) for a in AXES)
    g = xl * 4 + y
    xf, wf = (xf0, xf1), (wf0, wf1)

    def rel_g(dx, dy):
        return ((xl + dx) % 2) * 4 + (y + dy) % 4

    def rel_w(dx, dz):
        return ((xh + dx) % 2) * 4 + (z + dz) % 4

    x_peer = {"xl": 1 - xl}
    y_up, y_down = {"y": (y + 1) % 4}, {"y": (y + 3) % 4}
    h_peer = {"xh": 1 - xh}
    z_up, z_down = {"z": (z + 1) % 4}, {"z": (z + 3) % 4}
    sibling = {"c": 1 - c}

    count = [0, 0]
    sends = []

    def new_recv():
        count[0] += 1
        return rsem.at[count[0] - 1]

    def new_send(view):
        count[1] += 1
        sem = ssem.at[count[1] - 1]
        sends.append((view, sem))
        return sem

    class Recv:
        def __init__(self, sem, view):
            self.sem, self.view = sem, view

        def wait_recv(self):
            pltpu.make_async_remote_copy(
                src_ref=self.view, dst_ref=self.view, send_sem=ssem.at[0], recv_sem=self.sem,
                device_id=x_peer, device_id_type=MESH,
            ).wait_recv()

    def send(src, dst, device, send_sem, recv_sem=None):
        copy = pltpu.make_async_remote_copy(
            src_ref=src, dst_ref=dst, send_sem=send_sem, recv_sem=new_recv() if recv_sem is None else recv_sem,
            device_id=device, device_id_type=MESH,
        )
        copy.start()
        return copy

    cb = pl.multiple_of(c * WB, WB)
    wg = xh * 4 + z
    loads = [
        pltpu.make_async_copy(obs, xf0.at[g, pl.ds(0, TR), :], lsem.at[0]),
        pltpu.make_async_copy(wts.at[0], wf0.at[wg, pl.ds(cb, WB), :], lsem.at[1]),
        pltpu.make_async_copy(wts.at[1], wf1.at[wg, pl.ds(cb, WB), :], lsem.at[2]),
        pltpu.make_async_copy(nxt, xf0.at[g, pl.ds(TR, AR), :], lsem.at[3]),
        pltpu.make_async_copy(head_in, head, lsem.at[4]),
        pltpu.make_async_copy(acting_in, acting, lsem.at[5]),
        pltpu.make_async_copy(actions_in, actions, lsem.at[6]),
        pltpu.make_async_copy(rewards_in, rewards, lsem.at[7]),
        pltpu.make_async_copy(finished_in, finished, lsem.at[8]),
    ]
    for load in loads:
        load.start()

    barrier = pltpu.get_barrier_semaphore()
    friends = [x_peer, y_up, y_down, h_peer, z_up, z_down, sibling]
    for friend in friends:
        pl.semaphore_signal(barrier, inc=1, device_id=friend, device_id_type=MESH)
    pl.semaphore_wait(barrier, len(friends))

    def x_start(layer, first, amount):
        buf, half = xf[layer], amount // 2
        lo, hi = pl.ds(first, half), pl.ds(first + half, half)

        out = new_send(buf.at[pl.ds(0, 7), pl.ds(0, amount), :])

        def go(block, rows, device, recv_sem=None):
            return send(buf.at[block, rows, :], buf.at[block, rows, :], device, out, recv_sem)

        near = Recv(new_recv(), buf.at[0, pl.ds(0, amount), :])
        far = Recv(new_recv(), buf.at[pl.ds(0, 3), pl.ds(0, amount), :])
        return {"go": go, "lo": lo, "hi": hi, "near": near, "far": far}

    def x_own(st, rows):
        go, lo = st["go"], st["lo"]
        if rows == "lo":
            st["up_lo"] = go(g, lo, y_up)
            st["x_lo"] = go(g, lo, x_peer)
        else:
            st["dn_hi"] = go(g, st["hi"], y_down)
            st["x_hi"] = go(g, st["hi"], x_peer)
            go(g, st["hi"], y_up, st["near"].sem)
            go(g, lo, y_down, st["near"].sem)

    def x_fwd1(st):
        go = st["go"]
        st["up_lo"].wait_recv()
        st["f_lo"] = go(rel_g(0, 3), st["lo"], y_up)
        st["dn_hi"].wait_recv()
        st["f_hi"] = go(rel_g(0, 1), st["hi"], y_down)

    def x_fwd2(st):
        go, block, far = st["go"], rel_g(1, 0), st["far"].sem
        st["x_lo"].wait_recv()
        go(block, st["lo"], y_up, far)
        go(block, st["lo"], y_down, far)
        st["x_hi"].wait_recv()
        go(block, st["hi"], y_up, far)
        go(block, st["hi"], y_down, far)

    def x_fwd3(st):
        go, block, far = st["go"], rel_g(0, 2), st["far"].sem
        st["f_lo"].wait_recv()
        go(block, st["lo"], x_peer, far)
        st["f_hi"].wait_recv()
        go(block, st["hi"], x_peer, far)

    def x_near(st):
        st["near"].wait_recv()

    def x_far(st):
        st["far"].wait_recv()

    half_w = WB // 2

    def w_piece(block, part):
        if part == "all":
            return (block, pl.ds(cb, WB), slice(None))
        start = cb if part == "lo" else cb + half_w
        return (block, pl.ds(pl.multiple_of(start, half_w), half_w), slice(None))

    def w_start(layer):
        buf = wf[layer]

        out = new_send(xf[layer].at[pl.ds(0, 6), :, :])

        def go(block, part, device, recv_sem=None):
            where = w_piece(block, part)
            return send(buf.at[where], buf.at[where], device, out, recv_sem)

        st = {"go": go}
        st["f"] = Recv(new_recv(), buf.at[0, pl.ds(0, WB), :])
        st["g"] = Recv(new_recv(), buf.at[0, pl.ds(0, WB), :])
        st["sib"] = Recv(new_recv(), buf.at[pl.ds(0, 4), :, :])
        st["up_lo"] = go(wg, "lo", z_up)
        st["dn_hi"] = go(wg, "hi", z_down)
        st["h"] = go(wg, "all", h_peer)
        st["up_hi"] = go(wg, "hi", z_up)
        st["dn_lo"] = go(wg, "lo", z_down)
        w_share(st, wg)
        return st

    def w_share(st, block):
        st["go"](block, "all", sibling, st["sib"].sem)

    def w_fwd1(st):
        go = st["go"]
        st["up_lo"].wait_recv()
        go(rel_w(0, 3), "lo", z_up, st["f"].sem)
        st["dn_hi"].wait_recv()
        go(rel_w(0, 1), "hi", z_down, st["f"].sem)

    def w_fwd2(st):
        go, far = st["go"], rel_w(1, 0)
        st["h"].wait_recv()
        st["h_up_lo"] = go(far, "lo", z_up)
        st["h_dn_hi"] = go(far, "hi", z_down)
        st["h_up_hi"] = go(far, "hi", z_up)
        st["h_dn_lo"] = go(far, "lo", z_down)
        w_share(st, far)
        st["up_hi"].wait_recv()
        w_share(st, rel_w(0, 3))
        st["dn_lo"].wait_recv()
        w_share(st, rel_w(0, 1))

    def w_fwd3(st):
        go = st["go"]
        st["h_up_lo"].wait_recv()
        go(rel_w(1, 3), "lo", z_up, st["g"].sem)
        st["h_dn_hi"].wait_recv()
        go(rel_w(1, 1), "hi", z_down, st["g"].sem)
        st["f"].wait_recv()
        w_share(st, rel_w(0, 2))

    def w_finish(st):
        st["h_up_hi"].wait_recv()
        w_share(st, rel_w(1, 3))
        st["h_dn_lo"].wait_recv()
        w_share(st, rel_w(1, 1))
        st["g"].wait_recv()
        w_share(st, rel_w(1, 2))
        st["sib"].wait_recv()

    def blocks(layer, first, amount, j0, j1, fresh):
        buf, weights = xf[layer], wf[layer]
        rows = slice(first, first + amount)
        if fresh:
            acc[rows, :] = nn(buf[g, rows, :], weights[g])

        def body(j, carry):
            block = ((xl + j // 4) % 2) * 4 + (y + j % 4) % 4
            acc[rows, :] += nn(buf[block, rows, :], weights[block])
            return carry

        lax.fori_loop(j0, j1, body, 0)

    def activate(first, amount, out, slope, tile=64):
        def body(i, carry):
            rows = pl.ds(pl.multiple_of(first + i * tile, tile), tile)
            value = acc[rows, :]
            sigma = jax.nn.sigmoid(value)
            out(rows, (value * sigma).astype(BF16))
            if slope is not None:
                slope[rows, :] = sigma * (1.0 + value * (1.0 - sigma))
            return carry

        lax.fori_loop(0, amount // tile, body, 0)

    def into_x1(rows, value):
        xf1[g, rows, :] = value

    def into_x2(rows, value):
        x2[rows, :] = value

    def next_layer(first, slope):
        st = x_start(1, first, CH)
        activate(first, CH // 2, into_x1, slope)
        x_own(st, "lo")
        activate(first + CH // 2, CH // 2, into_x1, slope)
        x_own(st, "hi")
        return st

    def to_group(src, dst, landed):
        out, got = new_send(landed), new_recv()
        for k in range(1, 8):
            gt = (g + k) % 8
            send(src, dst.at[g], {"xl": gt // 4, "y": gt % 4}, out, got)
        return Recv(got, landed)

    def from_group(own_part, dst):
        total = own_part[...]
        for k in range(1, 8):
            total = total + dst[(g + 8 - k) % 8]
        return total

    def head_send(ch):
        hs[ch] = nt(headt[0:32, :], x2[CH * ch : CH * (ch + 1), :])[0:24, :]
        return to_group(hs.at[ch], hr.at[ch], hr.at[ch, pl.ds(0, 7), :, :])

    def head_loss(ch, got):
        got.wait_recv()
        total = from_group(hs.at[ch], hr.at[ch])
        grad = vtrace(total, misc[ch, 0:24, :], misc[ch, 24:25, :], misc[ch, 25:26, :], misc[ch, 26:27, :])
        tmp[0:24, :] = grad
        rows = slice(CH * ch, CH * (ch + 1))
        og_r[rows, :] = tmp[...].T.astype(BF16)
        pg1[rows, :] = (nn(og_r[rows, :], headt[...]) * slope1[rows, :]).astype(BF16)
        pg1t[:, rows] = pg1[rows, :].T

    where_g = (rel_g(1, 2), rel_g(1, 1), rel_g(1, 3), rel_g(0, 1), rel_g(0, 3), rel_g(0, 2), rel_g(1, 0))

    class Scatter:
        def __init__(self, first, amount, col, cols):
            half = amount // 2
            self.rows = slice(first, first + amount)
            self.lo, self.hi = slice(first, first + half), slice(first + half, first + amount)
            self.cs = slice(col, col + cols)
            self.out = new_send(sb.at[:, self.ds(self.rows), self.ds(self.cs)])
            self.s2 = [Recv(new_recv(), rb.at[pl.ds(0, 2), self.ds(rows), self.ds(self.cs)]) for rows in (self.lo, self.hi)]
            self.last = Recv(new_recv(), rb.at[pl.ds(0, 3), self.ds(self.rows), self.ds(self.cs)])

        def ds(self, rows):
            return pl.ds(rows.start, rows.stop - rows.start)

        def piece(self, block):
            return nt(pg1[self.rows, :], wf1[block, self.cs, :])

        def make(self, k):
            sb[k, self.rows, self.cs] = self.piece(where_g[k]).astype(BF16)

        def push(self, k, rows, device, recv_sem=None):
            where = (k, self.ds(rows), self.ds(self.cs))
            return send(sb.at[where], rb.at[where], device, self.out, recv_sem)

        def add_in(self, k, rows, *terms):
            value = sb[k, rows, self.cs].astype(F32)
            for term in terms:
                value = value + rb[term, rows, self.cs].astype(F32)
            sb[k, rows, self.cs] = value.astype(BF16)

        def first(self):
            self.make(0)
            self.s1 = [self.push(0, self.lo, x_peer), self.push(0, self.hi, x_peer)]

        def make_rest(self):
            self.make(5)
            self.make(6)
            own[self.rows, self.cs] = self.piece(g)

        def push_two(self):
            for i, rows in enumerate((self.lo, self.hi)):
                self.push(1, rows, y_up, self.s2[i].sem)
                self.push(2, rows, y_down, self.s2[i].sem)

        def push_plain(self):
            self.push(3, self.hi, y_up, self.last.sem)
            self.push(4, self.lo, y_down, self.last.sem)

        def rest(self):
            self.make(1)
            self.make(2)
            self.push_two()
            self.make(3)
            self.make(4)
            self.push_plain()
            self.make_rest()

        def prepare(self):
            self.first()
            for k in range(1, 5):
                self.make(k)
            self.make_rest()

        def mid1(self):
            self.s1[0].wait_recv()
            self.add_in(5, self.lo, 0)
            self.s4u = self.push(5, self.lo, y_up)
            self.s1[1].wait_recv()
            self.add_in(5, self.hi, 0)
            self.s4d = self.push(5, self.hi, y_down)

        def mid2(self):
            for i, rows in enumerate((self.lo, self.hi)):
                self.s2[i].wait_recv()
                self.add_in(6, rows, 1, 2)
                self.push(6, rows, x_peer, self.last.sem)

        def mid3(self):
            self.s4u.wait_recv()
            self.add_in(3, self.lo, 5)
            self.push(3, self.lo, y_up, self.last.sem)
            self.s4d.wait_recv()
            self.add_in(4, self.hi, 5)
            self.push(4, self.hi, y_down, self.last.sem)

        def close(self):
            self.last.wait_recv()
            cs = self.cs
            for r in range(self.rows.start, self.rows.stop, 128):
                rows = slice(r, r + 128)
                value = own[rows, cs] + rb[3, rows, cs].astype(F32) + rb[4, rows, cs].astype(F32) + rb[6, rows, cs].astype(F32)
                pg0t[cs, rows] = (value * slope0[rows, cs]).astype(BF16).T

    class Weights:
        def __init__(self, layer, pgt, bufs, col, cols, extra, halves=(0, 1)):
            self.halves = halves
            self.layer, self.pgt, self.extra = layer, pgt, extra
            self.dws, self.dwr, self.q, self.rz1, self.rz2, self.xs, self.rx = bufs
            self.cols, self.size = cols, cols + extra
            self.cs, self.top = slice(col, col + cols), slice(col + cols, col + cols + extra)
            self.all, half = slice(col, col + self.size), col + cols // 2
            self.low, self.high = slice(col, half), slice(half, col + self.size)
            self.base = count[0]
            count[0] += 8
            every = self.ds(self.all)
            self.out = new_send(self.q.at[pl.ds(0, 7), every, :])
            self.give_sem = new_send(self.dws.at[:, every, :])
            self.sums = {xr: Recv(new_recv(), self.rz2.at[xr, :, every, :]) for xr in halves}
            self.st = {}

        def ds(self, rows):
            return pl.ds(rows.start, rows.stop - rows.start)

        def block(self, i):
            return ((xh + 1 - i % 2) % 2) * 4 + (z + 2 + i // 2) % 4

        def copy_of(self, i):
            every = self.ds(self.all)
            return pltpu.make_async_remote_copy(
                src_ref=self.dws.at[i, every, :], dst_ref=self.dwr.at[i, every, :],
                send_sem=self.give_sem, recv_sem=rsem.at[self.base + i],
                device_id=sibling, device_id_type=MESH,
            )

        def head_rows(self, block, core):
            return hgp[pl.ds(pl.multiple_of((2 * block + core) * 32, 32), 32), :]

        def give(self, i0, i1):
            other = pl.multiple_of((1 - c) * WB, WB)

            def body(i, carry):
                block = self.block(i)
                term = nn(self.pgt[self.cs, :], xf[self.layer][block, 0:TR, pl.ds(other, WB)])
                self.dws[i, self.cs, :] = term.astype(BF16)
                if self.extra:
                    self.dws[i, self.top, 0:128] = self.head_rows(block, 1 - c).astype(BF16)
                    self.dws[i, self.top, 128:256] = jnp.zeros((self.extra, 128), BF16)
                self.copy_of(i).start()
                return carry

            lax.fori_loop(i0, i1, body, 0)

        def keep(self, i0, i1):
            q, dwr, cs, top = self.q, self.dwr, self.cs, self.top

            def body(i, carry):
                block = self.block(i)
                term = nn(self.pgt[cs, :], xf[self.layer][block, 0:TR, pl.ds(cb, WB)])
                self.copy_of(i).wait_recv()
                q[i, cs, :] = (term + dwr[i, cs, :].astype(F32)).astype(BF16)
                if self.extra:
                    q[i, top, 0:128] = (self.head_rows(block, c) + dwr[i, top, 0:128].astype(F32)).astype(BF16)
                    q[i, top, 128:256] = jnp.zeros((self.extra, 128), BF16)
                return carry

            lax.fori_loop(i0, i1, body, 0)

        def go(self, i, rows, dst, device, recv_sem=None):
            where = self.ds(rows)
            return send(self.q.at[i, where, :], dst.at[where, :], device, self.out, recv_sem)

        def z_first(self):
            for xr in self.halves:
                self.st["a", xr] = self.go(xr, self.low, self.rz1.at[xr], z_up)
                self.st["b", xr] = self.go(xr, self.high, self.rz1.at[xr], z_down)

        def z_plain(self):
            for xr in self.halves:
                self.go(6 + xr, self.high, self.rz2.at[xr, 0], z_up, self.sums[xr].sem)
                self.go(2 + xr, self.low, self.rz2.at[xr, 1], z_down, self.sums[xr].sem)

        def late(self):
            self.keep(2, 4)
            self.keep(6, 8)
            self.z_plain()
            self.keep(4, 6)

        def z_added(self):
            q, rz1, st = self.q, self.rz1, self.st
            for xr in self.halves:
                for name, i, rows, side, device in (("a", 6, self.low, 0, z_up), ("b", 2, self.high, 1, z_down)):
                    st[name, xr].wait_recv()
                    value = q[i + xr, rows, :].astype(F32) + rz1[xr, rows, :].astype(F32)
                    q[i + xr, rows, :] = value.astype(BF16)
                    self.go(i + xr, rows, self.rz2.at[xr, side], device, self.sums[xr].sem)

        def z_sum(self, xr):
            self.sums[xr].wait_recv()
            every = self.all
            return (
                self.q[4 + xr, every, :].astype(F32)
                + self.rz2[xr, 0, every, :].astype(F32)
                + self.rz2[xr, 1, every, :].astype(F32)
            )

        def cross(self):
            every = self.ds(self.all)
            self.xs[self.all, :] = self.z_sum(0).astype(BF16)
            self.h = send(self.xs.at[every, :], self.rx.at[every, :], h_peer, self.out)

        def result(self):
            value = self.z_sum(1)
            if 0 in self.halves:
                self.h.wait_recv()
                value = value + self.rx[self.all, :].astype(F32)
            dw_out[self.layer, :, self.cs] = value[0 : self.cols, :].T
            if self.extra:
                hg_out[...] = value[self.cols :, 0:128].T[0 : ACT + 1, :]

    loads[0].wait()
    loads[1].wait()
    w0 = w_start(0)
    a0, b0 = x_start(0, 0, CH), x_start(0, CH, CH)
    x_own(a0, "lo")
    x_own(a0, "hi")
    x_own(b0, "lo")
    x_own(b0, "hi")
    for load in loads[2:]:
        load.wait()

    headt[...] = jnp.zeros_like(headt)
    headt[0 : ACT + 1, :] = head[...]
    misc[...] = jnp.zeros_like(misc)
    for r in range(8):
        ch, lane = r // 4, STEPS * (r % 4)
        steps = slice(lane, lane + STEPS - 1)
        misc[ch, 0:ACT, steps] = acting[:, r, :]
        misc[ch, 24:25, steps] = actions[r : r + 1, :].astype(F32)
        misc[ch, 25:26, steps] = rewards[r : r + 1, :]
        misc[ch, 26:27, steps] = finished[r : r + 1, :].astype(F32)
    tmp[...] = jnp.zeros_like(tmp)

    w_fwd1(w0)
    x_fwd1(a0)
    w_fwd2(w0)
    x_fwd1(b0)
    x_fwd2(a0)
    w_fwd3(w0)
    x_fwd3(a0)
    x_fwd2(b0)
    x_fwd3(b0)
    w1 = w_start(1)
    w_finish(w0)
    x_near(a0)
    blocks(0, 0, CH, 1, 5, True)
    x_far(a0)
    blocks(0, 0, CH, 5, 8, False)
    a1 = next_layer(0, slope0)
    w_fwd1(w1)
    x_near(b0)
    blocks(0, CH, CH, 1, 5, True)
    x_far(b0)
    blocks(0, CH, CH, 5, 8, False)
    b1 = next_layer(CH, slope0)

    x_fwd1(a1)
    w_fwd2(w1)
    x_fwd1(b1)
    x_fwd2(a1)
    w_fwd3(w1)
    x_fwd3(a1)
    x_fwd3(b1)
    x_fwd2(b1)
    w_finish(w1)
    x_near(a1)
    blocks(1, 0, CH, 1, 5, True)
    x_far(a1)
    blocks(1, 0, CH, 5, 8, False)
    activate(0, CH, into_x2, slope1)
    head_a = head_send(0)
    c0 = x_start(0, TR, AR)
    x_own(c0, "lo")
    x_own(c0, "hi")
    x_near(b1)
    blocks(1, CH, CH, 1, 5, True)
    x_far(b1)
    blocks(1, CH, CH, 5, 8, False)
    activate(CH, CH, into_x2, slope1)
    head_b = head_send(1)

    da1, da2 = Scatter(0, CH, 0, CH), Scatter(0, CH, CH, CH)
    db1, db2 = Scatter(CH, CH, 0, CH), Scatter(CH, CH, CH, CH)
    g1 = Weights(1, pg1t, (dws1, dwr1, q1, rz1a, rz2a, xs1, rx1), 0, FB, ER - FB)
    bufs0 = (dws0, dwr0, q0, rz1b, rz2b, xs0, rx0)
    g0a = Weights(0, pg0t, bufs0, 0, CH, 0)
    g0b = Weights(0, pg0t, bufs0, CH, CH, 0)
    head_loss(0, head_a)
    da1.first()
    da1.rest()
    x_fwd1(c0)
    da2.prepare()
    head_loss(1, head_b)
    db1.first()
    hgp[...] = tn(x2[0:TR, :], og_r[...])
    g1.give(0, 2)
    db1.rest()
    g1.keep(0, 2)
    g1.z_first()
    da1.mid1()
    da1.mid2()
    g1.give(2, 8)
    db2.prepare()
    db1.mid1()
    x_fwd2(c0)
    x_fwd3(c0)
    g1.keep(2, 4)
    db1.mid2()
    g1.keep(6, 8)
    g1.z_plain()
    da1.mid3()
    g1.keep(4, 6)
    db1.mid3()
    da2.mid1()
    db2.mid1()
    da2.push_two()
    db2.push_two()
    da2.push_plain()
    db2.push_plain()
    g1.z_added()
    x_near(c0)
    x_far(c0)
    blocks(0, TR, AR, 1, 8, True)
    activate(TR, AR, into_x1, None)
    da1.close()
    db1.close()
    g0a.give(0, 2)
    g0a.keep(0, 2)
    g0a.z_first()
    da2.mid3()
    db2.mid3()
    g0a.give(2, 8)
    da2.mid2()
    g0a.keep(2, 4)
    g0a.keep(6, 8)
    g0a.z_plain()
    db2.mid2()
    c1 = x_start(1, TR, AR)
    x_own(c1, "lo")
    x_own(c1, "hi")
    g0a.keep(4, 6)
    g0a.z_added()
    g1.cross()
    da2.close()
    db2.close()
    g0b.give(0, 2)
    g0b.keep(0, 2)
    g0b.z_first()
    x_fwd1(c1)
    x_fwd2(c1)
    g0b.give(2, 8)
    g0b.late()
    x_fwd3(c1)
    g0b.z_added()
    g0a.cross()
    x_near(c1)
    blocks(1, TR, AR, 1, 5, True)
    x_far(c1)
    blocks(1, TR, AR, 5, 8, False)
    activate(TR, AR, into_x2, None)
    ha_s[...] = nt(headt[0:32, :], x2[TR : TR + AR, :])[0:24, :]
    acts = to_group(ha_s, ha_r, ha_r.at[pl.ds(0, 7), :, :])
    g0b.cross()
    g1.result()
    g0a.result()
    acts.wait_recv()
    al_out[...] = from_group(ha_s, ha_r)[0:ACT, :]
    g0b.result()

    for view, sem in sends:
        pltpu.make_async_remote_copy(
            src_ref=view, dst_ref=view, send_sem=sem, recv_sem=rsem.at[0], device_id=x_peer, device_id_type=MESH,
        ).wait_send()
    assert (count[0], count[1]) == (N_RECV, N_SEND), count


def hand_out_kernel(dw, hg, al, dw_out, hg_out, al_out, sems):
    copies = [pltpu.make_async_copy(a, b, sems.at[i]) for i, (a, b) in enumerate(((dw, dw_out), (hg, hg_out), (al, al_out)))]
    for copy in copies:
        copy.start()
    for copy in copies:
        copy.wait()


def hand_out(*arrays):
    arrays = [pltpu.with_memory_space_constraint(a, pltpu.VMEM) for a in arrays]
    hbm = pl.BlockSpec(memory_space=pltpu.HBM)
    return pl.pallas_call(
        hand_out_kernel,
        out_shape=tuple(jax.ShapeDtypeStruct(a.shape, a.dtype) for a in arrays),
        in_specs=[pl.BlockSpec(memory_space=pltpu.VMEM)] * 3,
        out_specs=(hbm,) * 3,
        scratch_shapes=[pltpu.SemaphoreType.DMA((3,))],
        name="hand_out",
    )(*arrays)


def per_device(observations, next_observations, trunk_weights, head_weights, acting, actions, rewards, finished):
    v = pltpu.VMEM
    dw_bufs = lambda rows: [
        v((8, rows, WB), BF16), v((8, rows, WB), BF16), v((8, rows, WB), BF16), v((2, rows, WB), BF16),
        v((2, 2, rows, WB), BF16), v((rows, WB), BF16), v((rows, WB), BF16),
    ]
    scratch = [
        v((8, TR + AR, FB), BF16), v((8, TR + AR, FB), BF16), v((8, FB, FB), BF16), v((8, FB, FB), BF16),
        v((TR + AR, FB), F32), v((TR, FB), F32), v((TR, FB), F32), v((TR + AR, FB), BF16),
        v((128, FB), BF16), v((128, CH), F32), v((2, 32, CH), F32),
        v((2, 24, CH), F32), v((2, 8, 24, CH), F32), v((24, 128), F32), v((8, 24, 128), F32),
        v((TR, 128), BF16), v((TR, FB), BF16), v((FB, TR), BF16), v((FB, TR), BF16), v((FB, 128), F32),
        v((7, TR, FB), BF16), v((7, TR, FB), BF16), v((TR, FB), F32),
        *dw_bufs(ER), *dw_bufs(FB),
        v((ACT + 1, FB), BF16), v((ACT, 8, STEPS - 1), F32), v((8, STEPS - 1), jnp.int32), v((8, STEPS - 1), F32),
        v((8, STEPS - 1), jnp.int32),
        pltpu.SemaphoreType.DMA((N_SEND,)), pltpu.SemaphoreType.DMA((N_RECV,)), pltpu.SemaphoreType.DMA((9,)),
    ]
    hbm = pl.BlockSpec(memory_space=pltpu.HBM)
    vm = pl.BlockSpec(memory_space=pltpu.VMEM)
    trunk_grads, head_grads, actor_logits = pl.pallas_call(
        kernel,
        out_shape=(
            pltpu.VMEM((2, WB, FB), F32),
            pltpu.VMEM((ACT + 1, 32), F32),
            pltpu.VMEM((ACT, AR), F32),
        ),
        in_specs=[hbm] * 8,
        out_specs=(vm,) * 3,
        scratch_shapes=scratch,
        compiler_params=pltpu.CompilerParams(
            collective_id=0, has_side_effects=True, vmem_limit_bytes=58 * 1024 * 1024
        ),
        name="learner_step",
    )(
        observations.reshape(TR, FB), next_observations, trunk_weights, head_weights.T, acting.transpose(2, 0, 1),
        actions, rewards, finished,
    )
    trunk_grads, head_grads, actor_logits = hand_out(trunk_grads, head_grads, actor_logits)
    return trunk_grads, head_grads.T, actor_logits.T


def solution(mesh):
    split = Mesh(mesh.devices.reshape(SIZES), AXES)
    return jax.shard_map(
        per_device,
        mesh=split,
        in_specs=(
            P(DP, None, GROUP),
            P(DP, GROUP),
            P(None, DP, GROUP),
            P(GROUP, None),
            P(DP, None, None),
            P(DP, None),
            P(DP, None),
            P(DP, None),
        ),
        out_specs=(P(None, DP, GROUP), P(GROUP + DP, None), P(DP, None)),
        check_vma=False,
    )
```

```python
import functools

import jax
import jax.numpy as jnp
from jax import lax
from jax.experimental import pallas as pl
from jax.experimental.pallas import tpu as pltpu
from jax.sharding import Mesh
from jax.sharding import PartitionSpec as P

AXES = ("xl", "y", "xh", "z", "c")
SIZES = (2, 4, 2, 4, 2)
DP = ("xh", "z", "c")
GROUP = ("xl", "y")
MESH = pl.DeviceIdType.MESH
F32 = jnp.float32
BF16 = jnp.bfloat16

discount_rate = 0.99
value_weight = 0.5
entropy_weight = 0.1
loss_divisor = 16.0

TR = 512
AR = 128
FB = 512
WB = 256
STEPS = 64
ACT = 18
ER = 544
N_RECV, N_SEND = 112, 21
CH = 256


def nn(a, b):
    return jnp.dot(a, b, preferred_element_type=F32)


def nt(a, b):
    return lax.dot_general(a, b, (((1,), (1,)), ((), ())), preferred_element_type=F32)


def tn(a, b):
    return lax.dot_general(a, b, (((0,), (0,)), ((), ())), preferred_element_type=F32)


def vtrace(logits, behave, action, reward, finished):
    row = lax.broadcasted_iota(jnp.int32, logits.shape, 0)
    step = lax.broadcasted_iota(jnp.int32, reward.shape, 1)
    live = step % STEPS < STEPS - 1
    lanes = reward.shape[1]
    is_act = row < ACT

    def log_softmax(values):
        top = jnp.max(jnp.where(is_act, values, -3.0e38), axis=0, keepdims=True)
        shifted = jnp.where(is_act, values - top, 0.0)
        total = jnp.sum(jnp.where(is_act, jnp.exp(shifted), 0.0), axis=0, keepdims=True)
        return jnp.where(is_act, shifted - jnp.log(total), 0.0)

    log_policy = log_softmax(logits)
    log_behave = log_softmax(behave)
    chosen = jnp.where(row.astype(F32) == action, 1.0, 0.0)
    ratio = jnp.exp(jnp.sum((log_policy - log_behave) * chosen, axis=0, keepdims=True))
    clipped = jnp.minimum(ratio, 1.0)
    discount = discount_rate * (1.0 - finished)
    current = logits[ACT : ACT + 1, :]
    following = pltpu.roll(current, lanes - 1, 1)
    delta = jnp.where(live, clipped * (reward + discount * following - current), 0.0)
    factor = jnp.where(live, discount * clipped, 0.0)
    for shift in (1, 2, 4, 8, 16, 32):
        delta = delta + factor * pltpu.roll(delta, lanes - shift, 1)
        factor = factor * pltpu.roll(factor, lanes - shift, 1)
    targets = current + delta
    next_targets = pltpu.roll(targets, lanes - 1, 1)
    advantage = clipped * (reward + discount * next_targets - current)
    probability = jnp.where(is_act, jnp.exp(log_policy), 0.0)
    entropy = -jnp.sum(probability * log_policy, axis=0, keepdims=True)
    logit_grad = (
        -advantage * (chosen - probability)
        + entropy_weight * probability * (log_policy + entropy)
    ) / loss_divisor
    value_grad = -value_weight * (targets - current) / loss_divisor
    grad = jnp.where(is_act, logit_grad, jnp.where(row == ACT, value_grad, 0.0))
    return jnp.where(live, grad, 0.0)


def kernel(
    obs, nxt, wts, head_in, acting_in, actions_in, rewards_in, finished_in,
    dw_out, hg_out, al_out,
    xf0, xf1, wf0, wf1, acc, slope0, slope1, x2, headt, tmp, misc,
    hs, hr, ha_s, ha_r, og_r, pg1, pg1t, pg0t, hgp,
    sb, rb, own,
    dws1, dwr1, q1, rz1a, rz2a, xs1, rx1,
    dws0, dwr0, q0, rz1b, rz2b, xs0, rx0,
    head, acting, actions, rewards, finished, ssem, rsem, lsem,
):
    xl, y, xh, z, c = (lax.axis_index(a) for a in AXES)
    g = xl * 4 + y
    xf, wf = (xf0, xf1), (wf0, wf1)

    def rel_g(dx, dy):
        return ((xl + dx) % 2) * 4 + (y + dy) % 4

    def rel_w(dx, dz):
        return ((xh + dx) % 2) * 4 + (z + dz) % 4

    x_peer = {"xl": 1 - xl}
    y_up, y_down = {"y": (y + 1) % 4}, {"y": (y + 3) % 4}
    h_peer = {"xh": 1 - xh}
    z_up, z_down = {"z": (z + 1) % 4}, {"z": (z + 3) % 4}
    sibling = {"c": 1 - c}

    count = [0, 0]
    sends = []

    def new_recv():
        count[0] += 1
        return rsem.at[count[0] - 1]

    def new_send(view):
        count[1] += 1
        sem = ssem.at[count[1] - 1]
        sends.append((view, sem))
        return sem

    class Recv:
        def __init__(self, sem, view):
            self.sem, self.view = sem, view

        def wait_recv(self):
            pltpu.make_async_remote_copy(
                src_ref=self.view, dst_ref=self.view, send_sem=ssem.at[0], recv_sem=self.sem,
                device_id=x_peer, device_id_type=MESH,
            ).wait_recv()

    def send(src, dst, device, send_sem, recv_sem=None):
        copy = pltpu.make_async_remote_copy(
            src_ref=src, dst_ref=dst, send_sem=send_sem, recv_sem=new_recv() if recv_sem is None else recv_sem,
            device_id=device, device_id_type=MESH,
        )
        copy.start()
        return copy

    cb = pl.multiple_of(c * WB, WB)
    wg = xh * 4 + z
    loads = [
        pltpu.make_async_copy(obs, xf0.at[g, pl.ds(0, TR), :], lsem.at[0]),
        pltpu.make_async_copy(wts.at[0], wf0.at[wg, pl.ds(cb, WB), :], lsem.at[1]),
        pltpu.make_async_copy(wts.at[1], wf1.at[wg, pl.ds(cb, WB), :], lsem.at[2]),
        pltpu.make_async_copy(nxt, xf0.at[g, pl.ds(TR, AR), :], lsem.at[3]),
        pltpu.make_async_copy(head_in, head, lsem.at[4]),
        pltpu.make_async_copy(acting_in, acting, lsem.at[5]),
        pltpu.make_async_copy(actions_in, actions, lsem.at[6]),
        pltpu.make_async_copy(rewards_in, rewards, lsem.at[7]),
        pltpu.make_async_copy(finished_in, finished, lsem.at[8]),
    ]
    for load in loads:
        load.start()

    barrier = pltpu.get_barrier_semaphore()
    friends = [x_peer, y_up, y_down, h_peer, z_up, z_down, sibling]
    for friend in friends:
        pl.semaphore_signal(barrier, inc=1, device_id=friend, device_id_type=MESH)
    pl.semaphore_wait(barrier, len(friends))

    def x_start(layer, first, amount):
        buf, half = xf[layer], amount // 2
        lo, hi = pl.ds(first, half), pl.ds(first + half, half)

        out = new_send(buf.at[pl.ds(0, 7), pl.ds(0, amount), :])

        def go(block, rows, device, recv_sem=None):
            return send(buf.at[block, rows, :], buf.at[block, rows, :], device, out, recv_sem)

        near, first_two, passed = (Recv(new_recv(), buf.at[0, pl.ds(0, amount), :]) for _ in range(3))
        far = Recv(new_recv(), buf.at[pl.ds(0, 3), pl.ds(0, amount), :])
        return {"go": go, "lo": lo, "hi": hi, "near": near, "far": far, "two": first_two, "f": passed}

    def x_own(st, rows):
        go, lo = st["go"], st["lo"]
        if rows == "lo":
            go(g, lo, y_up, st["two"].sem)
            st["x_lo"] = go(g, lo, x_peer)
        else:
            go(g, st["hi"], y_down, st["two"].sem)
            st["x_hi"] = go(g, st["hi"], x_peer)
            go(g, st["hi"], y_up, st["near"].sem)
            go(g, lo, y_down, st["near"].sem)

    def x_fwd1(st):
        go = st["go"]
        st["two"].wait_recv()
        go(rel_g(0, 3), st["lo"], y_up, st["f"].sem)
        go(rel_g(0, 1), st["hi"], y_down, st["f"].sem)

    def x_fwd2(st):
        go, block, far = st["go"], rel_g(1, 0), st["far"].sem
        st["x_lo"].wait_recv()
        go(block, st["lo"], y_up, far)
        go(block, st["lo"], y_down, far)
        st["x_hi"].wait_recv()
        go(block, st["hi"], y_up, far)
        go(block, st["hi"], y_down, far)

    def x_fwd3(st):
        go, block, far = st["go"], rel_g(0, 2), st["far"].sem
        st["f"].wait_recv()
        go(block, st["lo"], x_peer, far)
        go(block, st["hi"], x_peer, far)

    def x_near(st):
        st["near"].wait_recv()

    def x_far(st):
        st["far"].wait_recv()

    half_w = WB // 2

    def w_piece(block, part):
        if part == "all":
            return (block, pl.ds(cb, WB), slice(None))
        start = cb if part == "lo" else cb + half_w
        return (block, pl.ds(pl.multiple_of(start, half_w), half_w), slice(None))

    def w_start(layer):
        buf = wf[layer]

        out = new_send(xf[layer].at[pl.ds(0, 6), :, :])

        def go(block, part, device, recv_sem=None):
            where = w_piece(block, part)
            return send(buf.at[where], buf.at[where], device, out, recv_sem)

        st = {"go": go}
        for name in ("f", "g", "two", "others", "h_two", "h_others"):
            st[name] = Recv(new_recv(), buf.at[0, pl.ds(0, WB), :])
        st["sib"] = Recv(new_recv(), buf.at[pl.ds(0, 4), :, :])
        go(wg, "lo", z_up, st["two"].sem)
        go(wg, "hi", z_down, st["two"].sem)
        st["h"] = go(wg, "all", h_peer)
        go(wg, "hi", z_up, st["others"].sem)
        go(wg, "lo", z_down, st["others"].sem)
        w_share(st, wg)
        return st

    def w_share(st, block):
        st["go"](block, "all", sibling, st["sib"].sem)

    def w_fwd1(st):
        go = st["go"]
        st["two"].wait_recv()
        go(rel_w(0, 3), "lo", z_up, st["f"].sem)
        go(rel_w(0, 1), "hi", z_down, st["f"].sem)

    def w_fwd2(st):
        go, far = st["go"], rel_w(1, 0)
        st["h"].wait_recv()
        go(far, "lo", z_up, st["h_two"].sem)
        go(far, "hi", z_down, st["h_two"].sem)
        go(far, "hi", z_up, st["h_others"].sem)
        go(far, "lo", z_down, st["h_others"].sem)
        w_share(st, far)
        st["others"].wait_recv()
        w_share(st, rel_w(0, 3))
        w_share(st, rel_w(0, 1))

    def w_fwd3(st):
        go = st["go"]
        st["h_two"].wait_recv()
        go(rel_w(1, 3), "lo", z_up, st["g"].sem)
        go(rel_w(1, 1), "hi", z_down, st["g"].sem)
        st["f"].wait_recv()
        w_share(st, rel_w(0, 2))

    def w_finish(st):
        st["h_others"].wait_recv()
        w_share(st, rel_w(1, 3))
        w_share(st, rel_w(1, 1))
        st["g"].wait_recv()
        w_share(st, rel_w(1, 2))
        st["sib"].wait_recv()

    def blocks(layer, first, amount, j0, j1, fresh):
        buf, weights = xf[layer], wf[layer]
        rows = slice(first, first + amount)
        if fresh:
            acc[rows, :] = nn(buf[g, rows, :], weights[g])

        def body(j, carry):
            block = ((xl + j // 4) % 2) * 4 + (y + j % 4) % 4
            acc[rows, :] += nn(buf[block, rows, :], weights[block])
            return carry

        lax.fori_loop(j0, j1, body, 0)

    def activate(first, amount, out, slope, tile=64):
        def body(i, carry):
            rows = pl.ds(pl.multiple_of(first + i * tile, tile), tile)
            value = acc[rows, :]
            sigma = jax.nn.sigmoid(value)
            out(rows, (value * sigma).astype(BF16))
            if slope is not None:
                slope[rows, :] = sigma * (1.0 + value * (1.0 - sigma))
            return carry

        lax.fori_loop(0, amount // tile, body, 0)

    def into_x1(rows, value):
        xf1[g, rows, :] = value

    def into_x2(rows, value):
        x2[rows, :] = value

    def next_layer(first, slope):
        st = x_start(1, first, CH)
        activate(first, CH // 2, into_x1, slope)
        x_own(st, "lo")
        activate(first + CH // 2, CH // 2, into_x1, slope)
        x_own(st, "hi")
        return st

    def to_group(src, dst, landed):
        out, got = new_send(landed), new_recv()
        for k in range(1, 8):
            gt = (g + k) % 8
            send(src, dst.at[g], {"xl": gt // 4, "y": gt % 4}, out, got)
        return Recv(got, landed)

    def from_group(own_part, dst):
        total = own_part[...]
        for k in range(1, 8):
            total = total + dst[(g + 8 - k) % 8]
        return total

    def head_send(ch):
        hs[ch] = nt(headt[0:32, :], x2[CH * ch : CH * (ch + 1), :])[0:24, :]
        return to_group(hs.at[ch], hr.at[ch], hr.at[ch, pl.ds(0, 7), :, :])

    def head_loss(ch, got):
        got.wait_recv()
        total = from_group(hs.at[ch], hr.at[ch])
        grad = vtrace(total, misc[ch, 0:24, :], misc[ch, 24:25, :], misc[ch, 25:26, :], misc[ch, 26:27, :])
        tmp[0:24, :] = grad
        rows = slice(CH * ch, CH * (ch + 1))
        og_r[rows, :] = tmp[...].T.astype(BF16)
        pg1[rows, :] = (nn(og_r[rows, :], headt[...]) * slope1[rows, :]).astype(BF16)
        pg1t[:, rows] = pg1[rows, :].T

    where_g = (rel_g(1, 2), rel_g(1, 1), rel_g(1, 3), rel_g(0, 1), rel_g(0, 3), rel_g(0, 2), rel_g(1, 0))

    class Scatter:
        def __init__(self, first, amount, col, cols):
            half = amount // 2
            self.rows = slice(first, first + amount)
            self.lo, self.hi = slice(first, first + half), slice(first + half, first + amount)
            self.cs = slice(col, col + cols)
            self.out = new_send(sb.at[:, self.ds(self.rows), self.ds(self.cs)])
            self.s2 = [Recv(new_recv(), rb.at[pl.ds(0, 2), self.ds(rows), self.ds(self.cs)]) for rows in (self.lo, self.hi)]
            self.s4 = Recv(new_recv(), rb.at[0, self.ds(self.rows), self.ds(self.cs)])
            self.last = Recv(new_recv(), rb.at[pl.ds(0, 3), self.ds(self.rows), self.ds(self.cs)])

        def ds(self, rows):
            return pl.ds(rows.start, rows.stop - rows.start)

        def piece(self, block):
            return nt(pg1[self.rows, :], wf1[block, self.cs, :])

        def make(self, k):
            sb[k, self.rows, self.cs] = self.piece(where_g[k]).astype(BF16)

        def push(self, k, rows, device, recv_sem=None):
            where = (k, self.ds(rows), self.ds(self.cs))
            return send(sb.at[where], rb.at[where], device, self.out, recv_sem)

        def add_in(self, k, rows, *terms):
            value = sb[k, rows, self.cs].astype(F32)
            for term in terms:
                value = value + rb[term, rows, self.cs].astype(F32)
            sb[k, rows, self.cs] = value.astype(BF16)

        def first(self):
            self.make(0)
            self.s1 = [self.push(0, self.lo, x_peer), self.push(0, self.hi, x_peer)]

        def make_rest(self):
            self.make(5)
            self.make(6)
            own[self.rows, self.cs] = self.piece(g)

        def push_two(self):
            for i, rows in enumerate((self.lo, self.hi)):
                self.push(1, rows, y_up, self.s2[i].sem)
                self.push(2, rows, y_down, self.s2[i].sem)

        def push_plain(self):
            self.push(3, self.hi, y_up, self.last.sem)
            self.push(4, self.lo, y_down, self.last.sem)

        def rest(self):
            self.make(1)
            self.make(2)
            self.push_two()
            self.make(3)
            self.make(4)
            self.push_plain()
            self.make_rest()

        def prepare(self):
            self.first()
            for k in range(1, 5):
                self.make(k)
            self.make_rest()

        def mid1(self):
            self.s1[0].wait_recv()
            self.add_in(5, self.lo, 0)
            self.push(5, self.lo, y_up, self.s4.sem)
            self.s1[1].wait_recv()
            self.add_in(5, self.hi, 0)
            self.push(5, self.hi, y_down, self.s4.sem)

        def mid2(self):
            for i, rows in enumerate((self.lo, self.hi)):
                self.s2[i].wait_recv()
                self.add_in(6, rows, 1, 2)
                self.push(6, rows, x_peer, self.last.sem)

        def mid3(self):
            self.s4.wait_recv()
            self.add_in(3, self.lo, 5)
            self.push(3, self.lo, y_up, self.last.sem)
            self.add_in(4, self.hi, 5)
            self.push(4, self.hi, y_down, self.last.sem)

        def close(self):
            self.last.wait_recv()
            cs = self.cs
            for r in range(self.rows.start, self.rows.stop, 128):
                rows = slice(r, r + 128)
                value = own[rows, cs] + rb[3, rows, cs].astype(F32) + rb[4, rows, cs].astype(F32) + rb[6, rows, cs].astype(F32)
                pg0t[cs, rows] = (value * slope0[rows, cs]).astype(BF16).T

    class Weights:
        def __init__(self, layer, pgt, bufs, col, cols, extra, halves=(0, 1)):
            self.halves = halves
            self.layer, self.pgt, self.extra = layer, pgt, extra
            self.dws, self.dwr, self.q, self.rz1, self.rz2, self.xs, self.rx = bufs
            self.cols, self.size = cols, cols + extra
            self.cs, self.top = slice(col, col + cols), slice(col + cols, col + cols + extra)
            self.all, half = slice(col, col + self.size), col + cols // 2
            self.low, self.high = slice(col, half), slice(half, col + self.size)
            self.base = count[0]
            count[0] += 4
            every = self.ds(self.all)
            self.out = new_send(self.q.at[pl.ds(0, 7), every, :])
            self.give_sem = new_send(self.dws.at[:, every, :])
            self.sums = {xr: Recv(new_recv(), self.rz2.at[xr, :, every, :]) for xr in halves}
            self.st = {}

        def ds(self, rows):
            return pl.ds(rows.start, rows.stop - rows.start)

        def block(self, i):
            return ((xh + 1 - i % 2) % 2) * 4 + (z + 2 + i // 2) % 4

        def copy_of(self, i):
            every = self.ds(self.all)
            return pltpu.make_async_remote_copy(
                src_ref=self.dws.at[i, every, :], dst_ref=self.dwr.at[i, every, :],
                send_sem=self.give_sem, recv_sem=rsem.at[self.base + i // 2],
                device_id=sibling, device_id_type=MESH,
            )

        def head_rows(self, block, core):
            return hgp[pl.ds(pl.multiple_of((2 * block + core) * 32, 32), 32), :]

        def give(self, i0, i1):
            other = pl.multiple_of((1 - c) * WB, WB)

            def body(i, carry):
                block = self.block(i)
                term = nn(self.pgt[self.cs, :], xf[self.layer][block, 0:TR, pl.ds(other, WB)])
                self.dws[i, self.cs, :] = term.astype(BF16)
                if self.extra:
                    self.dws[i, self.top, 0:128] = self.head_rows(block, 1 - c).astype(BF16)
                    self.dws[i, self.top, 128:256] = jnp.zeros((self.extra, 128), BF16)
                self.copy_of(i).start()
                return carry

            lax.fori_loop(i0, i1, body, 0)

        def keep(self, i0, i1):
            q, dwr, cs, top = self.q, self.dwr, self.cs, self.top
            assert i1 == i0 + 2
            Recv(rsem.at[self.base + i0 // 2], dwr.at[pl.ds(i0, 2), self.ds(self.all), :]).wait_recv()

            def body(i, carry):
                block = self.block(i)
                term = nn(self.pgt[cs, :], xf[self.layer][block, 0:TR, pl.ds(cb, WB)])
                q[i, cs, :] = (term + dwr[i, cs, :].astype(F32)).astype(BF16)
                if self.extra:
                    q[i, top, 0:128] = (self.head_rows(block, c) + dwr[i, top, 0:128].astype(F32)).astype(BF16)
                    q[i, top, 128:256] = jnp.zeros((self.extra, 128), BF16)
                return carry

            lax.fori_loop(i0, i1, body, 0)

        def go(self, i, rows, dst, device, recv_sem=None):
            where = self.ds(rows)
            return send(self.q.at[i, where, :], dst.at[where, :], device, self.out, recv_sem)

        def z_first(self):
            for xr in self.halves:
                self.st["a", xr] = self.go(xr, self.low, self.rz1.at[xr], z_up)
                self.st["b", xr] = self.go(xr, self.high, self.rz1.at[xr], z_down)

        def z_plain(self):
            for xr in self.halves:
                self.go(6 + xr, self.high, self.rz2.at[xr, 0], z_up, self.sums[xr].sem)
                self.go(2 + xr, self.low, self.rz2.at[xr, 1], z_down, self.sums[xr].sem)

        def late(self):
            self.keep(2, 4)
            self.keep(6, 8)
            self.z_plain()
            self.keep(4, 6)

        def z_added(self):
            q, rz1, st = self.q, self.rz1, self.st
            for xr in self.halves:
                for name, i, rows, side, device in (("a", 6, self.low, 0, z_up), ("b", 2, self.high, 1, z_down)):
                    st[name, xr].wait_recv()
                    value = q[i + xr, rows, :].astype(F32) + rz1[xr, rows, :].astype(F32)
                    q[i + xr, rows, :] = value.astype(BF16)
                    self.go(i + xr, rows, self.rz2.at[xr, side], device, self.sums[xr].sem)

        def z_sum(self, xr):
            self.sums[xr].wait_recv()
            every = self.all
            return (
                self.q[4 + xr, every, :].astype(F32)
                + self.rz2[xr, 0, every, :].astype(F32)
                + self.rz2[xr, 1, every, :].astype(F32)
            )

        def cross(self):
            every = self.ds(self.all)
            self.xs[self.all, :] = self.z_sum(0).astype(BF16)
            self.h = send(self.xs.at[every, :], self.rx.at[every, :], h_peer, self.out)

        def result(self):
            value = self.z_sum(1)
            if 0 in self.halves:
                self.h.wait_recv()
                value = value + self.rx[self.all, :].astype(F32)
            dw_out[self.layer, :, self.cs] = value[0 : self.cols, :].T
            if self.extra:
                hg_out[...] = value[self.cols :, 0:128].T[0 : ACT + 1, :]

    loads[0].wait()
    loads[1].wait()
    w0 = w_start(0)
    a0, b0 = x_start(0, 0, CH), x_start(0, CH, CH)
    x_own(a0, "lo")
    x_own(a0, "hi")
    x_own(b0, "lo")
    x_own(b0, "hi")
    for load in loads[2:]:
        load.wait()

    headt[...] = jnp.zeros_like(headt)
    headt[0 : ACT + 1, :] = head[...]
    misc[...] = jnp.zeros_like(misc)
    for r in range(8):
        ch, lane = r // 4, STEPS * (r % 4)
        steps = slice(lane, lane + STEPS - 1)
        misc[ch, 0:ACT, steps] = acting[:, r, :]
        misc[ch, 24:25, steps] = actions[r : r + 1, :].astype(F32)
        misc[ch, 25:26, steps] = rewards[r : r + 1, :]
        misc[ch, 26:27, steps] = finished[r : r + 1, :].astype(F32)
    tmp[...] = jnp.zeros_like(tmp)

    w_fwd1(w0)
    x_fwd1(a0)
    w_fwd2(w0)
    x_fwd1(b0)
    x_fwd2(a0)
    w_fwd3(w0)
    x_fwd3(a0)
    x_fwd2(b0)
    x_fwd3(b0)
    w1 = w_start(1)
    w_finish(w0)
    x_near(a0)
    blocks(0, 0, CH, 1, 5, True)
    x_far(a0)
    blocks(0, 0, CH, 5, 8, False)
    a1 = next_layer(0, slope0)
    w_fwd1(w1)
    x_near(b0)
    blocks(0, CH, CH, 1, 5, True)
    x_far(b0)
    blocks(0, CH, CH, 5, 8, False)
    b1 = next_layer(CH, slope0)

    x_fwd1(a1)
    w_fwd2(w1)
    x_fwd1(b1)
    x_fwd2(a1)
    w_fwd3(w1)
    x_fwd3(a1)
    x_fwd3(b1)
    x_fwd2(b1)
    w_finish(w1)
    x_near(a1)
    blocks(1, 0, CH, 1, 5, True)
    x_far(a1)
    blocks(1, 0, CH, 5, 8, False)
    activate(0, CH, into_x2, slope1)
    head_a = head_send(0)
    c0 = x_start(0, TR, AR)
    x_own(c0, "lo")
    x_own(c0, "hi")
    x_near(b1)
    blocks(1, CH, CH, 1, 5, True)
    x_far(b1)
    blocks(1, CH, CH, 5, 8, False)
    activate(CH, CH, into_x2, slope1)
    head_b = head_send(1)

    da1, da2 = Scatter(0, CH, 0, CH), Scatter(0, CH, CH, CH)
    db1, db2 = Scatter(CH, CH, 0, CH), Scatter(CH, CH, CH, CH)
    g1 = Weights(1, pg1t, (dws1, dwr1, q1, rz1a, rz2a, xs1, rx1), 0, FB, ER - FB)
    bufs0 = (dws0, dwr0, q0, rz1b, rz2b, xs0, rx0)
    g0a = Weights(0, pg0t, bufs0, 0, CH, 0)
    g0b = Weights(0, pg0t, bufs0, CH, CH, 0)
    head_loss(0, head_a)
    da1.first()
    da1.rest()
    x_fwd1(c0)
    da2.prepare()
    head_loss(1, head_b)
    db1.first()
    hgp[...] = tn(x2[0:TR, :], og_r[...])
    g1.give(0, 2)
    db1.rest()
    g1.keep(0, 2)
    g1.z_first()
    da1.mid1()
    da1.mid2()
    g1.give(2, 8)
    db2.prepare()
    db1.mid1()
    x_fwd2(c0)
    x_fwd3(c0)
    g1.keep(2, 4)
    db1.mid2()
    g1.keep(6, 8)
    g1.z_plain()
    da1.mid3()
    g1.keep(4, 6)
    db1.mid3()
    da2.mid1()
    db2.mid1()
    da2.push_two()
    db2.push_two()
    da2.push_plain()
    db2.push_plain()
    g1.z_added()
    x_near(c0)
    x_far(c0)
    blocks(0, TR, AR, 1, 8, True)
    activate(TR, AR, into_x1, None)
    da1.close()
    db1.close()
    g0a.give(0, 2)
    g0a.keep(0, 2)
    g0a.z_first()
    da2.mid3()
    db2.mid3()
    g0a.give(2, 8)
    da2.mid2()
    g0a.keep(2, 4)
    g0a.keep(6, 8)
    g0a.z_plain()
    db2.mid2()
    c1 = x_start(1, TR, AR)
    x_own(c1, "lo")
    x_own(c1, "hi")
    g0a.keep(4, 6)
    g0a.z_added()
    g1.cross()
    da2.close()
    db2.close()
    g0b.give(0, 2)
    g0b.keep(0, 2)
    g0b.z_first()
    x_fwd1(c1)
    x_fwd2(c1)
    g0b.give(2, 8)
    g0b.late()
    x_fwd3(c1)
    g0b.z_added()
    g0a.cross()
    x_near(c1)
    blocks(1, TR, AR, 1, 5, True)
    x_far(c1)
    blocks(1, TR, AR, 5, 8, False)
    activate(TR, AR, into_x2, None)
    ha_s[...] = nt(headt[0:32, :], x2[TR : TR + AR, :])[0:24, :]
    acts = to_group(ha_s, ha_r, ha_r.at[pl.ds(0, 7), :, :])
    g0b.cross()
    g1.result()
    g0a.result()
    acts.wait_recv()
    al_out[...] = from_group(ha_s, ha_r)[0:ACT, :]
    g0b.result()

    for view, sem in sends:
        pltpu.make_async_remote_copy(
            src_ref=view, dst_ref=view, send_sem=sem, recv_sem=rsem.at[0], device_id=x_peer, device_id_type=MESH,
        ).wait_send()
    assert (count[0], count[1]) == (N_RECV, N_SEND), count


def hand_out_kernel(dw, hg, al, dw_out, hg_out, al_out, sems):
    copies = [pltpu.make_async_copy(a, b, sems.at[i]) for i, (a, b) in enumerate(((dw, dw_out), (hg, hg_out), (al, al_out)))]
    for copy in copies:
        copy.start()
    for copy in copies:
        copy.wait()


def hand_out(*arrays):
    arrays = [pltpu.with_memory_space_constraint(a, pltpu.VMEM) for a in arrays]
    hbm = pl.BlockSpec(memory_space=pltpu.HBM)
    return pl.pallas_call(
        hand_out_kernel,
        out_shape=tuple(jax.ShapeDtypeStruct(a.shape, a.dtype) for a in arrays),
        in_specs=[pl.BlockSpec(memory_space=pltpu.VMEM)] * 3,
        out_specs=(hbm,) * 3,
        scratch_shapes=[pltpu.SemaphoreType.DMA((3,))],
        name="hand_out",
    )(*arrays)


def per_device(observations, next_observations, trunk_weights, head_weights, acting, actions, rewards, finished):
    v = pltpu.VMEM
    dw_bufs = lambda rows: [
        v((8, rows, WB), BF16), v((8, rows, WB), BF16), v((8, rows, WB), BF16), v((2, rows, WB), BF16),
        v((2, 2, rows, WB), BF16), v((rows, WB), BF16), v((rows, WB), BF16),
    ]
    scratch = [
        v((8, TR + AR, FB), BF16), v((8, TR + AR, FB), BF16), v((8, FB, FB), BF16), v((8, FB, FB), BF16),
        v((TR + AR, FB), F32), v((TR, FB), F32), v((TR, FB), F32), v((TR + AR, FB), BF16),
        v((128, FB), BF16), v((128, CH), F32), v((2, 32, CH), F32),
        v((2, 24, CH), F32), v((2, 8, 24, CH), F32), v((24, 128), F32), v((8, 24, 128), F32),
        v((TR, 128), BF16), v((TR, FB), BF16), v((FB, TR), BF16), v((FB, TR), BF16), v((FB, 128), F32),
        v((7, TR, FB), BF16), v((7, TR, FB), BF16), v((TR, FB), F32),
        *dw_bufs(ER), *dw_bufs(FB),
        v((ACT + 1, FB), BF16), v((ACT, 8, STEPS - 1), F32), v((8, STEPS - 1), jnp.int32), v((8, STEPS - 1), F32),
        v((8, STEPS - 1), jnp.int32),
        pltpu.SemaphoreType.DMA((N_SEND,)), pltpu.SemaphoreType.DMA((N_RECV,)), pltpu.SemaphoreType.DMA((9,)),
    ]
    hbm = pl.BlockSpec(memory_space=pltpu.HBM)
    vm = pl.BlockSpec(memory_space=pltpu.VMEM)
    trunk_grads, head_grads, actor_logits = pl.pallas_call(
        kernel,
        out_shape=(
            pltpu.VMEM((2, WB, FB), F32),
            pltpu.VMEM((ACT + 1, 32), F32),
            pltpu.VMEM((ACT, AR), F32),
        ),
        in_specs=[hbm] * 8,
        out_specs=(vm,) * 3,
        scratch_shapes=scratch,
        compiler_params=pltpu.CompilerParams(
            collective_id=0, has_side_effects=True, vmem_limit_bytes=58 * 1024 * 1024
        ),
        name="learner_step",
    )(
        observations.reshape(TR, FB), next_observations, trunk_weights, head_weights.T, acting.transpose(2, 0, 1),
        actions, rewards, finished,
    )
    trunk_grads, head_grads, actor_logits = hand_out(trunk_grads, head_grads, actor_logits)
    return trunk_grads, head_grads.T, actor_logits.T


def solution(mesh):
    split = Mesh(mesh.devices.reshape(SIZES), AXES)
    return jax.shard_map(
        per_device,
        mesh=split,
        in_specs=(
            P(DP, None, GROUP),
            P(DP, GROUP),
            P(None, DP, GROUP),
            P(GROUP, None),
            P(DP, None, None),
            P(DP, None),
            P(DP, None),
            P(DP, None),
        ),
        out_specs=(P(None, DP, GROUP), P(GROUP + DP, None), P(DP, None)),
        check_vma=False,
    )
```

```python
import functools

import jax
import jax.numpy as jnp
from jax import lax
from jax.experimental import pallas as pl
from jax.experimental.pallas import tpu as pltpu
from jax.sharding import Mesh
from jax.sharding import PartitionSpec as P

AXES = ("xl", "y", "xh", "z", "c")
SIZES = (2, 4, 2, 4, 2)
DP = ("xh", "z", "c")
GROUP = ("xl", "y")
MESH = pl.DeviceIdType.MESH
F32 = jnp.float32
BF16 = jnp.bfloat16

discount_rate = 0.99
value_weight = 0.5
entropy_weight = 0.1
loss_divisor = 16.0

TR = 512
AR = 128
FB = 512
WB = 256
STEPS = 64
ACT = 18
ER = 544
N_RECV, N_SEND = 118, 21
CH = 256


def nn(a, b):
    return jnp.dot(a, b, preferred_element_type=F32)


def nt(a, b):
    return lax.dot_general(a, b, (((1,), (1,)), ((), ())), preferred_element_type=F32)


def tn(a, b):
    return lax.dot_general(a, b, (((0,), (0,)), ((), ())), preferred_element_type=F32)


def vtrace(logits, behave, action, reward, finished):
    row = lax.broadcasted_iota(jnp.int32, logits.shape, 0)
    step = lax.broadcasted_iota(jnp.int32, reward.shape, 1)
    live = step % STEPS < STEPS - 1
    lanes = reward.shape[1]
    is_act = row < ACT

    def log_softmax(values):
        top = jnp.max(jnp.where(is_act, values, -3.0e38), axis=0, keepdims=True)
        shifted = jnp.where(is_act, values - top, 0.0)
        total = jnp.sum(jnp.where(is_act, jnp.exp(shifted), 0.0), axis=0, keepdims=True)
        return jnp.where(is_act, shifted - jnp.log(total), 0.0)

    log_policy = log_softmax(logits)
    log_behave = log_softmax(behave)
    chosen = jnp.where(row.astype(F32) == action, 1.0, 0.0)
    ratio = jnp.exp(jnp.sum((log_policy - log_behave) * chosen, axis=0, keepdims=True))
    clipped = jnp.minimum(ratio, 1.0)
    discount = discount_rate * (1.0 - finished)
    current = logits[ACT : ACT + 1, :]
    following = pltpu.roll(current, lanes - 1, 1)
    delta = jnp.where(live, clipped * (reward + discount * following - current), 0.0)
    factor = jnp.where(live, discount * clipped, 0.0)
    for shift in (1, 2, 4, 8, 16, 32):
        delta = delta + factor * pltpu.roll(delta, lanes - shift, 1)
        factor = factor * pltpu.roll(factor, lanes - shift, 1)
    targets = current + delta
    next_targets = pltpu.roll(targets, lanes - 1, 1)
    advantage = clipped * (reward + discount * next_targets - current)
    probability = jnp.where(is_act, jnp.exp(log_policy), 0.0)
    entropy = -jnp.sum(probability * log_policy, axis=0, keepdims=True)
    logit_grad = (
        -advantage * (chosen - probability)
        + entropy_weight * probability * (log_policy + entropy)
    ) / loss_divisor
    value_grad = -value_weight * (targets - current) / loss_divisor
    grad = jnp.where(is_act, logit_grad, jnp.where(row == ACT, value_grad, 0.0))
    return jnp.where(live, grad, 0.0)


def kernel(
    obs, nxt, wts, head_in, acting_in, actions_in, rewards_in, finished_in,
    dw_out, hg_out, al_out,
    xf0, xf1, wf0, wf1, acc, slope0, slope1, x2, headt, tmp, misc,
    hs, hr, ha_s, ha_r, og_r, pg1, pg1t, pg0t, hgp,
    sb, rb, own,
    dws1, dwr1, q1, rz1a, rz2a, xs1, rx1,
    dws0, dwr0, q0, rz1b, rz2b, xs0, rx0,
    head, acting, actions, rewards, finished, ssem, rsem, lsem,
):
    xl, y, xh, z, c = (lax.axis_index(a) for a in AXES)
    g = xl * 4 + y
    xf, wf = (xf0, xf1), (wf0, wf1)

    def rel_g(dx, dy):
        return ((xl + dx) % 2) * 4 + (y + dy) % 4

    def rel_w(dx, dz):
        return ((xh + dx) % 2) * 4 + (z + dz) % 4

    x_peer = {"xl": 1 - xl}
    y_up, y_down = {"y": (y + 1) % 4}, {"y": (y + 3) % 4}
    h_peer = {"xh": 1 - xh}
    z_up, z_down = {"z": (z + 1) % 4}, {"z": (z + 3) % 4}
    sibling = {"c": 1 - c}

    count = [0, 0]
    sends = []

    def new_recv():
        count[0] += 1
        return rsem.at[count[0] - 1]

    def new_send(view):
        count[1] += 1
        sem = ssem.at[count[1] - 1]
        sends.append((view, sem))
        return sem

    class Recv:
        def __init__(self, sem, view):
            self.sem, self.view = sem, view

        def wait_recv(self):
            pltpu.make_async_remote_copy(
                src_ref=self.view, dst_ref=self.view, send_sem=ssem.at[0], recv_sem=self.sem,
                device_id=x_peer, device_id_type=MESH,
            ).wait_recv()

    def send(src, dst, device, send_sem, recv_sem=None):
        copy = pltpu.make_async_remote_copy(
            src_ref=src, dst_ref=dst, send_sem=send_sem, recv_sem=new_recv() if recv_sem is None else recv_sem,
            device_id=device, device_id_type=MESH,
        )
        copy.start()
        return copy

    cb = pl.multiple_of(c * WB, WB)
    wg = xh * 4 + z
    loads = [
        pltpu.make_async_copy(obs, xf0.at[g, pl.ds(0, TR), :], lsem.at[0]),
        pltpu.make_async_copy(wts.at[0], wf0.at[wg, pl.ds(cb, WB), :], lsem.at[1]),
        pltpu.make_async_copy(wts.at[1], wf1.at[wg, pl.ds(cb, WB), :], lsem.at[2]),
        pltpu.make_async_copy(nxt, xf0.at[g, pl.ds(TR, AR), :], lsem.at[3]),
        pltpu.make_async_copy(head_in, head, lsem.at[4]),
        pltpu.make_async_copy(acting_in, acting, lsem.at[5]),
        pltpu.make_async_copy(actions_in, actions, lsem.at[6]),
        pltpu.make_async_copy(rewards_in, rewards, lsem.at[7]),
        pltpu.make_async_copy(finished_in, finished, lsem.at[8]),
    ]
    for load in loads:
        load.start()

    barrier = pltpu.get_barrier_semaphore()
    friends = [x_peer, y_up, y_down, h_peer, z_up, z_down, sibling]
    for friend in friends:
        pl.semaphore_signal(barrier, inc=1, device_id=friend, device_id_type=MESH)
    pl.semaphore_wait(barrier, len(friends))

    def x_start(layer, first, amount):
        buf, half = xf[layer], amount // 2
        lo, hi = pl.ds(first, half), pl.ds(first + half, half)

        out = new_send(buf.at[pl.ds(0, 7), pl.ds(0, amount), :])

        def go(block, rows, device, recv_sem=None):
            return send(buf.at[block, rows, :], buf.at[block, rows, :], device, out, recv_sem)

        near, first_two, passed = (Recv(new_recv(), buf.at[0, pl.ds(0, amount), :]) for _ in range(3))
        side = Recv(new_recv(), buf.at[pl.ds(0, 2), pl.ds(0, amount), :])
        far = Recv(new_recv(), buf.at[0, pl.ds(0, amount), :])
        return {"go": go, "lo": lo, "hi": hi, "near": near, "side": side, "far": far, "two": first_two, "f": passed}

    def x_own(st, rows):
        go, lo = st["go"], st["lo"]
        if rows == "lo":
            go(g, lo, y_up, st["two"].sem)
            st["x_lo"] = go(g, lo, x_peer)
        else:
            go(g, st["hi"], y_down, st["two"].sem)
            st["x_hi"] = go(g, st["hi"], x_peer)
            go(g, st["hi"], y_up, st["near"].sem)
            go(g, lo, y_down, st["near"].sem)

    def x_fwd1(st):
        go = st["go"]
        st["two"].wait_recv()
        go(rel_g(0, 3), st["lo"], y_up, st["f"].sem)
        go(rel_g(0, 1), st["hi"], y_down, st["f"].sem)

    def x_fwd2(st):
        go, block, far = st["go"], rel_g(1, 0), st["side"].sem
        st["x_lo"].wait_recv()
        go(block, st["lo"], y_up, far)
        go(block, st["lo"], y_down, far)
        st["x_hi"].wait_recv()
        go(block, st["hi"], y_up, far)
        go(block, st["hi"], y_down, far)

    def x_fwd3(st):
        go, block, far = st["go"], rel_g(0, 2), st["far"].sem
        st["f"].wait_recv()
        go(block, st["lo"], x_peer, far)
        go(block, st["hi"], x_peer, far)

    def x_near(st):
        st["near"].wait_recv()

    def x_side(st):
        st["side"].wait_recv()

    def x_far(st):
        st["far"].wait_recv()

    half_w = WB // 2

    def w_piece(block, part):
        if part == "all":
            return (block, pl.ds(cb, WB), slice(None))
        start = cb if part == "lo" else cb + half_w
        return (block, pl.ds(pl.multiple_of(start, half_w), half_w), slice(None))

    def w_start(layer):
        buf = wf[layer]

        out = new_send(xf[layer].at[pl.ds(0, 6), :, :])

        def go(block, part, device, recv_sem=None):
            where = w_piece(block, part)
            return send(buf.at[where], buf.at[where], device, out, recv_sem)

        st = {"go": go}
        for name in ("f", "g", "two", "others", "h_two", "h_others"):
            st[name] = Recv(new_recv(), buf.at[0, pl.ds(0, WB), :])
        st["sib"] = Recv(new_recv(), buf.at[pl.ds(0, 4), :, :])
        go(wg, "lo", z_up, st["two"].sem)
        go(wg, "hi", z_down, st["two"].sem)
        st["h"] = go(wg, "all", h_peer)
        go(wg, "hi", z_up, st["others"].sem)
        go(wg, "lo", z_down, st["others"].sem)
        w_share(st, wg)
        return st

    def w_share(st, block):
        st["go"](block, "all", sibling, st["sib"].sem)

    def w_fwd1(st):
        go = st["go"]
        st["two"].wait_recv()
        go(rel_w(0, 3), "lo", z_up, st["f"].sem)
        go(rel_w(0, 1), "hi", z_down, st["f"].sem)

    def w_fwd2(st):
        go, far = st["go"], rel_w(1, 0)
        st["h"].wait_recv()
        go(far, "lo", z_up, st["h_two"].sem)
        go(far, "hi", z_down, st["h_two"].sem)
        go(far, "hi", z_up, st["h_others"].sem)
        go(far, "lo", z_down, st["h_others"].sem)
        w_share(st, far)
        st["others"].wait_recv()
        w_share(st, rel_w(0, 3))
        w_share(st, rel_w(0, 1))

    def w_fwd3(st):
        go = st["go"]
        st["h_two"].wait_recv()
        go(rel_w(1, 3), "lo", z_up, st["g"].sem)
        go(rel_w(1, 1), "hi", z_down, st["g"].sem)
        st["f"].wait_recv()
        w_share(st, rel_w(0, 2))

    def w_finish(st):
        st["h_others"].wait_recv()
        w_share(st, rel_w(1, 3))
        w_share(st, rel_w(1, 1))
        st["g"].wait_recv()
        w_share(st, rel_w(1, 2))
        st["sib"].wait_recv()

    def blocks(layer, first, amount, j0, j1, fresh):
        buf, weights = xf[layer], wf[layer]
        rows = slice(first, first + amount)
        if fresh:
            acc[rows, :] = nn(buf[g, rows, :], weights[g])

        def body(j, carry):
            step = j % 4
            step = step + (step // 2) * (5 - 2 * step)
            block = ((xl + j // 4) % 2) * 4 + (y + step) % 4
            acc[rows, :] += nn(buf[block, rows, :], weights[block])
            return carry

        lax.fori_loop(j0, j1, body, 0)

    def activate(first, amount, out, slope, tile=64):
        def body(i, carry):
            rows = pl.ds(pl.multiple_of(first + i * tile, tile), tile)
            value = acc[rows, :]
            sigma = jax.nn.sigmoid(value)
            out(rows, (value * sigma).astype(BF16))
            if slope is not None:
                slope[rows, :] = sigma * (1.0 + value * (1.0 - sigma))
            return carry

        lax.fori_loop(0, amount // tile, body, 0)

    def into_x1(rows, value):
        xf1[g, rows, :] = value

    def into_x2(rows, value):
        x2[rows, :] = value

    def next_layer(first, slope):
        st = x_start(1, first, CH)
        activate(first, CH // 2, into_x1, slope)
        x_own(st, "lo")
        activate(first + CH // 2, CH // 2, into_x1, slope)
        x_own(st, "hi")
        return st

    def to_group(src, dst, landed):
        out, got = new_send(landed), new_recv()
        for k in range(1, 8):
            gt = (g + k) % 8
            send(src, dst.at[g], {"xl": gt // 4, "y": gt % 4}, out, got)
        return Recv(got, landed)

    def from_group(own_part, dst):
        total = own_part[...]
        for k in range(1, 8):
            total = total + dst[(g + 8 - k) % 8]
        return total

    def head_send(ch):
        hs[ch] = nt(headt[0:32, :], x2[CH * ch : CH * (ch + 1), :])[0:24, :]
        return to_group(hs.at[ch], hr.at[ch], hr.at[ch, pl.ds(0, 7), :, :])

    def head_loss(ch, got):
        got.wait_recv()
        total = from_group(hs.at[ch], hr.at[ch])
        grad = vtrace(total, misc[ch, 0:24, :], misc[ch, 24:25, :], misc[ch, 25:26, :], misc[ch, 26:27, :])
        tmp[0:24, :] = grad
        rows = slice(CH * ch, CH * (ch + 1))
        og_r[rows, :] = tmp[...].T.astype(BF16)
        pg1[rows, :] = (nn(og_r[rows, :], headt[...]) * slope1[rows, :]).astype(BF16)
        pg1t[:, rows] = pg1[rows, :].T

    where_g = (rel_g(1, 2), rel_g(1, 1), rel_g(1, 3), rel_g(0, 1), rel_g(0, 3), rel_g(0, 2), rel_g(1, 0))

    class Scatter:
        def __init__(self, first, amount, col, cols):
            half = amount // 2
            self.rows = slice(first, first + amount)
            self.lo, self.hi = slice(first, first + half), slice(first + half, first + amount)
            self.cs = slice(col, col + cols)
            self.out = new_send(sb.at[:, self.ds(self.rows), self.ds(self.cs)])
            self.s2 = [Recv(new_recv(), rb.at[pl.ds(0, 2), self.ds(rows), self.ds(self.cs)]) for rows in (self.lo, self.hi)]
            self.s4 = Recv(new_recv(), rb.at[0, self.ds(self.rows), self.ds(self.cs)])
            self.last = Recv(new_recv(), rb.at[pl.ds(0, 3), self.ds(self.rows), self.ds(self.cs)])

        def ds(self, rows):
            return pl.ds(rows.start, rows.stop - rows.start)

        def piece(self, block):
            return nt(pg1[self.rows, :], wf1[block, self.cs, :])

        def make(self, k):
            sb[k, self.rows, self.cs] = self.piece(where_g[k]).astype(BF16)

        def push(self, k, rows, device, recv_sem=None):
            where = (k, self.ds(rows), self.ds(self.cs))
            return send(sb.at[where], rb.at[where], device, self.out, recv_sem)

        def add_in(self, k, rows, *terms):
            value = sb[k, rows, self.cs].astype(F32)
            for term in terms:
                value = value + rb[term, rows, self.cs].astype(F32)
            sb[k, rows, self.cs] = value.astype(BF16)

        def first(self):
            self.make(0)
            self.s1 = [self.push(0, self.lo, x_peer), self.push(0, self.hi, x_peer)]

        def make_rest(self):
            self.make(5)
            self.make(6)
            own[self.rows, self.cs] = self.piece(g)

        def push_two(self):
            for i, rows in enumerate((self.lo, self.hi)):
                self.push(1, rows, y_up, self.s2[i].sem)
                self.push(2, rows, y_down, self.s2[i].sem)

        def push_plain(self):
            self.push(3, self.hi, y_up, self.last.sem)
            self.push(4, self.lo, y_down, self.last.sem)

        def rest(self):
            self.make(1)
            self.make(2)
            self.push_two()
            self.make(3)
            self.make(4)
            self.push_plain()
            self.make_rest()

        def prepare(self):
            self.first()
            for k in range(1, 5):
                self.make(k)
            self.make_rest()

        def mid1(self):
            self.s1[0].wait_recv()
            self.add_in(5, self.lo, 0)
            self.push(5, self.lo, y_up, self.s4.sem)
            self.s1[1].wait_recv()
            self.add_in(5, self.hi, 0)
            self.push(5, self.hi, y_down, self.s4.sem)

        def mid2(self):
            for i, rows in enumerate((self.lo, self.hi)):
                self.s2[i].wait_recv()
                self.add_in(6, rows, 1, 2)
                self.push(6, rows, x_peer, self.last.sem)

        def mid3(self):
            self.s4.wait_recv()
            self.add_in(3, self.lo, 5)
            self.push(3, self.lo, y_up, self.last.sem)
            self.add_in(4, self.hi, 5)
            self.push(4, self.hi, y_down, self.last.sem)

        def close(self):
            self.last.wait_recv()
            cs = self.cs
            for r in range(self.rows.start, self.rows.stop, 128):
                rows = slice(r, r + 128)
                value = own[rows, cs] + rb[3, rows, cs].astype(F32) + rb[4, rows, cs].astype(F32) + rb[6, rows, cs].astype(F32)
                pg0t[cs, rows] = (value * slope0[rows, cs]).astype(BF16).T

    class Weights:
        def __init__(self, layer, pgt, bufs, col, cols, extra, halves=(0, 1)):
            self.halves = halves
            self.layer, self.pgt, self.extra = layer, pgt, extra
            self.dws, self.dwr, self.q, self.rz1, self.rz2, self.xs, self.rx = bufs
            self.cols, self.size = cols, cols + extra
            self.cs, self.top = slice(col, col + cols), slice(col + cols, col + cols + extra)
            self.all, half = slice(col, col + self.size), col + cols // 2
            self.low, self.high = slice(col, half), slice(half, col + self.size)
            self.base = count[0]
            count[0] += 4
            every = self.ds(self.all)
            self.out = new_send(self.q.at[pl.ds(0, 7), every, :])
            self.give_sem = new_send(self.dws.at[:, every, :])
            self.sums = {xr: Recv(new_recv(), self.rz2.at[xr, :, every, :]) for xr in halves}
            self.st = {}

        def ds(self, rows):
            return pl.ds(rows.start, rows.stop - rows.start)

        def block(self, i):
            return ((xh + 1 - i % 2) % 2) * 4 + (z + 2 + i // 2) % 4

        def copy_of(self, i):
            every = self.ds(self.all)
            return pltpu.make_async_remote_copy(
                src_ref=self.dws.at[i, every, :], dst_ref=self.dwr.at[i, every, :],
                send_sem=self.give_sem, recv_sem=rsem.at[self.base + i // 2],
                device_id=sibling, device_id_type=MESH,
            )

        def head_rows(self, block, core):
            return hgp[pl.ds(pl.multiple_of((2 * block + core) * 32, 32), 32), :]

        def give(self, i0, i1):
            other = pl.multiple_of((1 - c) * WB, WB)

            def body(i, carry):
                block = self.block(i)
                term = nn(self.pgt[self.cs, :], xf[self.layer][block, 0:TR, pl.ds(other, WB)])
                self.dws[i, self.cs, :] = term.astype(BF16)
                if self.extra:
                    self.dws[i, self.top, 0:128] = self.head_rows(block, 1 - c).astype(BF16)
                    self.dws[i, self.top, 128:256] = jnp.zeros((self.extra, 128), BF16)
                self.copy_of(i).start()
                return carry

            lax.fori_loop(i0, i1, body, 0)

        def keep(self, i0, i1):
            q, dwr, cs, top = self.q, self.dwr, self.cs, self.top
            assert i1 == i0 + 2
            Recv(rsem.at[self.base + i0 // 2], dwr.at[pl.ds(i0, 2), self.ds(self.all), :]).wait_recv()

            def body(i, carry):
                block = self.block(i)
                term = nn(self.pgt[cs, :], xf[self.layer][block, 0:TR, pl.ds(cb, WB)])
                q[i, cs, :] = (term + dwr[i, cs, :].astype(F32)).astype(BF16)
                if self.extra:
                    q[i, top, 0:128] = (self.head_rows(block, c) + dwr[i, top, 0:128].astype(F32)).astype(BF16)
                    q[i, top, 128:256] = jnp.zeros((self.extra, 128), BF16)
                return carry

            lax.fori_loop(i0, i1, body, 0)

        def go(self, i, rows, dst, device, recv_sem=None):
            where = self.ds(rows)
            return send(self.q.at[i, where, :], dst.at[where, :], device, self.out, recv_sem)

        def z_first(self):
            for xr in self.halves:
                self.st["a", xr] = self.go(xr, self.low, self.rz1.at[xr], z_up)
                self.st["b", xr] = self.go(xr, self.high, self.rz1.at[xr], z_down)

        def z_plain(self):
            for xr in self.halves:
                self.go(6 + xr, self.high, self.rz2.at[xr, 0], z_up, self.sums[xr].sem)
                self.go(2 + xr, self.low, self.rz2.at[xr, 1], z_down, self.sums[xr].sem)

        def late(self):
            self.keep(2, 4)
            self.keep(6, 8)
            self.z_plain()
            self.keep(4, 6)

        def z_added(self):
            q, rz1, st = self.q, self.rz1, self.st
            for xr in self.halves:
                for name, i, rows, side, device in (("a", 6, self.low, 0, z_up), ("b", 2, self.high, 1, z_down)):
                    st[name, xr].wait_recv()
                    value = q[i + xr, rows, :].astype(F32) + rz1[xr, rows, :].astype(F32)
                    q[i + xr, rows, :] = value.astype(BF16)
                    self.go(i + xr, rows, self.rz2.at[xr, side], device, self.sums[xr].sem)

        def z_sum(self, xr):
            self.sums[xr].wait_recv()
            every = self.all
            return (
                self.q[4 + xr, every, :].astype(F32)
                + self.rz2[xr, 0, every, :].astype(F32)
                + self.rz2[xr, 1, every, :].astype(F32)
            )

        def cross(self):
            every = self.ds(self.all)
            self.xs[self.all, :] = self.z_sum(0).astype(BF16)
            self.h = send(self.xs.at[every, :], self.rx.at[every, :], h_peer, self.out)

        def result(self):
            value = self.z_sum(1)
            if 0 in self.halves:
                self.h.wait_recv()
                value = value + self.rx[self.all, :].astype(F32)
            dw_out[self.layer, :, self.cs] = value[0 : self.cols, :].T
            if self.extra:
                hg_out[...] = value[self.cols :, 0:128].T[0 : ACT + 1, :]

    loads[0].wait()
    loads[1].wait()
    w0 = w_start(0)
    a0, b0 = x_start(0, 0, CH), x_start(0, CH, CH)
    x_own(a0, "lo")
    x_own(a0, "hi")
    x_own(b0, "lo")
    x_own(b0, "hi")
    for load in loads[2:]:
        load.wait()

    headt[...] = jnp.zeros_like(headt)
    headt[0 : ACT + 1, :] = head[...]
    misc[...] = jnp.zeros_like(misc)
    for r in range(8):
        ch, lane = r // 4, STEPS * (r % 4)
        steps = slice(lane, lane + STEPS - 1)
        misc[ch, 0:ACT, steps] = acting[:, r, :]
        misc[ch, 24:25, steps] = actions[r : r + 1, :].astype(F32)
        misc[ch, 25:26, steps] = rewards[r : r + 1, :]
        misc[ch, 26:27, steps] = finished[r : r + 1, :].astype(F32)
    tmp[...] = jnp.zeros_like(tmp)

    w_fwd1(w0)
    x_fwd1(a0)
    w_fwd2(w0)
    x_fwd1(b0)
    x_fwd2(a0)
    w_fwd3(w0)
    x_fwd3(a0)
    x_fwd2(b0)
    x_fwd3(b0)
    w1 = w_start(1)
    w_finish(w0)
    x_near(a0)
    blocks(0, 0, CH, 1, 5, True)
    x_side(a0)
    blocks(0, 0, CH, 5, 7, False)
    x_far(a0)
    blocks(0, 0, CH, 7, 8, False)
    a1 = next_layer(0, slope0)
    w_fwd1(w1)
    x_near(b0)
    blocks(0, CH, CH, 1, 5, True)
    x_side(b0)
    blocks(0, CH, CH, 5, 7, False)
    x_far(b0)
    blocks(0, CH, CH, 7, 8, False)
    b1 = next_layer(CH, slope0)

    x_fwd1(a1)
    w_fwd2(w1)
    x_fwd1(b1)
    x_fwd2(a1)
    w_fwd3(w1)
    x_fwd3(a1)
    x_fwd3(b1)
    x_fwd2(b1)
    w_finish(w1)
    x_near(a1)
    blocks(1, 0, CH, 1, 5, True)
    x_side(a1)
    blocks(1, 0, CH, 5, 7, False)
    x_far(a1)
    blocks(1, 0, CH, 7, 8, False)
    activate(0, CH, into_x2, slope1)
    head_a = head_send(0)
    c0 = x_start(0, TR, AR)
    x_own(c0, "lo")
    x_own(c0, "hi")
    x_near(b1)
    blocks(1, CH, CH, 1, 5, True)
    x_side(b1)
    blocks(1, CH, CH, 5, 7, False)
    x_far(b1)
    blocks(1, CH, CH, 7, 8, False)
    activate(CH, CH, into_x2, slope1)
    head_b = head_send(1)

    da1, da2 = Scatter(0, CH, 0, CH), Scatter(0, CH, CH, CH)
    db1, db2 = Scatter(CH, CH, 0, CH), Scatter(CH, CH, CH, CH)
    g1 = Weights(1, pg1t, (dws1, dwr1, q1, rz1a, rz2a, xs1, rx1), 0, FB, ER - FB)
    bufs0 = (dws0, dwr0, q0, rz1b, rz2b, xs0, rx0)
    g0a = Weights(0, pg0t, bufs0, 0, CH, 0)
    g0b = Weights(0, pg0t, bufs0, CH, CH, 0)
    head_loss(0, head_a)
    da1.first()
    da1.rest()
    x_fwd1(c0)
    da2.prepare()
    head_loss(1, head_b)
    db1.first()
    hgp[...] = tn(x2[0:TR, :], og_r[...])
    g1.give(0, 2)
    db1.rest()
    g1.keep(0, 2)
    g1.z_first()
    da1.mid1()
    da1.mid2()
    g1.give(2, 8)
    db2.prepare()
    db1.mid1()
    x_fwd2(c0)
    x_fwd3(c0)
    g1.keep(2, 4)
    db1.mid2()
    g1.keep(6, 8)
    g1.z_plain()
    da1.mid3()
    g1.keep(4, 6)
    db1.mid3()
    da2.mid1()
    db2.mid1()
    da2.push_two()
    db2.push_two()
    da2.push_plain()
    db2.push_plain()
    g1.z_added()
    x_near(c0)
    x_side(c0)
    x_far(c0)
    blocks(0, TR, AR, 1, 8, True)
    activate(TR, AR, into_x1, None)
    da1.close()
    db1.close()
    g0a.give(0, 2)
    g0a.keep(0, 2)
    g0a.z_first()
    da2.mid3()
    db2.mid3()
    g0a.give(2, 8)
    da2.mid2()
    g0a.keep(2, 4)
    g0a.keep(6, 8)
    g0a.z_plain()
    db2.mid2()
    c1 = x_start(1, TR, AR)
    x_own(c1, "lo")
    x_own(c1, "hi")
    g0a.keep(4, 6)
    g0a.z_added()
    g1.cross()
    da2.close()
    db2.close()
    g0b.give(0, 2)
    g0b.keep(0, 2)
    g0b.z_first()
    x_fwd1(c1)
    x_fwd2(c1)
    g0b.give(2, 8)
    g0b.late()
    x_fwd3(c1)
    g0b.z_added()
    g0a.cross()
    x_near(c1)
    blocks(1, TR, AR, 1, 5, True)
    x_side(c1)
    blocks(1, TR, AR, 5, 7, False)
    x_far(c1)
    blocks(1, TR, AR, 7, 8, False)
    activate(TR, AR, into_x2, None)
    ha_s[...] = nt(headt[0:32, :], x2[TR : TR + AR, :])[0:24, :]
    acts = to_group(ha_s, ha_r, ha_r.at[pl.ds(0, 7), :, :])
    g0b.cross()
    g1.result()
    g0a.result()
    acts.wait_recv()
    al_out[...] = from_group(ha_s, ha_r)[0:ACT, :]
    g0b.result()

    for view, sem in sends:
        pltpu.make_async_remote_copy(
            src_ref=view, dst_ref=view, send_sem=sem, recv_sem=rsem.at[0], device_id=x_peer, device_id_type=MESH,
        ).wait_send()
    assert (count[0], count[1]) == (N_RECV, N_SEND), count


def hand_out_kernel(dw, hg, al, dw_out, hg_out, al_out, sems):
    copies = [pltpu.make_async_copy(a, b, sems.at[i]) for i, (a, b) in enumerate(((dw, dw_out), (hg, hg_out), (al, al_out)))]
    for copy in copies:
        copy.start()
    for copy in copies:
        copy.wait()


def hand_out(*arrays):
    arrays = [pltpu.with_memory_space_constraint(a, pltpu.VMEM) for a in arrays]
    hbm = pl.BlockSpec(memory_space=pltpu.HBM)
    return pl.pallas_call(
        hand_out_kernel,
        out_shape=tuple(jax.ShapeDtypeStruct(a.shape, a.dtype) for a in arrays),
        in_specs=[pl.BlockSpec(memory_space=pltpu.VMEM)] * 3,
        out_specs=(hbm,) * 3,
        scratch_shapes=[pltpu.SemaphoreType.DMA((3,))],
        name="hand_out",
    )(*arrays)


def per_device(observations, next_observations, trunk_weights, head_weights, acting, actions, rewards, finished):
    v = pltpu.VMEM
    dw_bufs = lambda rows: [
        v((8, rows, WB), BF16), v((8, rows, WB), BF16), v((8, rows, WB), BF16), v((2, rows, WB), BF16),
        v((2, 2, rows, WB), BF16), v((rows, WB), BF16), v((rows, WB), BF16),
    ]
    scratch = [
        v((8, TR + AR, FB), BF16), v((8, TR + AR, FB), BF16), v((8, FB, FB), BF16), v((8, FB, FB), BF16),
        v((TR + AR, FB), F32), v((TR, FB), F32), v((TR, FB), F32), v((TR + AR, FB), BF16),
        v((128, FB), BF16), v((128, CH), F32), v((2, 32, CH), F32),
        v((2, 24, CH), F32), v((2, 8, 24, CH), F32), v((24, 128), F32), v((8, 24, 128), F32),
        v((TR, 128), BF16), v((TR, FB), BF16), v((FB, TR), BF16), v((FB, TR), BF16), v((FB, 128), F32),
        v((7, TR, FB), BF16), v((7, TR, FB), BF16), v((TR, FB), F32),
        *dw_bufs(ER), *dw_bufs(FB),
        v((ACT + 1, FB), BF16), v((ACT, 8, STEPS - 1), F32), v((8, STEPS - 1), jnp.int32), v((8, STEPS - 1), F32),
        v((8, STEPS - 1), jnp.int32),
        pltpu.SemaphoreType.DMA((N_SEND,)), pltpu.SemaphoreType.DMA((N_RECV,)), pltpu.SemaphoreType.DMA((9,)),
    ]
    hbm = pl.BlockSpec(memory_space=pltpu.HBM)
    vm = pl.BlockSpec(memory_space=pltpu.VMEM)
    trunk_grads, head_grads, actor_logits = pl.pallas_call(
        kernel,
        out_shape=(
            pltpu.VMEM((2, WB, FB), F32),
            pltpu.VMEM((ACT + 1, 32), F32),
            pltpu.VMEM((ACT, AR), F32),
        ),
        in_specs=[hbm] * 8,
        out_specs=(vm,) * 3,
        scratch_shapes=scratch,
        compiler_params=pltpu.CompilerParams(
            collective_id=0, has_side_effects=True, vmem_limit_bytes=58 * 1024 * 1024
        ),
        name="learner_step",
    )(
        observations.reshape(TR, FB), next_observations, trunk_weights, head_weights.T, acting.transpose(2, 0, 1),
        actions, rewards, finished,
    )
    trunk_grads, head_grads, actor_logits = hand_out(trunk_grads, head_grads, actor_logits)
    return trunk_grads, head_grads.T, actor_logits.T


def solution(mesh):
    split = Mesh(mesh.devices.reshape(SIZES), AXES)
    return jax.shard_map(
        per_device,
        mesh=split,
        in_specs=(
            P(DP, None, GROUP),
            P(DP, GROUP),
            P(None, DP, GROUP),
            P(GROUP, None),
            P(DP, None, None),
            P(DP, None),
            P(DP, None),
            P(DP, None),
        ),
        out_specs=(P(None, DP, GROUP), P(GROUP + DP, None), P(DP, None)),
        check_vma=False,
    )
```
